256 devices in a mesh: frames: 64 (over y, x, z_lo), pix: 4 (over z_hi, core).
Axes of the slice: x: 4, y: 4, z: 8 (z_hi: 2, z_lo: 4; z = z_hi * 4 + z_lo), core: 2. Of those that a mesh axis runs over, the one named last changes fastest.
Arguments:
- edge_frames: int32 [2, 12288], P(None, 'frames'), may hold values from 0 to 1023, as said below
- rotvec: float32 [3, 1024], replicated, may hold values from -0.06 to 0.06
- trans: float32 [3, 1024], replicated, may hold values from -0.15 to 0.15
- inv_depth: float32 [1024, 3072], P('frames', 'pix'), may hold values from 0.2 to 1
- depth_damping: float32 [1024, 3072], P('frames', 'pix'), may hold values from 0.01 to 0.1
- flow: float32 [12288, 2, 3072], P('frames', None, 'pix'), may hold values from -0.3 to 0.3
- weight: float32 [12288, 2, 3072], P('frames', None, 'pix'), may hold values from 0.02 to 1
- mask: int32 [12288, 3072], P('frames', 'pix'), may hold values 0 or 1
Outputs:
- pose_step: float32 [6, 1024], P(None, 'frames')
- depth_step: float32 [1024, 3072], P('frames', 'pix')
The draws below stay inside these ranges and needn't reach their ends.
Inputs may be any that keep to these rules, and one draw needn't show every extreme that they name: Edge e of the block of 192 edges held by one index of frames has its target edge_frames[1, e] among that index's 16 keyframes; its source edge_frames[0, e] differs from the target by 1 to 8, and in every block some source lies exactly 8 away.
All inputs are finite; a program needn't handle non-finite values. No bound on the sum of `mask` on one device may be relied on, other than what follows from the above.
Results may differ from the reference program's by a relative error of at most 0.00015.
Values sent between devices are 32-bit elements; how exact they have to be, the bound alone decides.
No kernel may reach another device: no remote copies, remote signals or barrier semaphores. Data moves between devices by JAX's collectives and lax.ppermute only.
A program may use at most 64 MiB of HBM per device.

```python
import math
import jax
import jax.numpy as jnp
from jax import lax

F_DEV = 16
EDGE_DEV = 192
ROWS = 48
COLS = 64
RADIUS = 8
ITERS = 6
FRAMES = 1024
EDGES = 12288
PIX = 3072


def draw_edge_frames(key, part):
    keys = jax.random.split(jax.random.fold_in(key, 11), 4)
    index = jnp.arange(EDGES, dtype=jnp.int32)
    block = index // EDGE_DEV
    slot = index % EDGE_DEV
    first = jax.random.randint(keys[0], (EDGES,), 0, F_DEV)
    second = jax.random.randint(keys[1], (EDGES,), 0, F_DEV)
    local = jnp.minimum(first, second)
    local = jnp.where(slot == 0, 0, jnp.where(slot == 1, F_DEV - 1, local))
    offset = jax.random.randint(keys[2], (EDGES,), 1, RADIUS + 1)
    offset = jnp.where(slot < 2, RADIUS, offset)
    sign = 2 * jax.random.randint(keys[3], (EDGES,), 0, 2) - 1
    sign = jnp.where(slot == 0, -1, jnp.where(slot == 1, 1, sign))
    target = block * F_DEV + local
    source = target + sign * offset
    source = jnp.where((source < 0) | (source >= FRAMES), target - sign * offset, source)
    return jnp.stack([source, target]).astype(jnp.int32)


def draw_flow(key, part):
    keys = jax.random.split(jax.random.fold_in(key, 23), 2)
    shared = jnp.clip(0.06 * jax.random.normal(keys[0], (EDGES, 2, 1), jnp.float32), -0.2, 0.2)
    noise = jnp.clip(0.03 * jax.random.normal(keys[1], (EDGES, 2, PIX), jnp.float32), -0.1, 0.1)
    return shared + noise


def touch_ends(drawn, stream_key, low, high):
    place = [jax.random.randint(jax.random.fold_in(stream_key, axis), (), 0, length) for axis, length in enumerate(drawn.shape)]
    main_axis = drawn.shape.index(max(drawn.shape))
    neighbour = place[:main_axis] + [(place[main_axis] + 1) % drawn.shape[main_axis]] + place[main_axis + 1:]
    return drawn.at[tuple(place)].set(low).at[tuple(neighbour)].set(high)


def shard_levels(rng, shape, cuts, least, largest):
    gain = 1.0
    for axis_at, parts in cuts:
        steps = jax.random.uniform(jax.random.fold_in(jax.random.fold_in(rng, 6), axis_at), (parts,), jnp.float32, least / len(cuts), largest / len(cuts))
        gain = gain * jnp.repeat(jnp.exp(steps), shape[axis_at] // parts).reshape((-1,) + (1,) * (len(shape) - 1 - axis_at))
    return gain


def setup_inputs(seed: int = 0) -> dict:
    key_list = jax.random.split(jax.random.key(seed), 9)
    return {
        "edge_frames": draw_edge_frames(jax.random.fold_in(key_list[8], 71), 0),
        "rotvec": jnp.clip(jax.random.uniform(key_list[1], (3, FRAMES), jnp.float32, -0.06, 0.06), -0.06, 0.06),
        "trans": jnp.clip(jax.random.uniform(key_list[2], (3, FRAMES), jnp.float32, -0.15, 0.15), -0.15, 0.15),
        "inv_depth": jnp.clip(jnp.exp(math.log(1.0) - 1.609438 * jax.random.uniform(key_list[3], (FRAMES, PIX), jnp.float32) ** shard_levels(key_list[3], (FRAMES, PIX), ((0, 64), (1, 4)), -0.2, 0.2)), 0.2, 1.0),
        "depth_damping": jnp.clip(jnp.exp(math.log(0.1) - 2.3025851 * jax.random.uniform(key_list[4], (FRAMES, PIX), jnp.float32) ** shard_levels(key_list[4], (FRAMES, PIX), ((0, 64), (1, 4)), -0.2, 0.2)), 0.01, 0.1),
        "flow": draw_flow(jax.random.fold_in(key_list[8], 71), 0),
        "weight": jnp.clip(jnp.exp(math.log(1.0) - 3.912023 * jax.random.uniform(key_list[6], (EDGES, 2, PIX), jnp.float32) ** shard_levels(key_list[6], (EDGES, 2, PIX), ((0, 64), (2, 4)), -0.2, 0.2)), 0.02, 1.0),
        "mask": touch_ends((jax.random.randint(key_list[7], (EDGES, PIX), 0, 4) < 3).astype(jnp.int32), jax.random.fold_in(key_list[7], 1), 0, 1),
    }


exact = lax.Precision.HIGHEST
pose_regularizer = 100.0


def pixel_coords(pixel):
    row = pixel // COLS
    column = pixel % COLS
    col_coord = (column.astype(jnp.float32) - 0.5 * (COLS - 1)) / COLS
    row_coord = (row.astype(jnp.float32) - 0.5 * (ROWS - 1)) / COLS
    return col_coord, row_coord


def rotations(rotvec):
    omega_x, omega_y, omega_z = rotvec[0], rotvec[1], rotvec[2]
    zero = jnp.zeros_like(omega_x)
    cross = [[zero, -omega_z, omega_y], [omega_z, zero, -omega_x], [-omega_y, omega_x, zero]]
    theta_sq = omega_x * omega_x + omega_y * omega_y + omega_z * omega_z
    first_coef = 1.0 - theta_sq / 6.0 + theta_sq * theta_sq / 120.0
    second_coef = 0.5 - theta_sq / 24.0 + theta_sq * theta_sq / 720.0
    lines = []
    for row in range(3):
        entries = []
        for column in range(3):
            square = cross[row][0] * cross[0][column] + cross[row][1] * cross[1][column] + cross[row][2] * cross[2][column]
            entries.append(float(row == column) + first_coef * cross[row][column] + second_coef * square)
        lines.append(jnp.stack(entries))
    return jnp.stack(lines)


def relative(rot, trans, source, target):
    rot_source = jnp.take(rot, source, axis=2)
    rot_target = jnp.take(rot, target, axis=2)
    rel_rot = jnp.einsum('ike,jke->ije', rot_target, rot_source, precision=exact)
    rel_trans = jnp.take(trans, target, axis=1) - jnp.einsum('ije,je->ie', rel_rot, jnp.take(trans, source, axis=1), precision=exact)
    zero = jnp.zeros_like(rel_trans[0])
    skew = jnp.stack([jnp.stack([zero, -rel_trans[2], rel_trans[1]]),
                      jnp.stack([rel_trans[2], zero, -rel_trans[0]]),
                      jnp.stack([-rel_trans[1], rel_trans[0], zero])])
    corner = jnp.einsum('ike,kje->ije', skew, rel_rot, precision=exact)
    upper = jnp.concatenate([rel_rot, corner], axis=1)
    lower = jnp.concatenate([jnp.zeros_like(rel_rot), rel_rot], axis=1)
    return rel_rot, rel_trans, jnp.concatenate([upper, lower], axis=0)


def geometry(rel_rot, rel_trans, depth, flow, weight, mask, col_coord, row_coord):
    def coordinate(line):
        return (rel_rot[line, 0][:, None] * col_coord + rel_rot[line, 1][:, None] * row_coord
                + rel_rot[line, 2][:, None] + depth * rel_trans[line][:, None])
    inverse_z = 1.0 / coordinate(2)
    proj_u = coordinate(0) * inverse_z
    proj_v = coordinate(1) * inverse_z
    depth_scale = depth * inverse_z
    slope_u = inverse_z * (rel_trans[0][:, None] - proj_u * rel_trans[2][:, None])
    slope_v = inverse_z * (rel_trans[1][:, None] - proj_v * rel_trans[2][:, None])
    live = mask.astype(jnp.float32)
    conf_u = weight[:, 0] * live
    conf_v = weight[:, 1] * live
    error_u = col_coord + flow[:, 0] - proj_u
    error_v = row_coord + flow[:, 1] - proj_v
    return proj_u, proj_v, depth_scale, slope_u, slope_v, conf_u, conf_v, error_u, error_v


def apply_pose(geo, motion):
    proj_u, proj_v, depth_scale = geo[0], geo[1], geo[2]
    part = [motion[index][:, None] for index in range(6)]
    cross_uv = proj_u * proj_v
    lin_u = depth_scale * (part[0] - proj_u * part[2]) - cross_uv * part[3] + (1.0 + proj_u * proj_u) * part[4] - proj_v * part[5]
    lin_v = depth_scale * (part[1] - proj_v * part[2]) - (1.0 + proj_v * proj_v) * part[3] + cross_uv * part[4] + proj_u * part[5]
    return lin_u, lin_v


def pose_terms(geo, part_u, part_v):
    proj_u, proj_v, depth_scale = geo[0], geo[1], geo[2]
    heavy_u = geo[5] * part_u
    heavy_v = geo[6] * part_v
    cross_uv = proj_u * proj_v
    entries = [depth_scale * heavy_u, depth_scale * heavy_v,
               -depth_scale * (proj_u * heavy_u + proj_v * heavy_v),
               -cross_uv * heavy_u - (1.0 + proj_v * proj_v) * heavy_v,
               (1.0 + proj_u * proj_u) * heavy_u + cross_uv * heavy_v,
               -proj_v * heavy_u + proj_u * heavy_v]
    return jnp.stack([jnp.sum(entry, axis=1) for entry in entries])


def spread(motion, source, target, adjoint):
    return jnp.take(motion, target, axis=1) - jnp.einsum('jke,ke->je', adjoint, jnp.take(motion, source, axis=1), precision=exact)


def reference(edge_frames, rotvec, trans, inv_depth, depth_damping, flow, weight, mask):
    col_coord, row_coord = pixel_coords(jnp.arange(PIX, dtype=jnp.int32))
    rot = rotations(rotvec)
    blocks = EDGES // EDGE_DEV
    packed = (edge_frames[0].reshape(blocks, EDGE_DEV), edge_frames[1].reshape(blocks, EDGE_DEV),
              flow.reshape(blocks, EDGE_DEV, 2, PIX), weight.reshape(blocks, EDGE_DEV, 2, PIX),
              mask.reshape(blocks, EDGE_DEV, PIX))

    def sweep(update, init):
        def advance(carry, item):
            source, target, flow_block, weight_block, mask_block = item
            rel_rot, rel_trans, adjoint = relative(rot, trans, source, target)
            geo = geometry(rel_rot, rel_trans, jnp.take(inv_depth, source, axis=0), flow_block,
                           weight_block, mask_block, col_coord, row_coord)
            return update(carry, source, target, adjoint, geo), None
        return lax.scan(advance, init, packed)[0]

    def totals_update(carry, source, target, adjoint, geo):
        terms = jnp.stack([geo[5] * geo[3] * geo[3] + geo[6] * geo[4] * geo[4],
                           -(geo[3] * geo[5] * geo[7] + geo[4] * geo[6] * geo[8])])
        return carry.at[:, source].add(terms)

    totals = sweep(totals_update, jnp.zeros((2, FRAMES, PIX), jnp.float32))
    curvature = totals[0] + depth_damping
    base_step = totals[1] / curvature

    def pose_sweep(motion, image):
        def update(carry, source, target, adjoint, geo):
            at_source = jnp.take(image, source, axis=0)
            if motion is None:
                part_u = -geo[7] - geo[3] * at_source
                part_v = -geo[8] - geo[4] * at_source
            else:
                lin_u, lin_v = apply_pose(geo, spread(motion, source, target, adjoint))
                part_u = lin_u - geo[3] * at_source
                part_v = lin_v - geo[4] * at_source
            target_terms = pose_terms(geo, part_u, part_v)
            source_terms = -jnp.einsum('jke,je->ke', adjoint, target_terms, precision=exact)
            return carry.at[:, target].add(target_terms).at[:, source].add(source_terms)
        return sweep(update, jnp.zeros((6, FRAMES), jnp.float32))

    def depth_sweep(motion):
        def update(carry, source, target, adjoint, geo):
            lin_u, lin_v = apply_pose(geo, spread(motion, source, target, adjoint))
            return carry.at[source].add(geo[3] * geo[5] * lin_u + geo[4] * geo[6] * lin_v)
        return sweep(update, jnp.zeros((FRAMES, PIX), jnp.float32))

    def reduced(motion):
        image = depth_sweep(motion) / curvature
        return pose_sweep(motion, image) + pose_regularizer * motion

    rhs = pose_sweep(None, base_step)
    solution = jnp.zeros_like(rhs)
    residual = rhs
    direction = rhs
    norm_now = jnp.sum(residual * residual)
    for step in range(ITERS):
        product = reduced(direction)
        alpha = norm_now / jnp.sum(direction * product)
        solution = solution + alpha * direction
        residual = residual - alpha * product
        norm_next = jnp.sum(residual * residual)
        direction = residual + (norm_next / norm_now) * direction
        norm_now = norm_next
    depth_step = base_step - depth_sweep(solution) / curvature
    return solution, depth_step
```

```python
import functools
import jax
import jax.numpy as jnp
from jax import lax
from jax.experimental import pallas as pl
from jax.experimental.pallas import tpu as pltpu
from jax.sharding import PartitionSpec as P

ROWS = 48
COLS = 64
RADIUS = 8
ITERS = 6
HIGHEST = lax.Precision.HIGHEST
F32 = jnp.float32
BF16 = jnp.bfloat16
LANES = 128
FD = 16
SLOTS = 16
GROUP = FD * 6
SIDE = RADIUS * (RADIUS + 1) // 2
POSE_REG = 100.0


def iota(shape, dim):
    return lax.broadcasted_iota(jnp.int32, shape, dim)


def thirds(x):
    first = x.astype(BF16)
    rest = x - first.astype(F32)
    second = rest.astype(BF16)
    return first, second, (rest - second.astype(F32)).astype(BF16)


def scatter_kernel(where_ref, ef_ref, flow_ref, weight_ref, mask_ref, own_ref, down_ref, up_ref):
    edges = ef_ref.shape[1]
    start = where_ref[0]
    source = ef_ref[0:1, :] - start
    delta = ef_ref[1:2, :] - start - source
    slot = jnp.where(delta < 0, delta + 8, delta + 7)
    own_at = jnp.where((source >= 0) & (source < FD), source * SLOTS + slot, -1)
    j = source + 8
    down_at = jnp.where(source < 0, ((j * (j + 1)) >> 1) + delta - 8 + j, -1)
    j = 23 - source
    up_at = jnp.where(source >= FD, ((j * (j + 1)) >> 1) + slot, -1)
    hot = jnp.concatenate(
        [
            (iota((FD * SLOTS, edges), 0) == own_at).astype(F32),
            (iota((40, edges), 0) == down_at).astype(F32),
            (iota((40, edges), 0) == up_at).astype(F32),
        ],
        axis=0,
    ).astype(BF16)
    down_ref[0:8, :] = jnp.zeros((8, down_ref.shape[1]), F32)
    per_edge = 2 * (mask_ref.shape[1] // LANES)
    for chunk in range(mask_ref.shape[1] // LANES):
        lanes = pl.ds(chunk * LANES, LANES)
        live = mask_ref[:, lanes].astype(F32)
        parts = []
        for comp in range(2):
            rows = pl.ds(chunk * 2 + comp, edges, stride=per_edge)
            conf = weight_ref[rows, :] * live
            parts.append((conf, conf * flow_ref[rows, :]))
        values = jnp.concatenate([parts[0][0], parts[1][0], parts[0][1], parts[1][1]], axis=1)
        got = sum(
            jnp.dot(hot, piece, preferred_element_type=F32) for piece in reversed(thirds(values))
        )
        for q in range(4):
            cut = got[:, q * LANES : (q + 1) * LANES]
            own_ref[q * 256 : (q + 1) * 256, lanes] = cut[0:256]
            down_ref[8 + q * SIDE : 8 + (q + 1) * SIDE, lanes] = cut[256 : 256 + SIDE]
            up_ref[q * SIDE : (q + 1) * SIDE, lanes] = cut[296 : 296 + SIDE]


def rotation_rows(w):
    x, y, z = w
    zero = jnp.zeros_like(x)
    cross = [[zero, -z, y], [z, zero, -x], [-y, x, zero]]
    sq = x * x + y * y + z * z
    first = 1.0 - sq / 6.0 + sq * sq / 120.0
    second = 0.5 - sq / 24.0 + sq * sq / 720.0
    return [
        [
            float(i == k)
            + first * cross[i][k]
            + second * sum(cross[i][m] * cross[m][k] for m in range(3))
            for k in range(3)
        ]
        for i in range(3)
    ]


def pose_kernel(where_ref, rotvec_ref, trans_ref, tab_ref, b_ref, bt_ref):
    start = where_ref[0]
    frames = rotvec_ref.shape[1]
    pair = iota((1, FD * SLOTS), 1)
    slot = pair & 15
    delta = jnp.where(slot < 8, slot - 8, slot - 7)
    at_source = start + (pair >> 4)
    at_target = jnp.clip(at_source + delta, 0, frames - 1)
    poses = jnp.concatenate([rotvec_ref[...], trans_ref[...], jnp.zeros((2, frames), F32)], axis=0)

    def pick(at):
        hot = (iota((frames, FD * SLOTS), 0) == at).astype(F32)
        return jnp.dot(poses, hot, precision=HIGHEST, preferred_element_type=F32)

    src = pick(at_source)
    tgt = pick(at_target)
    rs = rotation_rows([src[k : k + 1] for k in range(3)])
    rt = rotation_rows([tgt[k : k + 1] for k in range(3)])
    rel = [[sum(rt[i][k] * rs[m][k] for k in range(3)) for m in range(3)] for i in range(3)]
    tr = [
        tgt[3 + i : 4 + i] - sum(rel[i][m] * src[3 + m : 4 + m] for m in range(3)) for i in range(3)
    ]
    corner = [
        [tr[1] * rel[2][m] - tr[2] * rel[1][m] for m in range(3)],
        [tr[2] * rel[0][m] - tr[0] * rel[2][m] for m in range(3)],
        [tr[0] * rel[1][m] - tr[1] * rel[0][m] for m in range(3)],
    ]
    lines = [x for row in rel for x in row] + tr + [x for row in corner for x in row]
    lines = jnp.concatenate(lines + [jnp.zeros((LANES - len(lines), FD * SLOTS), F32)], axis=0)
    tab_ref[...] = lines.T

    lane3 = iota((SLOTS, 3 * LANES), 1)
    row3 = iota((SLOTS, 3 * LANES), 0)
    off3 = jnp.where(row3 < 8, row3 - 8, row3 - 7)

    def build(f, carry):
        frame = f + off3 + FD
        home = (frame >> 4) * LANES + (frame & 15) * 6
        tab = tab_ref[pl.ds(pl.multiple_of(f * SLOTS, SLOTS), SLOTS), :]
        for c in range(6):
            block = jnp.where(lane3 == home + c, 1.0, 0.0)
            for d in range(6):
                if c < 3:
                    at = c * 3 + d if d < 3 else 12 + c * 3 + d - 3
                elif d >= 3:
                    at = (c - 3) * 3 + d - 3
                else:
                    continue
                block = block - jnp.where(
                    lane3 == LANES + f * 6 + d, jnp.broadcast_to(tab[:, at : at + 1], lane3.shape), 0.0
                )
            b_ref[pl.ds(pl.multiple_of(f * GROUP + c * SLOTS, SLOTS), SLOTS), :] = block
        return carry

    lax.fori_loop(0, FD, build, 0)
    for g in range(4):
        cols = slice(g * 384, (g + 1) * 384)
        below = b_ref[cols, 0:LANES].T
        own = b_ref[cols, LANES : 2 * LANES].T
        above = b_ref[cols, 2 * LANES : 3 * LANES].T
        bt_ref[0:48, cols] = below[48:96]
        bt_ref[48:144, cols] = own[0:96]
        bt_ref[144:192, cols] = above[0:48]


def main_kernel(
    where_ref, own_ref, rdown_ref, rup_ref, depth_ref, damp_ref, tab_ref, b_ref, bt_ref,
    keep_ref, send_ref, g_ref, base_ref, scale_ref,
    half_ref, geo_ref, hi_ref, in_ref, q_ref, w_ref, t_ref,
):
    core = where_ref[2]
    plocal = depth_ref.shape[1]
    chunks = plocal // LANES
    row8 = iota((8, plocal), 0)
    for f in range(FD):
        j = 7 - f if f < 8 else f - 8
        base = j * (j + 1) // 2
        for q in range(4):
            if f < 8:
                extra = jnp.where(row8 <= j, rup_ref[q * SIDE + base : q * SIDE + base + 8, :], 0.0)
                at = q * 256 + f * SLOTS
            else:
                first = 8 + q * SIDE + base - 7 + j
                extra = jnp.where(row8 >= 7 - j, rdown_ref[first : first + 8, :], 0.0)
                at = q * 256 + f * SLOTS + 8
            half_ref[(q * FD + f) * 8 : (q * FD + f + 1) * 8, :] = own_ref[at : at + 8, :] + extra
        in_ref[f * 8 : f * 8 + 8, :] = jnp.broadcast_to(depth_ref[f : f + 1, :], (8, plocal))
        in_ref[128 + f * 8 : 136 + f * 8, :] = jnp.broadcast_to(damp_ref[f : f + 1, :], (8, plocal))
    lane = iota((8, LANES), 1)
    row = iota((8, LANES), 0)

    def frame(f, carry, merged):
        eight = pl.ds(pl.multiple_of(f * 8, 8), 8)
        def conf(q, h, lanes):
            if h == merged:
                at = (q * FD + f) * 8
                return half_ref[pl.ds(pl.multiple_of(at, 8), 8), lanes]
            at = q * 256 + f * SLOTS + 8 * h
            return own_ref[pl.ds(pl.multiple_of(at, 8), 8), lanes]

        params = []
        for h in range(2):
            tab = tab_ref[pl.ds(pl.multiple_of(f * SLOTS + 8 * h, 8), 8), :]
            params.append([jnp.broadcast_to(tab[:, k : k + 1], (8, LANES)) for k in range(12)])
        base_all = []
        scale_all = []
        for c in range(chunks):
            lanes = pl.ds(c * LANES, LANES)
            pixel = where_ref[1] + c * LANES + lane
            col = ((pixel & (COLS - 1)).astype(F32) - 0.5 * (COLS - 1)) / COLS
            line = ((pixel >> 6).astype(F32) - 0.5 * (ROWS - 1)) / COLS
            depth = in_ref[eight, lanes]
            curv = 0.0
            grad = 0.0
            for h in range(2):
                r = params[h]
                z = r[6] * col + r[7] * line + r[8] + depth * r[11]
                inv = 1.0 / z
                u = (r[0] * col + r[1] * line + r[2] + depth * r[9]) * inv
                v = (r[3] * col + r[4] * line + r[5] + depth * r[10]) * inv
                s = depth * inv
                su = inv * (r[9] - u * r[11])
                sv = inv * (r[10] - v * r[11])
                cu = conf(0, h, lanes)
                cv = conf(1, h, lanes)
                eu = cu * (col - u) + conf(2, h, lanes)
                ev = cv * (line - v) + conf(3, h, lanes)
                au = cu * su
                av = cv * sv
                curv = curv + au * su + av * sv
                grad = grad - (su * eu + sv * ev)
                for k, x in enumerate((u, v, s, au, av, eu, ev)):
                    geo_ref[k * 16 + 8 * h : k * 16 + 8 * h + 8, lanes] = x
            damp = in_ref[pl.ds(pl.multiple_of(128 + f * 8, 8), 8), lanes]
            total = damp + jnp.sum(curv, axis=0, keepdims=True)
            base = jnp.sum(grad, axis=0, keepdims=True) / total
            scale = 1.0 / jnp.sqrt(total)
            base_ref[eight, lanes] = base
            scale_ref[eight, lanes] = scale
            base_all.append(base)
            scale_all.append(scale)
        cols = {}
        for h in range(2):
            acc = [0.0] * 27
            for c in range(chunks):
                lanes = pl.ds(c * LANES, LANES)
                u, v, s, au, av, eu, ev = [
                    geo_ref[k * 16 + 8 * h : k * 16 + 8 * h + 8, lanes] for k in range(7)
                ]
                cu = conf(0, h, lanes)
                cv = conf(1, h, lanes)
                base = base_all[c]
                scale = scale_all[c]
                hu = -eu - au * base
                hv = -ev - av * base
                uv = u * v
                u1 = 1.0 + u * u
                v1 = 1.0 + v * v

                def pull(pu, pv):
                    spu = s * pu
                    spv = s * pv
                    return (
                        spu,
                        spv,
                        -(u * spu + v * spv),
                        -(uv * pu) - v1 * pv,
                        u1 * pu + uv * pv,
                        u * pv - v * pu,
                    )

                for k, x in enumerate(pull(au * scale, av * scale)):
                    at = pl.ds(pl.multiple_of(f * GROUP + k * SLOTS + 8 * h, 8), 8)
                    g_ref[at, lanes] = x
                    hi_ref[k * SLOTS + 8 * h : k * SLOTS + 8 * h + 8, lanes] = x
                su_ = cu * s
                sv_ = cv * s
                ju = (None, None, None, -uv, u1, -v)
                jv = (None, None, None, -v1, uv, u)
                terms = list(pull(hu, hv))
                a00 = su_ * s
                a11 = sv_ * s
                a02 = -(a00 * u)
                a12 = -(a11 * v)
                a22 = -(a02 * u + a12 * v)
                terms += [a00, a11, a02, a12, a22]
                tu = [su_ * ju[k] for k in (3, 4, 5)]
                tv = [sv_ * jv[k] for k in (3, 4, 5)]
                terms += tu + tv
                terms += [-(u * tu[k] + v * tv[k]) for k in range(3)]
                wu = [cu * ju[k] for k in (3, 4, 5)]
                wv = [cv * jv[k] for k in (3, 4, 5)]
                for a in range(3):
                    for b in range(a, 3):
                        terms.append(wu[a] * ju[3 + b] + wv[a] * jv[3 + b])
                acc = [x + y for x, y in zip(acc, terms)]
            assert len(acc) == len(terms)
            sums = [jnp.sum(x, axis=1, keepdims=True) for x in acc]
            a = {(0, 0): sums[6], (1, 1): sums[7], (0, 2): sums[8], (1, 2): sums[9], (2, 2): sums[10]}
            for k in range(3):
                a[(0, 3 + k)] = sums[11 + k]
                a[(1, 3 + k)] = sums[14 + k]
                a[(2, 3 + k)] = sums[17 + k]
            at = 20
            for x in range(3):
                for y in range(x, 3):
                    a[(3 + x, 3 + y)] = sums[at]
                    at += 1
            for c in range(6):
                block = jnp.zeros((8, LANES), F32)
                for d in range(6):
                    key = (min(c, d), max(c, d))
                    if key == (0, 1):
                        continue
                    block = jnp.where(
                        lane == d * SLOTS + 8 * h + row, jnp.broadcast_to(a[key], (8, LANES)), block
                    )
                q_ref[c * SLOTS + 8 * h : c * SLOTS + 8 * h + 8, :] = block
                cols[(c, h)] = sums[c]
        g = hi_ref[...]
        top = g.astype(BF16)
        low = (g - top.astype(F32)).astype(BF16)
        left = jnp.concatenate([top, low, top], axis=1)
        right = jnp.concatenate([top, top, low], axis=1)
        m = lax.dot_general(left, right, (((1,), (1,)), ((), ())), preferred_element_type=F32)
        q = q_ref[:, 0:GROUP] - m
        rows = pl.ds(pl.multiple_of(f * GROUP, 8), GROUP)
        w_ref[rows, :] = jnp.dot(q, b_ref[rows, :], precision=HIGHEST, preferred_element_type=F32)
        for c in range(6):
            for h in range(2):
                at = pl.ds(pl.multiple_of(f * GROUP + c * SLOTS + 8 * h, 8), 8)
                w_ref[at, 0:LANES] = jnp.where(
                    lane == LANES - 1, jnp.broadcast_to(cols[(c, h)], (8, LANES)), w_ref[at, 0:LANES]
                )
        return carry

    lax.fori_loop(0, 8, functools.partial(frame, merged=0), 0)
    lax.fori_loop(8, 16, functools.partial(frame, merged=1), 0)
    t_ref[...] = jnp.dot(bt_ref[...], w_ref[...], precision=HIGHEST, preferred_element_type=F32)
    keep_ref[0:48, :] = t_ref[pl.ds(pl.multiple_of(48 + 48 * core, 8), 48), :]
    keep_ref[48:96, :] = t_ref[pl.ds(pl.multiple_of(144 - 144 * core, 8), 48), :]
    send_ref[0:48, :] = t_ref[pl.ds(pl.multiple_of(96 - 48 * core, 8), 48), :]
    send_ref[48:96, :] = t_ref[pl.ds(pl.multiple_of(144 * core, 8), 48), :]


def rows_kernel(where_ref, own_ref, own2_ref, rim_ref, rim2_ref, out_ref):
    core = where_ref[2]
    own = own_ref[...] + own2_ref[...]
    rim = rim_ref[...] + rim2_ref[...]
    lane = iota((48, LANES), 1)
    below = rim[:, 0:LANES]
    mid = rim[:, LANES : 2 * LANES]
    above = rim[:, 2 * LANES :]
    vec = jnp.where(lane == LANES - 1, below, 0.0)
    below = jnp.where(lane == LANES - 1, 0.0, below)
    low = core == 0
    out_ref[:, 0:LANES] = own[:, 0:LANES] + vec + jnp.where(low, mid, 0.0)
    out_ref[:, LANES : 2 * LANES] = own[:, LANES : 2 * LANES] + jnp.where(low, above, below)
    out_ref[:, 2 * LANES :] = own[:, 2 * LANES :] + jnp.where(low, 0.0, mid)


def to_row(column):
    return jnp.sum(
        jnp.where(iota((GROUP, LANES), 0) == iota((GROUP, LANES), 1), column, 0.0),
        axis=0,
        keepdims=True,
    )


def full_kernel(where_ref, mine_ref, other_ref, s_ref, r_ref):
    core = where_ref[2]
    mine = mine_ref[...]
    other = other_ref[...]
    low = core == 0
    s = jnp.concatenate([jnp.where(low, mine, other), jnp.where(low, other, mine)], axis=0)
    r_ref[...] = jnp.zeros((8, LANES), F32)
    r_ref[0:1, :] = to_row(s[:, LANES - 1 : LANES])
    r = iota((GROUP, 3 * LANES), 0)
    l = iota((GROUP, 3 * LANES), 1)
    s = jnp.where(l == LANES - 1, 0.0, s)
    s_ref[...] = s + jnp.where(l == LANES + r, POSE_REG, 0.0)


def mv_kernel(s_ref, below_ref, own_ref, above_ref, out_ref, dots_ref):
    own = own_ref[0:1, :]
    s = s_ref[...]
    prod = (
        s[:, 0:LANES] * below_ref[0:1, :]
        + s[:, LANES : 2 * LANES] * own
        + s[:, 2 * LANES :] * above_ref[0:1, :]
    )
    y = to_row(jnp.sum(prod, axis=1, keepdims=True))
    out_ref[...] = jnp.zeros((8, LANES), F32)
    out_ref[0:1, :] = y
    rr = jnp.sum(own * own, axis=1, keepdims=True)
    ry = jnp.sum(own * y, axis=1, keepdims=True)
    row = iota((8, LANES), 0)
    dots_ref[...] = jnp.where(row == 0, jnp.broadcast_to(rr, (8, LANES)), jnp.broadcast_to(ry, (8, LANES)))


def final_kernel(below_ref, own_ref, above_ref, b_ref, g_ref, base_ref, scale_ref, out_ref, sum_ref):
    x0 = below_ref[0:1, :]
    x1 = own_ref[0:1, :]
    x2 = above_ref[0:1, :]

    def frame(f, carry):
        rows = pl.ds(pl.multiple_of(f * GROUP, 8), GROUP)
        prod = (
            b_ref[rows, 0:LANES] * x0
            + b_ref[rows, LANES : 2 * LANES] * x1
            + b_ref[rows, 2 * LANES : 3 * LANES] * x2
        )
        x = jnp.sum(prod, axis=1, keepdims=True)
        image = jnp.sum(g_ref[rows, :] * x, axis=0, keepdims=True)
        at = pl.ds(pl.multiple_of(f * 8, 8), 8)
        sum_ref[at, :] = base_ref[at, :] - scale_ref[at, :] * image
        return carry

    lax.fori_loop(0, FD, frame, 0)
    for f in range(FD):
        out_ref[f : f + 1, :] = sum_ref[f * 8 : f * 8 + 1, :]


SMEM = pl.BlockSpec(memory_space=pltpu.SMEM)
VMEM = pl.BlockSpec(memory_space=pltpu.VMEM)


def call(kernel, name, outs, smem, *args, scratch=()):
    return pl.pallas_call(
        kernel,
        name=name,
        out_shape=[jax.ShapeDtypeStruct(s, F32) for s in outs],
        in_specs=[SMEM] * smem + [VMEM] * (len(args) - smem),
        out_specs=[VMEM] * len(outs),
        scratch_shapes=list(scratch),
    )(*args)


def per_device(edge_frames, rotvec, trans, inv_depth, depth_damping, flow, weight, mask):
    f_dev, plocal = inv_depth.shape
    edges = mask.shape[0]
    count = lax.axis_size("frames")
    pixes = lax.axis_size("pix")
    fi = lax.axis_index("frames")
    pi = lax.axis_index("pix")
    spot = jnp.stack([fi * f_dev, pi * plocal, pi % 2]).astype(jnp.int32)

    def shift(block, step):
        return lax.ppermute(
            block, "frames", [(i, i + step) for i in range(count) if 0 <= i + step < count]
        )

    def view(x):
        return x.reshape(edges, 2, plocal // LANES, LANES).transpose(0, 2, 1, 3).reshape(-1, LANES)

    own, down, up = call(
        scatter_kernel, "scatter",
        [(4 * f_dev * SLOTS, plocal), (8 + 4 * SIDE, plocal), (4 * SIDE, plocal)],
        1, spot, edge_frames, view(flow), view(weight), mask,
    )
    from_after = shift(down, -1)
    from_before = shift(up, 1)
    tab, b, bt = call(
        pose_kernel, "pose",
        [(f_dev * SLOTS, LANES), (f_dev * GROUP, 3 * LANES), (192, f_dev * GROUP)],
        1, spot, rotvec, trans,
    )
    keep, send, g, base, scale = call(
        main_kernel, "main",
        [(96, 384), (96, 384), (f_dev * GROUP, plocal), (f_dev * 8, plocal), (f_dev * 8, plocal)],
        1, spot, own, from_after, from_before, inv_depth, depth_damping, tab, b, bt,
        scratch=[
            pltpu.VMEM((4 * FD * 8, plocal), F32),
            pltpu.VMEM((7 * 16, plocal), F32),
            pltpu.VMEM((GROUP, plocal), F32),
            pltpu.VMEM((256, plocal), F32),
            pltpu.VMEM((GROUP, LANES), F32),
            pltpu.VMEM((f_dev * GROUP, 3 * LANES), F32),
            pltpu.VMEM((192, 3 * LANES), F32),
        ],
    )
    got = lax.ppermute(send, "pix", [(i, i ^ 1) for i in range(pixes)])
    both = keep + got
    own_half, rim = both[:48], both[48:]
    both_axes = ("frames", "pix")

    def to_neighbour(flip):
        route = []
        for i in range(count):
            for k in range(pixes):
                to = i + 1 if k % 2 == 0 else i - 1
                if 0 <= to < count:
                    route.append((i * pixes + k, to * pixes + (k ^ flip)))
        return lax.ppermute(rim, both_axes, route)

    own_far = lax.ppermute(own_half, "pix", [(i, i ^ 2) for i in range(pixes)])
    rim_near = to_neighbour(0)
    rim_far = to_neighbour(2)
    (half,) = call(rows_kernel, "rows", [(48, 384)], 1, spot, own_half, own_far, rim_near, rim_far)
    other = lax.ppermute(half, "pix", [(i, i ^ 1) for i in range(pixes)])
    s, residual = call(full_kernel, "full", [(96, 384), (8, LANES)], 1, spot, half, other)

    def halo(v):
        return shift(v, 1), v, shift(v, -1)

    def total(v):
        for step in (1, 4, 16):
            v = v + sum(
                lax.ppermute(v, "frames", [(i, i ^ (k * step)) for i in range(count)])
                for k in (1, 2, 3)
            )
        return v

    def reduced(v):
        q, dots = call(mv_kernel, "mv", [(8, LANES), (8, LANES)], 0, s, *halo(v))
        dots = total(dots)
        return q, dots[0, 0], dots[1, 0]

    solution = jnp.zeros_like(residual)
    image, norm_now, product = reduced(residual)
    alpha = norm_now / product
    direction, along = residual, image
    for step in range(ITERS):
        solution = solution + alpha * direction
        residual = residual - alpha * along
        if step + 1 < ITERS:
            image, norm_next, product = reduced(residual)
            ratio = norm_next / norm_now
            alpha = norm_next / (product - ratio * norm_next / alpha)
            direction = residual + ratio * direction
            along = image + ratio * along
            norm_now = norm_next
    (depth_step,) = call(
        final_kernel, "final", [(f_dev, plocal)], 0, *halo(solution), b, g, base, scale,
        scratch=[pltpu.VMEM((f_dev * 8, plocal), F32)],
    )
    pose_step = solution[0, : f_dev * 6].reshape(f_dev, 6).T
    return pose_step, depth_step


def solution(mesh):
    return jax.shard_map(
        per_device,
        mesh=mesh,
        in_specs=(
            P(None, "frames"),
            P(),
            P(),
            P("frames", "pix"),
            P("frames", "pix"),
            P("frames", None, "pix"),
            P("frames", None, "pix"),
            P("frames", "pix"),
        ),
        out_specs=(P(None, "frames"), P("frames", "pix")),
        check_vma=False,
    )
```

```python
import functools
import jax
import jax.numpy as jnp
from jax import lax
from jax.experimental import pallas as pl
from jax.experimental.pallas import tpu as pltpu
from jax.sharding import PartitionSpec as P

ROWS = 48
COLS = 64
RADIUS = 8
ITERS = 6
HIGHEST = lax.Precision.HIGHEST
F32 = jnp.float32
BF16 = jnp.bfloat16
LANES = 128
FD = 16
SLOTS = 16
GROUP = FD * 6
SIDE = RADIUS * (RADIUS + 1) // 2
POSE_REG = 100.0


def iota(shape, dim):
    return lax.broadcasted_iota(jnp.int32, shape, dim)


def thirds(x):
    first = x.astype(BF16)
    rest = x - first.astype(F32)
    second = rest.astype(BF16)
    return first, second, (rest - second.astype(F32)).astype(BF16)


def scatter_kernel(where_ref, ef_ref, flow_ref, weight_ref, mask_ref, own_ref, down_ref, up_ref):
    edges = ef_ref.shape[1]
    start = where_ref[0]
    source = ef_ref[0:1, :] - start
    delta = ef_ref[1:2, :] - start - source
    slot = jnp.where(delta < 0, delta + 8, delta + 7)
    own_at = jnp.where((source >= 0) & (source < FD), source * SLOTS + slot, -1)
    j = source + 8
    down_at = jnp.where(source < 0, ((j * (j + 1)) >> 1) + delta - 8 + j, -1)
    j = 23 - source
    up_at = jnp.where(source >= FD, ((j * (j + 1)) >> 1) + slot, -1)
    hot = jnp.concatenate(
        [
            (iota((FD * SLOTS, edges), 0) == own_at).astype(F32),
            (iota((40, edges), 0) == down_at).astype(F32),
            (iota((40, edges), 0) == up_at).astype(F32),
        ],
        axis=0,
    ).astype(BF16)
    down_ref[0:8, :] = jnp.zeros((8, down_ref.shape[1]), F32)
    per_edge = 2 * (mask_ref.shape[1] // LANES)
    for chunk in range(mask_ref.shape[1] // LANES):
        lanes = pl.ds(chunk * LANES, LANES)
        live = mask_ref[:, lanes].astype(F32)
        parts = []
        for comp in range(2):
            rows = pl.ds(chunk * 2 + comp, edges, stride=per_edge)
            conf = weight_ref[rows, :] * live
            parts.append((conf, conf * flow_ref[rows, :]))
        values = jnp.concatenate([parts[0][0], parts[1][0], parts[0][1], parts[1][1]], axis=1)
        got = sum(
            jnp.dot(hot, piece, preferred_element_type=F32) for piece in reversed(thirds(values))
        )
        for q in range(4):
            cut = got[:, q * LANES : (q + 1) * LANES]
            own_ref[q * 256 : (q + 1) * 256, lanes] = cut[0:256]
            down_ref[8 + q * SIDE : 8 + (q + 1) * SIDE, lanes] = cut[256 : 256 + SIDE]
            up_ref[q * SIDE : (q + 1) * SIDE, lanes] = cut[296 : 296 + SIDE]


def rotation_rows(w):
    x, y, z = w
    zero = jnp.zeros_like(x)
    cross = [[zero, -z, y], [z, zero, -x], [-y, x, zero]]
    sq = x * x + y * y + z * z
    first = 1.0 - sq / 6.0 + sq * sq / 120.0
    second = 0.5 - sq / 24.0 + sq * sq / 720.0
    return [
        [
            float(i == k)
            + first * cross[i][k]
            + second * sum(cross[i][m] * cross[m][k] for m in range(3))
            for k in range(3)
        ]
        for i in range(3)
    ]


def pose_kernel(where_ref, rotvec_ref, trans_ref, tab_ref, b_ref, bt_ref):
    start = where_ref[0]
    frames = rotvec_ref.shape[1]
    pair = iota((1, FD * SLOTS), 1)
    slot = pair & 15
    delta = jnp.where(slot < 8, slot - 8, slot - 7)
    at_source = start + (pair >> 4)
    at_target = jnp.clip(at_source + delta, 0, frames - 1)
    poses = jnp.concatenate([rotvec_ref[...], trans_ref[...], jnp.zeros((2, frames), F32)], axis=0)

    def pick(at):
        hot = (iota((frames, FD * SLOTS), 0) == at).astype(F32)
        return jnp.dot(poses, hot, precision=HIGHEST, preferred_element_type=F32)

    src = pick(at_source)
    tgt = pick(at_target)
    rs = rotation_rows([src[k : k + 1] for k in range(3)])
    rt = rotation_rows([tgt[k : k + 1] for k in range(3)])
    rel = [[sum(rt[i][k] * rs[m][k] for k in range(3)) for m in range(3)] for i in range(3)]
    tr = [
        tgt[3 + i : 4 + i] - sum(rel[i][m] * src[3 + m : 4 + m] for m in range(3)) for i in range(3)
    ]
    corner = [
        [tr[1] * rel[2][m] - tr[2] * rel[1][m] for m in range(3)],
        [tr[2] * rel[0][m] - tr[0] * rel[2][m] for m in range(3)],
        [tr[0] * rel[1][m] - tr[1] * rel[0][m] for m in range(3)],
    ]
    lines = [x for row in rel for x in row] + tr + [x for row in corner for x in row]
    lines = jnp.concatenate(lines + [jnp.zeros((LANES - len(lines), FD * SLOTS), F32)], axis=0)
    tab_ref[...] = lines.T

    lane3 = iota((SLOTS, 3 * LANES), 1)
    row3 = iota((SLOTS, 3 * LANES), 0)
    off3 = jnp.where(row3 < 8, row3 - 8, row3 - 7)

    def build(f, carry):
        frame = f + off3 + FD
        home = (frame >> 4) * LANES + (frame & 15) * 6
        tab = tab_ref[pl.ds(pl.multiple_of(f * SLOTS, SLOTS), SLOTS), :]
        for c in range(6):
            block = jnp.where(lane3 == home + c, 1.0, 0.0)
            for d in range(6):
                if c < 3:
                    at = c * 3 + d if d < 3 else 12 + c * 3 + d - 3
                elif d >= 3:
                    at = (c - 3) * 3 + d - 3
                else:
                    continue
                block = block - jnp.where(
                    lane3 == LANES + f * 6 + d, jnp.broadcast_to(tab[:, at : at + 1], lane3.shape), 0.0
                )
            b_ref[pl.ds(pl.multiple_of(f * GROUP + c * SLOTS, SLOTS), SLOTS), :] = block
        return carry

    lax.fori_loop(0, FD, build, 0)
    for g in range(4):
        cols = slice(g * 384, (g + 1) * 384)
        below = b_ref[cols, 0:LANES].T
        own = b_ref[cols, LANES : 2 * LANES].T
        above = b_ref[cols, 2 * LANES : 3 * LANES].T
        bt_ref[0:48, cols] = below[48:96]
        bt_ref[48:144, cols] = own[0:96]
        bt_ref[144:192, cols] = above[0:48]


def main_kernel(
    where_ref, own_ref, rdown_ref, rup_ref, depth_ref, damp_ref, tab_ref, b_ref, bt_ref,
    keep_ref, send_ref, g_ref, base_ref, scale_ref,
    half_ref, geo_ref, hi_ref, in_ref, q_ref, w_ref, t_ref, sym_ref,
):
    core = where_ref[2]
    plocal = depth_ref.shape[1]
    chunks = plocal // LANES
    row8 = iota((8, plocal), 0)
    for f in range(FD):
        j = 7 - f if f < 8 else f - 8
        base = j * (j + 1) // 2
        for q in range(4):
            if f < 8:
                extra = jnp.where(row8 <= j, rup_ref[q * SIDE + base : q * SIDE + base + 8, :], 0.0)
                at = q * 256 + f * SLOTS
            else:
                first = 8 + q * SIDE + base - 7 + j
                extra = jnp.where(row8 >= 7 - j, rdown_ref[first : first + 8, :], 0.0)
                at = q * 256 + f * SLOTS + 8
            half_ref[(q * FD + f) * 8 : (q * FD + f + 1) * 8, :] = own_ref[at : at + 8, :] + extra
        in_ref[f * 8 : f * 8 + 8, :] = jnp.broadcast_to(depth_ref[f : f + 1, :], (8, plocal))
        in_ref[128 + f * 8 : 136 + f * 8, :] = jnp.broadcast_to(damp_ref[f : f + 1, :], (8, plocal))
    lane = iota((8, LANES), 1)
    row = iota((8, LANES), 0)

    def frame(f, carry, merged):
        eight = pl.ds(pl.multiple_of(f * 8, 8), 8)
        def conf(q, h, lanes):
            if h == merged:
                at = (q * FD + f) * 8
                return half_ref[pl.ds(pl.multiple_of(at, 8), 8), lanes]
            at = q * 256 + f * SLOTS + 8 * h
            return own_ref[pl.ds(pl.multiple_of(at, 8), 8), lanes]

        params = []
        for h in range(2):
            tab = tab_ref[pl.ds(pl.multiple_of(f * SLOTS + 8 * h, 8), 8), :]
            params.append([jnp.broadcast_to(tab[:, k : k + 1], (8, LANES)) for k in range(12)])
        base_all = []
        scale_all = []
        for c in range(chunks):
            lanes = pl.ds(c * LANES, LANES)
            pixel = where_ref[1] + c * LANES + lane
            col = ((pixel & (COLS - 1)).astype(F32) - 0.5 * (COLS - 1)) / COLS
            line = ((pixel >> 6).astype(F32) - 0.5 * (ROWS - 1)) / COLS
            depth = in_ref[eight, lanes]
            curv = 0.0
            grad = 0.0
            for h in range(2):
                r = params[h]
                z = r[6] * col + r[7] * line + r[8] + depth * r[11]
                inv = 1.0 / z
                u = (r[0] * col + r[1] * line + r[2] + depth * r[9]) * inv
                v = (r[3] * col + r[4] * line + r[5] + depth * r[10]) * inv
                s = depth * inv
                su = inv * (r[9] - u * r[11])
                sv = inv * (r[10] - v * r[11])
                cu = conf(0, h, lanes)
                cv = conf(1, h, lanes)
                eu = cu * (col - u) + conf(2, h, lanes)
                ev = cv * (line - v) + conf(3, h, lanes)
                au = cu * su
                av = cv * sv
                curv = curv + au * su + av * sv
                grad = grad - (su * eu + sv * ev)
                for k, x in enumerate((u, v, s, au, av, eu, ev)):
                    geo_ref[k * 16 + 8 * h : k * 16 + 8 * h + 8, lanes] = x
            damp = in_ref[pl.ds(pl.multiple_of(128 + f * 8, 8), 8), lanes]
            total = damp + jnp.sum(curv, axis=0, keepdims=True)
            base = jnp.sum(grad, axis=0, keepdims=True) / total
            scale = 1.0 / jnp.sqrt(total)
            base_ref[eight, lanes] = base
            scale_ref[eight, lanes] = scale
            base_all.append(base)
            scale_all.append(scale)
        cols = {}
        for h in range(2):
            acc = [0.0] * 27
            for c in range(chunks):
                lanes = pl.ds(c * LANES, LANES)
                u, v, s, au, av, eu, ev = [
                    geo_ref[k * 16 + 8 * h : k * 16 + 8 * h + 8, lanes] for k in range(7)
                ]
                cu = conf(0, h, lanes)
                cv = conf(1, h, lanes)
                base = base_all[c]
                scale = scale_all[c]
                hu = -eu - au * base
                hv = -ev - av * base
                uv = u * v
                u1 = 1.0 + u * u
                v1 = 1.0 + v * v

                def pull(pu, pv):
                    spu = s * pu
                    spv = s * pv
                    return (
                        spu,
                        spv,
                        -(u * spu + v * spv),
                        -(uv * pu) - v1 * pv,
                        u1 * pu + uv * pv,
                        u * pv - v * pu,
                    )

                for k, x in enumerate(pull(au * scale, av * scale)):
                    at = pl.ds(pl.multiple_of(f * GROUP + k * SLOTS + 8 * h, 8), 8)
                    g_ref[at, lanes] = x
                    hi_ref[k * SLOTS + 8 * h : k * SLOTS + 8 * h + 8, lanes] = x
                su_ = cu * s
                sv_ = cv * s
                ju = (None, None, None, -uv, u1, -v)
                jv = (None, None, None, -v1, uv, u)
                terms = list(pull(hu, hv))
                a00 = su_ * s
                a11 = sv_ * s
                a02 = -(a00 * u)
                a12 = -(a11 * v)
                a22 = -(a02 * u + a12 * v)
                terms += [a00, a11, a02, a12, a22]
                tu = [su_ * ju[k] for k in (3, 4, 5)]
                tv = [sv_ * jv[k] for k in (3, 4, 5)]
                terms += tu + tv
                terms += [-(u * tu[k] + v * tv[k]) for k in range(3)]
                wu = [cu * ju[k] for k in (3, 4, 5)]
                wv = [cv * jv[k] for k in (3, 4, 5)]
                for a in range(3):
                    for b in range(a, 3):
                        terms.append(wu[a] * ju[3 + b] + wv[a] * jv[3 + b])
                acc = [x + y for x, y in zip(acc, terms)]
            assert len(acc) == len(terms)
            sums = [jnp.sum(x, axis=1, keepdims=True) for x in acc]
            a = {(0, 0): sums[6], (1, 1): sums[7], (0, 2): sums[8], (1, 2): sums[9], (2, 2): sums[10]}
            for k in range(3):
                a[(0, 3 + k)] = sums[11 + k]
                a[(1, 3 + k)] = sums[14 + k]
                a[(2, 3 + k)] = sums[17 + k]
            at = 20
            for x in range(3):
                for y in range(x, 3):
                    a[(3 + x, 3 + y)] = sums[at]
                    at += 1
            for c in range(6):
                block = jnp.zeros((8, LANES), F32)
                for d in range(6):
                    key = (min(c, d), max(c, d))
                    if key == (0, 1):
                        continue
                    block = jnp.where(
                        lane == d * SLOTS + 8 * h + row, jnp.broadcast_to(a[key], (8, LANES)), block
                    )
                q_ref[c * SLOTS + 8 * h : c * SLOTS + 8 * h + 8, :] = block
                cols[(c, h)] = sums[c]
        g = hi_ref[...]
        top = g.astype(BF16)
        low = (g - top.astype(F32)).astype(BF16)
        left = jnp.concatenate([top, low, top], axis=1)
        right = jnp.concatenate([top, top, low], axis=1)
        m = lax.dot_general(left, right, (((1,), (1,)), ((), ())), preferred_element_type=F32)
        q = q_ref[:, 0:GROUP] - m
        rows = pl.ds(pl.multiple_of(f * GROUP, 8), GROUP)
        w_ref[rows, :] = jnp.dot(q, b_ref[rows, :], precision=HIGHEST, preferred_element_type=F32)
        for c in range(6):
            for h in range(2):
                at = pl.ds(pl.multiple_of(f * GROUP + c * SLOTS + 8 * h, 8), 8)
                w_ref[at, 0:LANES] = jnp.where(
                    lane == LANES - 1, jnp.broadcast_to(cols[(c, h)], (8, LANES)), w_ref[at, 0:LANES]
                )
        return carry

    lax.fori_loop(0, 8, functools.partial(frame, merged=0), 0)
    lax.fori_loop(8, 16, functools.partial(frame, merged=1), 0)
    t = jnp.dot(bt_ref[...], w_ref[...], precision=HIGHEST, preferred_element_type=F32)
    spans = ((0, 48, 48), (48, 144, LANES), (144, 192, 2 * LANES))
    t_ref[...] = jnp.zeros_like(t_ref)
    for lo, hi, at in spans:
        t_ref[at : at + hi - lo, :] = t[lo:hi]
    vector = iota((LANES, LANES), 1) == LANES - 1
    for a in range(3):
        for b in range(a, 3):
            at_a = slice(a * LANES, (a + 1) * LANES)
            at_b = slice(b * LANES, (b + 1) * LANES)
            upper = t_ref[at_a, at_b]
            lower = t_ref[at_b, at_a]
            mean = 0.5 * (jnp.where(vector, 0.0, upper) + jnp.where(vector, 0.0, lower).T)
            sym_ref[at_a, at_b] = jnp.where(vector, upper, mean)
            if a != b:
                sym_ref[at_b, at_a] = jnp.where(vector, lower, mean.T)
    for lo, hi, at in spans:
        t_ref[lo:hi, :] = sym_ref[at : at + hi - lo, :]
    keep_ref[0:48, :] = t_ref[pl.ds(pl.multiple_of(48 + 48 * core, 8), 48), :]
    keep_ref[48:96, :] = t_ref[pl.ds(pl.multiple_of(144 - 144 * core, 8), 48), :]
    send_ref[0:48, :] = t_ref[pl.ds(pl.multiple_of(96 - 48 * core, 8), 48), :]
    send_ref[48:96, :] = t_ref[pl.ds(pl.multiple_of(144 * core, 8), 48), :]


def rows_kernel(where_ref, own_ref, own2_ref, rim_ref, rim2_ref, out_ref):
    core = where_ref[2]
    own = own_ref[...] + own2_ref[...]
    rim = rim_ref[...] + rim2_ref[...]
    lane = iota((48, LANES), 1)
    below = rim[:, 0:LANES]
    mid = rim[:, LANES : 2 * LANES]
    above = rim[:, 2 * LANES :]
    vec = jnp.where(lane == LANES - 1, below, 0.0)
    below = jnp.where(lane == LANES - 1, 0.0, below)
    low = core == 0
    out_ref[:, 0:LANES] = own[:, 0:LANES] + vec + jnp.where(low, mid, 0.0)
    out_ref[:, LANES : 2 * LANES] = own[:, LANES : 2 * LANES] + jnp.where(low, above, below)
    out_ref[:, 2 * LANES :] = own[:, 2 * LANES :] + jnp.where(low, 0.0, mid)


def to_row(column):
    return jnp.sum(
        jnp.where(iota((GROUP, LANES), 0) == iota((GROUP, LANES), 1), column, 0.0),
        axis=0,
        keepdims=True,
    )


def full_kernel(where_ref, mine_ref, other_ref, s_ref, r_ref):
    core = where_ref[2]
    mine = mine_ref[...]
    other = other_ref[...]
    low = core == 0
    s = jnp.concatenate([jnp.where(low, mine, other), jnp.where(low, other, mine)], axis=0)
    r_ref[...] = jnp.zeros((8, LANES), F32)
    r_ref[0:1, :] = to_row(s[:, LANES - 1 : LANES]) * FIRST
    r = iota((GROUP, 3 * LANES), 0)
    l = iota((GROUP, 3 * LANES), 1)
    s = jnp.where(l == LANES - 1, 0.0, s)
    s_ref[...] = s + jnp.where(l == LANES + r, POSE_REG, 0.0)


SHRINK = 2.0**-15
FIRST = 2.0**-10
LARGEST_STEP = 1.001 / (POSE_REG * SHRINK)


def halves(x):
    t = 4097.0 * x
    top = t - (t - x)
    return top, x - top


def times(a, b):
    p = a * b
    ah, al = halves(a)
    bh, bl = halves(b)
    return p, ((ah * bh - p) + ah * bl + al * bh) + al * bl


def plus(a, b):
    t = a[0] + b[0]
    back = t - a[0]
    return t, (a[1] + b[1]) + ((a[0] - (t - back)) + (b[0] - back))


def tidy(a):
    t = a[0] + a[1]
    return t, a[1] - (t - a[0])


def mul(a, b):
    p, e = times(a[0], b[0])
    return tidy((p, e + (a[0] * b[1] + a[1] * b[0])))


def add(a, b):
    return tidy(plus(a, b))


def neg(a):
    return -a[0], -a[1]


def div(a, b):
    q = a[0] / b[0]
    rest = add(a, neg(mul((q, jnp.zeros_like(q)), b)))
    return tidy((q, rest[0] / b[0]))


def lane_total(a):
    for step in (64, 32, 16, 8, 4, 2, 1):
        a = plus(a, (pltpu.roll(a[0], step, 1), pltpu.roll(a[1], step, 1)))
    return a


def next_vector(s_ref, below_ref, own_ref, above_ref):
    acc = None
    for g, ref in enumerate((below_ref, own_ref, above_ref)):
        s = s_ref[:, g * LANES : (g + 1) * LANES]
        p, e = times(s, jnp.broadcast_to(ref[0:1, :], s.shape))
        term = p, e + s * ref[1:2, :]
        acc = term if acc is None else plus(acc, term)
    acc = lane_total(acc)
    row = tidy((to_row(acc[0]), to_row(acc[1])))
    return row[0] * SHRINK, row[1] * SHRINK


def put(ref, pair):
    ref[...] = jnp.zeros((8, LANES), F32)
    ref[0:1, :] = pair[0]
    ref[1:2, :] = pair[1]


def step_kernel(s_ref, below_ref, own_ref, above_ref, out_ref):
    put(out_ref, next_vector(s_ref, below_ref, own_ref, above_ref))


def moment_kernel(s_ref, below_ref, own_ref, above_ref, *rest):
    out_ref = rest[-1]
    rows = [(r[0:1, :], r[1:2, :]) for r in rest[:-1]] + [(own_ref[0:1, :], own_ref[1:2, :])]
    rows.append(next_vector(s_ref, below_ref, own_ref, above_ref))
    zero = jnp.zeros((1, LANES), F32)

    def stack(pick, part):
        lines = [rows[pick(m)][part] for m in range(2 * ITERS)]
        return jnp.concatenate(lines + [zero] * (16 - len(lines)), axis=0)

    lower, upper = (lambda m: m // 2), (lambda m: m - m // 2)
    a, b = (stack(lower, 0), stack(lower, 1)), (stack(upper, 0), stack(upper, 1))
    p, e = times(a[0], b[0])
    total = tidy(lane_total((p, e + (a[0] * b[1] + a[1] * b[0]))))
    diagonal = iota((16, LANES), 0) == iota((16, LANES), 1)
    put(
        out_ref,
        [jnp.sum(jnp.where(diagonal, x, 0.0), axis=0, keepdims=True) for x in total],
    )


def gather_sum(refs):
    acc = refs[0][0:1, :], refs[0][1:2, :]
    for r in refs[1:]:
        acc = plus(acc, (r[0:1, :], r[1:2, :]))
    return tidy(acc)


def sum_kernel(a_ref, b_ref, c_ref, d_ref, out_ref):
    put(out_ref, gather_sum((a_ref, b_ref, c_ref, d_ref)))


def solve_kernel(*refs):
    out_ref = refs[-1]
    total = gather_sum(refs[:4])
    vectors = refs[4:-1]
    m = [(total[0][:, k : k + 1], total[1][:, k : k + 1]) for k in range(2 * ITERS)]
    one = jnp.ones((1, 1), F32)
    zero = jnp.zeros((1, 1), F32)
    none = (zero, zero)

    def where(live, a, b):
        return jnp.where(live, a[0], b[0]), jnp.where(live, a[1], b[1])

    sigma = list(m)
    tau = list(m)
    rc = [(one, zero)] + [none] * ITERS
    pc = list(rc)
    xc = [none] * ITERS
    lead = one
    live = m[0][0] > 0.0
    for k in range(ITERS):
        alpha = div(sigma[k], where(live, tau[k + 1], (one, zero)))
        live = live & (alpha[0] > 0.0) & (alpha[0] < LARGEST_STEP)
        alpha = where(live, alpha, none)
        for i in range(k + 1):
            xc[i] = add(xc[i], mul(alpha, pc[i]))
        if k + 1 == ITERS:
            break
        back = neg(alpha)
        fresh = {i: add(sigma[i], mul(back, tau[i + 1])) for i in range(k + 1, 2 * ITERS - k - 1)}
        for i in range(k + 1, 0, -1):
            rc[i] = add(rc[i], mul(back, pc[i - 1]))
        lead = -lead * alpha[0]
        live = live & (lead * fresh[k + 1][0] > 1e-11 * m[0][0])
        beta = div(mul(back, fresh[k + 1]), where(live, sigma[k], (one, zero)))
        beta = where(live, beta, none)
        for i, x in fresh.items():
            tau[i] = add(x, mul(beta, tau[i]))
            sigma[i] = x
        pc = [add(rc[i], mul(beta, pc[i])) for i in range(k + 2)] + [none] * (ITERS - k - 1)
    for g in range(3):
        acc = None
        for k in range(ITERS):
            ref = vectors[3 * k + g]
            wide = tuple(jnp.broadcast_to(x, (1, LANES)) for x in xc[k])
            term = mul(wide, (ref[0:1, :], ref[1:2, :]))
            acc = term if acc is None else plus(acc, term)
        out_ref[g * 8 : g * 8 + 8, :] = jnp.broadcast_to(
            (acc[0] + acc[1]) * (SHRINK / FIRST), (8, LANES)
        )


def final_kernel(pose_ref, b_ref, g_ref, base_ref, scale_ref, out_ref, sum_ref):
    x0 = pose_ref[0:1, :]
    x1 = pose_ref[8:9, :]
    x2 = pose_ref[16:17, :]

    def frame(f, carry):
        rows = pl.ds(pl.multiple_of(f * GROUP, 8), GROUP)
        prod = (
            b_ref[rows, 0:LANES] * x0
            + b_ref[rows, LANES : 2 * LANES] * x1
            + b_ref[rows, 2 * LANES : 3 * LANES] * x2
        )
        x = jnp.sum(prod, axis=1, keepdims=True)
        image = jnp.sum(g_ref[rows, :] * x, axis=0, keepdims=True)
        at = pl.ds(pl.multiple_of(f * 8, 8), 8)
        sum_ref[at, :] = base_ref[at, :] - scale_ref[at, :] * image
        return carry

    lax.fori_loop(0, FD, frame, 0)
    for f in range(FD):
        out_ref[f : f + 1, :] = sum_ref[f * 8 : f * 8 + 1, :]


SMEM = pl.BlockSpec(memory_space=pltpu.SMEM)
VMEM = pl.BlockSpec(memory_space=pltpu.VMEM)


def call(kernel, name, outs, smem, *args, scratch=()):
    return pl.pallas_call(
        kernel,
        name=name,
        out_shape=[jax.ShapeDtypeStruct(s, F32) for s in outs],
        in_specs=[SMEM] * smem + [VMEM] * (len(args) - smem),
        out_specs=[VMEM] * len(outs),
        scratch_shapes=list(scratch),
    )(*args)


def per_device(edge_frames, rotvec, trans, inv_depth, depth_damping, flow, weight, mask):
    f_dev, plocal = inv_depth.shape
    edges = mask.shape[0]
    count = lax.axis_size("frames")
    pixes = lax.axis_size("pix")
    fi = lax.axis_index("frames")
    pi = lax.axis_index("pix")
    spot = jnp.stack([fi * f_dev, pi * plocal, pi % 2]).astype(jnp.int32)

    def shift(block, step):
        return lax.ppermute(
            block, "frames", [(i, i + step) for i in range(count) if 0 <= i + step < count]
        )

    def view(x):
        return x.reshape(edges, 2, plocal // LANES, LANES).transpose(0, 2, 1, 3).reshape(-1, LANES)

    own, down, up = call(
        scatter_kernel, "scatter",
        [(4 * f_dev * SLOTS, plocal), (8 + 4 * SIDE, plocal), (4 * SIDE, plocal)],
        1, spot, edge_frames, view(flow), view(weight), mask,
    )
    from_after = shift(down, -1)
    from_before = shift(up, 1)
    tab, b, bt = call(
        pose_kernel, "pose",
        [(f_dev * SLOTS, LANES), (f_dev * GROUP, 3 * LANES), (192, f_dev * GROUP)],
        1, spot, rotvec, trans,
    )
    keep, send, g, base, scale = call(
        main_kernel, "main",
        [(96, 384), (96, 384), (f_dev * GROUP, plocal), (f_dev * 8, plocal), (f_dev * 8, plocal)],
        1, spot, own, from_after, from_before, inv_depth, depth_damping, tab, b, bt,
        scratch=[
            pltpu.VMEM((4 * FD * 8, plocal), F32),
            pltpu.VMEM((7 * 16, plocal), F32),
            pltpu.VMEM((GROUP, plocal), F32),
            pltpu.VMEM((256, plocal), F32),
            pltpu.VMEM((GROUP, LANES), F32),
            pltpu.VMEM((f_dev * GROUP, 3 * LANES), F32),
            pltpu.VMEM((3 * LANES, 3 * LANES), F32),
            pltpu.VMEM((3 * LANES, 3 * LANES), F32),
        ],
    )
    got = lax.ppermute(send, "pix", [(i, i ^ 1) for i in range(pixes)])
    both = keep + got
    own_half, rim = both[:48], both[48:]
    both_axes = ("frames", "pix")

    def to_neighbour(flip):
        route = []
        for i in range(count):
            for k in range(pixes):
                to = i + 1 if k % 2 == 0 else i - 1
                if 0 <= to < count:
                    route.append((i * pixes + k, to * pixes + (k ^ flip)))
        return lax.ppermute(rim, both_axes, route)

    own_far = lax.ppermute(own_half, "pix", [(i, i ^ 2) for i in range(pixes)])
    rim_near = to_neighbour(0)
    rim_far = to_neighbour(2)
    (half,) = call(rows_kernel, "rows", [(48, 384)], 1, spot, own_half, own_far, rim_near, rim_far)
    other = lax.ppermute(half, "pix", [(i, i ^ 1) for i in range(pixes)])
    s, residual = call(full_kernel, "full", [(96, 384), (8, LANES)], 1, spot, half, other)

    def halo(v):
        return shift(v, 1), v, shift(v, -1)

    def mates(v, step):
        return [v] + [
            lax.ppermute(v, "frames", [(i, i ^ (k * step)) for i in range(count)]) for k in (1, 2, 3)
        ]

    vectors = []
    for k in range(ITERS - 1):
        vectors.append(halo(residual))
        (residual,) = call(step_kernel, "step", [(8, LANES)], 0, s, *vectors[-1])
    vectors.append(halo(residual))
    (part,) = call(
        moment_kernel, "moments", [(8, LANES)], 0, s, *vectors[-1], *[v[1] for v in vectors[:-1]]
    )
    for step in (1, 4):
        (part,) = call(sum_kernel, "sum", [(8, LANES)], 0, *mates(part, step))
    (pose,) = call(
        solve_kernel, "solve", [(24, LANES)], 0, *mates(part, 16), *[x for v in vectors for x in v]
    )
    (depth_step,) = call(
        final_kernel, "final", [(f_dev, plocal)], 0, pose, b, g, base, scale,
        scratch=[pltpu.VMEM((f_dev * 8, plocal), F32)],
    )
    pose_step = pose[8, : f_dev * 6].reshape(f_dev, 6).T
    return pose_step, depth_step


def solution(mesh):
    return jax.shard_map(
        per_device,
        mesh=mesh,
        in_specs=(
            P(None, "frames"),
            P(),
            P(),
            P("frames", "pix"),
            P("frames", "pix"),
            P("frames", None, "pix"),
            P("frames", None, "pix"),
            P("frames", "pix"),
        ),
        out_specs=(P(None, "frames"), P("frames", "pix")),
        check_vma=False,
    )
```

```python
import functools
import jax
import jax.numpy as jnp
from jax import lax
from jax.experimental import pallas as pl
from jax.experimental.pallas import tpu as pltpu
from jax.sharding import PartitionSpec as P

ROWS = 48
COLS = 64
RADIUS = 8
ITERS = 6
HIGHEST = lax.Precision.HIGHEST
F32 = jnp.float32
BF16 = jnp.bfloat16
LANES = 128
FD = 16
SLOTS = 16
GROUP = FD * 6
SIDE = RADIUS * (RADIUS + 1) // 2
POSE_REG = 100.0


def iota(shape, dim):
    return lax.broadcasted_iota(jnp.int32, shape, dim)


def thirds(x):
    first = x.astype(BF16)
    rest = x - first.astype(F32)
    second = rest.astype(BF16)
    return first, second, (rest - second.astype(F32)).astype(BF16)


def scatter_kernel(where_ref, ef_ref, flow_ref, weight_ref, mask_ref, own_ref, down_ref, up_ref):
    edges = ef_ref.shape[1]
    start = where_ref[0]
    source = ef_ref[0:1, :] - start
    delta = ef_ref[1:2, :] - start - source
    slot = jnp.where(delta < 0, delta + 8, delta + 7)
    own_at = jnp.where((source >= 0) & (source < FD), source * SLOTS + slot, -1)
    j = source + 8
    down_at = jnp.where(source < 0, ((j * (j + 1)) >> 1) + delta - 8 + j, -1)
    j = 23 - source
    up_at = jnp.where(source >= FD, ((j * (j + 1)) >> 1) + slot, -1)
    hot = jnp.concatenate(
        [
            (iota((FD * SLOTS, edges), 0) == own_at).astype(F32),
            (iota((40, edges), 0) == down_at).astype(F32),
            (iota((40, edges), 0) == up_at).astype(F32),
        ],
        axis=0,
    ).astype(BF16)
    down_ref[0:8, :] = jnp.zeros((8, down_ref.shape[1]), F32)
    per_edge = 2 * (mask_ref.shape[1] // LANES)
    for chunk in range(mask_ref.shape[1] // LANES):
        lanes = pl.ds(chunk * LANES, LANES)
        live = mask_ref[:, lanes].astype(F32)
        parts = []
        for comp in range(2):
            rows = pl.ds(chunk * 2 + comp, edges, stride=per_edge)
            conf = weight_ref[rows, :] * live
            parts.append((conf, conf * flow_ref[rows, :]))
        values = jnp.concatenate([parts[0][0], parts[1][0], parts[0][1], parts[1][1]], axis=1)
        got = sum(
            jnp.dot(hot, piece, preferred_element_type=F32) for piece in reversed(thirds(values))
        )
        for q in range(4):
            cut = got[:, q * LANES : (q + 1) * LANES]
            own_ref[q * 256 : (q + 1) * 256, lanes] = cut[0:256]
            down_ref[8 + q * SIDE : 8 + (q + 1) * SIDE, lanes] = cut[256 : 256 + SIDE]
            up_ref[q * SIDE : (q + 1) * SIDE, lanes] = cut[296 : 296 + SIDE]


def rotation_rows(w):
    x, y, z = w
    zero = jnp.zeros_like(x)
    cross = [[zero, -z, y], [z, zero, -x], [-y, x, zero]]
    sq = x * x + y * y + z * z
    first = 1.0 - sq / 6.0 + sq * sq / 120.0
    second = 0.5 - sq / 24.0 + sq * sq / 720.0
    return [
        [
            float(i == k)
            + first * cross[i][k]
            + second * sum(cross[i][m] * cross[m][k] for m in range(3))
            for k in range(3)
        ]
        for i in range(3)
    ]


def pose_kernel(where_ref, rotvec_ref, trans_ref, tab_ref, b_ref, bt_ref):
    start = where_ref[0]
    frames = rotvec_ref.shape[1]
    pair = iota((1, FD * SLOTS), 1)
    slot = pair & 15
    delta = jnp.where(slot < 8, slot - 8, slot - 7)
    at_source = start + (pair >> 4)
    at_target = jnp.clip(at_source + delta, 0, frames - 1)
    poses = jnp.concatenate([rotvec_ref[...], trans_ref[...], jnp.zeros((2, frames), F32)], axis=0)

    def pick(at):
        hot = (iota((frames, FD * SLOTS), 0) == at).astype(F32)
        return jnp.dot(poses, hot, precision=HIGHEST, preferred_element_type=F32)

    src = pick(at_source)
    tgt = pick(at_target)
    rs = rotation_rows([src[k : k + 1] for k in range(3)])
    rt = rotation_rows([tgt[k : k + 1] for k in range(3)])
    rel = [[sum(rt[i][k] * rs[m][k] for k in range(3)) for m in range(3)] for i in range(3)]
    tr = [
        tgt[3 + i : 4 + i] - sum(rel[i][m] * src[3 + m : 4 + m] for m in range(3)) for i in range(3)
    ]
    corner = [
        [tr[1] * rel[2][m] - tr[2] * rel[1][m] for m in range(3)],
        [tr[2] * rel[0][m] - tr[0] * rel[2][m] for m in range(3)],
        [tr[0] * rel[1][m] - tr[1] * rel[0][m] for m in range(3)],
    ]
    lines = [x for row in rel for x in row] + tr + [x for row in corner for x in row]
    lines = jnp.concatenate(lines + [jnp.zeros((LANES - len(lines), FD * SLOTS), F32)], axis=0)
    tab_ref[...] = lines.T

    lane3 = iota((SLOTS, 3 * LANES), 1)
    row3 = iota((SLOTS, 3 * LANES), 0)
    off3 = jnp.where(row3 < 8, row3 - 8, row3 - 7)

    def build(f, carry):
        frame = f + off3 + FD
        home = (frame >> 4) * LANES + (frame & 15) * 6
        tab = tab_ref[pl.ds(pl.multiple_of(f * SLOTS, SLOTS), SLOTS), :]
        for c in range(6):
            block = jnp.where(lane3 == home + c, 1.0, 0.0)
            for d in range(6):
                if c < 3:
                    at = c * 3 + d if d < 3 else 12 + c * 3 + d - 3
                elif d >= 3:
                    at = (c - 3) * 3 + d - 3
                else:
                    continue
                block = block - jnp.where(
                    lane3 == LANES + f * 6 + d, jnp.broadcast_to(tab[:, at : at + 1], lane3.shape), 0.0
                )
            b_ref[pl.ds(pl.multiple_of(f * GROUP + c * SLOTS, SLOTS), SLOTS), :] = block
        return carry

    lax.fori_loop(0, FD, build, 0)
    for g in range(4):
        cols = slice(g * 384, (g + 1) * 384)
        below = b_ref[cols, 0:LANES].T
        own = b_ref[cols, LANES : 2 * LANES].T
        above = b_ref[cols, 2 * LANES : 3 * LANES].T
        bt_ref[0:48, cols] = below[48:96]
        bt_ref[48:144, cols] = own[0:96]
        bt_ref[144:192, cols] = above[0:48]


def main_kernel(
    where_ref, own_ref, rdown_ref, rup_ref, depth_ref, damp_ref, tab_ref, b_ref, bt_ref,
    keep_ref, send_ref, g_ref, base_ref, scale_ref,
    half_ref, geo_ref, hi_ref, in_ref, q_ref, w_ref, t_ref,
):
    core = where_ref[2]
    plocal = depth_ref.shape[1]
    chunks = plocal // LANES
    row8 = iota((8, plocal), 0)
    for f in range(FD):
        j = 7 - f if f < 8 else f - 8
        base = j * (j + 1) // 2
        for q in range(4):
            if f < 8:
                extra = jnp.where(row8 <= j, rup_ref[q * SIDE + base : q * SIDE + base + 8, :], 0.0)
                at = q * 256 + f * SLOTS
            else:
                first = 8 + q * SIDE + base - 7 + j
                extra = jnp.where(row8 >= 7 - j, rdown_ref[first : first + 8, :], 0.0)
                at = q * 256 + f * SLOTS + 8
            half_ref[(q * FD + f) * 8 : (q * FD + f + 1) * 8, :] = own_ref[at : at + 8, :] + extra
        in_ref[f * 8 : f * 8 + 8, :] = jnp.broadcast_to(depth_ref[f : f + 1, :], (8, plocal))
        in_ref[128 + f * 8 : 136 + f * 8, :] = jnp.broadcast_to(damp_ref[f : f + 1, :], (8, plocal))
    lane = iota((8, LANES), 1)
    row = iota((8, LANES), 0)

    def frame(f, carry, merged):
        eight = pl.ds(pl.multiple_of(f * 8, 8), 8)
        def conf(q, h, lanes):
            if h == merged:
                at = (q * FD + f) * 8
                return half_ref[pl.ds(pl.multiple_of(at, 8), 8), lanes]
            at = q * 256 + f * SLOTS + 8 * h
            return own_ref[pl.ds(pl.multiple_of(at, 8), 8), lanes]

        params = []
        for h in range(2):
            tab = tab_ref[pl.ds(pl.multiple_of(f * SLOTS + 8 * h, 8), 8), :]
            params.append([jnp.broadcast_to(tab[:, k : k + 1], (8, LANES)) for k in range(12)])
        base_all = []
        scale_all = []
        for c in range(chunks):
            lanes = pl.ds(c * LANES, LANES)
            pixel = where_ref[1] + c * LANES + lane
            col = ((pixel & (COLS - 1)).astype(F32) - 0.5 * (COLS - 1)) / COLS
            line = ((pixel >> 6).astype(F32) - 0.5 * (ROWS - 1)) / COLS
            depth = in_ref[eight, lanes]
            curv = 0.0
            grad = 0.0
            for h in range(2):
                r = params[h]
                z = r[6] * col + r[7] * line + r[8] + depth * r[11]
                inv = 1.0 / z
                u = (r[0] * col + r[1] * line + r[2] + depth * r[9]) * inv
                v = (r[3] * col + r[4] * line + r[5] + depth * r[10]) * inv
                s = depth * inv
                su = inv * (r[9] - u * r[11])
                sv = inv * (r[10] - v * r[11])
                cu = conf(0, h, lanes)
                cv = conf(1, h, lanes)
                eu = cu * (col - u) + conf(2, h, lanes)
                ev = cv * (line - v) + conf(3, h, lanes)
                au = cu * su
                av = cv * sv
                curv = curv + au * su + av * sv
                grad = grad - (su * eu + sv * ev)
                for k, x in enumerate((u, v, s, au, av, eu, ev)):
                    geo_ref[k * 16 + 8 * h : k * 16 + 8 * h + 8, lanes] = x
            damp = in_ref[pl.ds(pl.multiple_of(128 + f * 8, 8), 8), lanes]
            total = damp + jnp.sum(curv, axis=0, keepdims=True)
            base = jnp.sum(grad, axis=0, keepdims=True) / total
            scale = 1.0 / jnp.sqrt(total)
            base_ref[eight, lanes] = base
            scale_ref[eight, lanes] = scale
            base_all.append(base)
            scale_all.append(scale)
        cols = {}
        for h in range(2):
            acc = [0.0] * 27
            for c in range(chunks):
                lanes = pl.ds(c * LANES, LANES)
                u, v, s, au, av, eu, ev = [
                    geo_ref[k * 16 + 8 * h : k * 16 + 8 * h + 8, lanes] for k in range(7)
                ]
                cu = conf(0, h, lanes)
                cv = conf(1, h, lanes)
                base = base_all[c]
                scale = scale_all[c]
                hu = -eu - au * base
                hv = -ev - av * base
                uv = u * v
                u1 = 1.0 + u * u
                v1 = 1.0 + v * v

                def pull(pu, pv):
                    spu = s * pu
                    spv = s * pv
                    return (
                        spu,
                        spv,
                        -(u * spu + v * spv),
                        -(uv * pu) - v1 * pv,
                        u1 * pu + uv * pv,
                        u * pv - v * pu,
                    )

                for k, x in enumerate(pull(au * scale, av * scale)):
                    at = pl.ds(pl.multiple_of(f * GROUP + k * SLOTS + 8 * h, 8), 8)
                    g_ref[at, lanes] = x
                    hi_ref[k * SLOTS + 8 * h : k * SLOTS + 8 * h + 8, lanes] = x
                su_ = cu * s
                sv_ = cv * s
                ju = (None, None, None, -uv, u1, -v)
                jv = (None, None, None, -v1, uv, u)
                terms = list(pull(hu, hv))
                a00 = su_ * s
                a11 = sv_ * s
                a02 = -(a00 * u)
                a12 = -(a11 * v)
                a22 = -(a02 * u + a12 * v)
                terms += [a00, a11, a02, a12, a22]
                tu = [su_ * ju[k] for k in (3, 4, 5)]
                tv = [sv_ * jv[k] for k in (3, 4, 5)]
                terms += tu + tv
                terms += [-(u * tu[k] + v * tv[k]) for k in range(3)]
                wu = [cu * ju[k] for k in (3, 4, 5)]
                wv = [cv * jv[k] for k in (3, 4, 5)]
                for a in range(3):
                    for b in range(a, 3):
                        terms.append(wu[a] * ju[3 + b] + wv[a] * jv[3 + b])
                acc = [x + y for x, y in zip(acc, terms)]
            assert len(acc) == len(terms)
            sums = [jnp.sum(x, axis=1, keepdims=True) for x in acc]
            a = {(0, 0): sums[6], (1, 1): sums[7], (0, 2): sums[8], (1, 2): sums[9], (2, 2): sums[10]}
            for k in range(3):
                a[(0, 3 + k)] = sums[11 + k]
                a[(1, 3 + k)] = sums[14 + k]
                a[(2, 3 + k)] = sums[17 + k]
            at = 20
            for x in range(3):
                for y in range(x, 3):
                    a[(3 + x, 3 + y)] = sums[at]
                    at += 1
            for c in range(6):
                block = jnp.zeros((8, LANES), F32)
                for d in range(6):
                    key = (min(c, d), max(c, d))
                    if key == (0, 1):
                        continue
                    block = jnp.where(
                        lane == d * SLOTS + 8 * h + row, jnp.broadcast_to(a[key], (8, LANES)), block
                    )
                q_ref[c * SLOTS + 8 * h : c * SLOTS + 8 * h + 8, :] = block
                cols[(c, h)] = sums[c]
        g = hi_ref[...]
        top = g.astype(BF16)
        low = (g - top.astype(F32)).astype(BF16)
        left = jnp.concatenate([top, low, top], axis=1)
        right = jnp.concatenate([top, top, low], axis=1)
        m = lax.dot_general(left, right, (((1,), (1,)), ((), ())), preferred_element_type=F32)
        q = q_ref[:, 0:GROUP] - m
        rows = pl.ds(pl.multiple_of(f * GROUP, 8), GROUP)
        w_ref[rows, :] = jnp.dot(q, b_ref[rows, :], precision=HIGHEST, preferred_element_type=F32)
        for c in range(6):
            for h in range(2):
                at = pl.ds(pl.multiple_of(f * GROUP + c * SLOTS + 8 * h, 8), 8)
                w_ref[at, 0:LANES] = jnp.where(
                    lane == LANES - 1, jnp.broadcast_to(cols[(c, h)], (8, LANES)), w_ref[at, 0:LANES]
                )
        return carry

    lax.fori_loop(0, 8, functools.partial(frame, merged=0), 0)
    lax.fori_loop(8, 16, functools.partial(frame, merged=1), 0)
    t = jnp.dot(bt_ref[...], w_ref[...], precision=HIGHEST, preferred_element_type=F32)
    t_ref[...] = t
    for lo, hi, group, first in ((0, 48, 0, 48), (48, 144, 1, 0), (144, 192, 2, 0)):
        count = hi - lo
        lanes = slice(group * LANES, (group + 1) * LANES)
        square = jnp.concatenate(
            [jnp.zeros((first, LANES), F32)] * (first > 0)
            + [t[lo:hi, lanes], jnp.zeros((LANES - first - count, LANES), F32)],
            axis=0,
        )
        mean = 0.5 * (square + square.T)
        t_ref[lo:hi, lanes] = mean[first : first + count]
    last = iota((48, LANES), 1) == LANES - 1

    def half(core):
        own = slice(48 + 48 * core, 96 + 48 * core)
        rim = slice(0, 48) if core else slice(144, 192)
        group = 0 if core else 2
        mine = jnp.where(last, t[own, 0:LANES], t_ref[own, LANES : 2 * LANES])
        theirs = jnp.where(last, t[rim, 0:LANES], t_ref[rim, group * LANES : (group + 1) * LANES])
        far = t_ref[rim, LANES : 2 * LANES] if core else jnp.zeros((48, LANES), F32)
        return mine, t_ref[own, 2 * LANES :], theirs, far

    def put_half(ref, core):
        for k, x in enumerate(half(core)):
            ref[(k // 2) * 48 : (k // 2 + 1) * 48, (k % 2) * LANES : (k % 2 + 1) * LANES] = x

    @pl.when(core == 0)
    def _():
        put_half(keep_ref, 0)
        put_half(send_ref, 1)

    @pl.when(core == 1)
    def _():
        put_half(keep_ref, 1)
        put_half(send_ref, 0)


def to_row(column):
    return jnp.sum(
        jnp.where(iota((GROUP, LANES), 0) == iota((GROUP, LANES), 1), column, 0.0),
        axis=0,
        keepdims=True,
    )


BLOCKS = 12


def quad_kernel(where_ref, own_ref, own2_ref, rim_ref, rim2_ref, out_ref):
    out_ref[...] = (own_ref[...] + own2_ref[...]) + (rim_ref[...] + rim2_ref[...])


def place_kernel(where_ref, a_ref, b_ref, c_ref, d_ref, out_ref):
    at = where_ref[3]
    for k, ref in enumerate((a_ref, b_ref, c_ref, d_ref)):
        out_ref[pl.ds(pl.multiple_of(48 * (at ^ k), 8), 48), :] = ref[...]


SHRINK = 2.0**-15
FIRST = 2.0**-10
LARGEST_STEP = 1.001 / (POSE_REG * SHRINK)


def halves(x):
    t = 4097.0 * x
    top = t - (t - x)
    return top, x - top


def times(a, b):
    p = a * b
    ah, al = halves(a)
    bh, bl = halves(b)
    return p, ((ah * bh - p) + ah * bl + al * bh) + al * bl


def plus(a, b):
    t = a[0] + b[0]
    back = t - a[0]
    return t, (a[1] + b[1]) + ((a[0] - (t - back)) + (b[0] - back))


def tidy(a):
    t = a[0] + a[1]
    return t, a[1] - (t - a[0])


def mul(a, b):
    p, e = times(a[0], b[0])
    return tidy((p, e + (a[0] * b[1] + a[1] * b[0])))


def add(a, b):
    return tidy(plus(a, b))


def neg(a):
    return -a[0], -a[1]


def div(a, b):
    q = a[0] / b[0]
    rest = add(a, neg(mul((q, jnp.zeros_like(q)), b)))
    return tidy((q, rest[0] / b[0]))


def lane_total(a):
    for step in (64, 32, 16, 8, 4, 2, 1):
        a = plus(a, (pltpu.roll(a[0], step, 1), pltpu.roll(a[1], step, 1)))
    return a


def to_column(row):
    eye = iota((GROUP, LANES), 0) == iota((GROUP, LANES), 1)
    return jnp.broadcast_to(
        jnp.sum(jnp.where(eye, row, 0.0), axis=1, keepdims=True), (GROUP, LANES)
    )


def block_at(j):
    return pl.ds(pl.multiple_of(j * GROUP, 8), GROUP)


def tile_at(j):
    return pl.ds(pl.multiple_of(j * 8, 8), 8)


def product(s_ref, up_ref, high_ref, low_ref, j):
    acc = None
    sources = (
        (s_ref[block_at(j), 0:LANES], j),
        (s_ref[block_at(j - 1), LANES : 2 * LANES], j - 1),
        (up_ref[block_at(j), :], j + 1),
    )
    for s, at in sources:
        high = high_ref[block_at(at), :]
        p, e = times(s, high)
        e = e + s * low_ref[block_at(at), :]
        for r in range(0, GROUP, 8):
            term = p[r : r + 8], e[r : r + 8]
            acc = term if acc is None else plus(acc, term)
    for step in (4, 2, 1):
        acc = plus(acc, (pltpu.roll(acc[0], step, 0), pltpu.roll(acc[1], step, 0)))
    acc = tidy(acc)
    return acc[0] * SHRINK, acc[1] * SHRINK


def store_tile(ref, at, pair):
    row = iota((8, LANES), 0)
    ref[tile_at(at), :] = jnp.where(row == 0, pair[0], jnp.where(row == 1, pair[1], 0.0))


def powers(s_ref, up_ref, v_ref, cols, first, count, edge, base):
    for k in range(count):
        here, there = cols[k % 2], cols[1 - k % 2]

        def one(j, carry):
            pair = product(s_ref, up_ref, here[0], here[1], j)
            store_tile(v_ref, (first + k) * BLOCKS + j, pair)
            there[0][block_at(j), :] = to_column(pair[0][0:1])
            there[1][block_at(j), :] = to_column(pair[1][0:1])
            return carry

        lax.fori_loop(base + k * edge, BLOCKS - base - k * edge, one, 0)


def first_kernel(
    where_ref, p_ref, c_ref, n_ref, p2_ref, c2_ref, n2_ref,
    s_ref, up_ref, v_ref, v4_ref, h0_ref, l0_ref, h1_ref, l1_ref,
):
    core = where_ref[2]
    mine = pl.multiple_of(48 * core, 8)
    theirs = pl.multiple_of(48 - 48 * core, 8)
    diagonal = iota((GROUP, LANES), 0) == iota((GROUP, LANES), 1)
    lane = iota((GROUP, LANES), 1)
    for j in range(BLOCKS):
        rows = slice((j % 4) * 48, (j % 4 + 1) * 48)
        a = (p_ref, c_ref, n_ref)[j // 4]
        b = (p2_ref, c2_ref, n2_ref)[j // 4]
        s_ref[pl.ds(j * GROUP + mine, 48), :] = a[rows, :]
        s_ref[pl.ds(j * GROUP + theirs, 48), :] = b[rows, :]
    zero = jnp.zeros((LANES - GROUP, LANES), F32)

    def prepare(j, carry):
        own = s_ref[block_at(j), 0:LANES]
        rhs = jnp.broadcast_to(own[:, LANES - 1 : LANES], (GROUP, LANES)) * FIRST
        h0_ref[block_at(j), :] = rhs
        l0_ref[block_at(j), :] = jnp.zeros_like(rhs)
        store_tile(v_ref, j, (to_row(rhs), jnp.zeros((1, LANES), F32)))
        s_ref[block_at(j), 0:LANES] = jnp.where(lane < GROUP, own, 0.0) + jnp.where(
            diagonal, POSE_REG, 0.0
        )
        up = jnp.concatenate([s_ref[block_at(j), LANES : 2 * LANES], zero], axis=0).T
        up_ref[block_at(j), :] = up[0:GROUP]
        return carry

    lax.fori_loop(0, BLOCKS, prepare, 0)
    cols = ((h0_ref, l0_ref), (h1_ref, l1_ref))
    powers(s_ref, up_ref, v_ref, cols, 1, 4, 1, 1)
    for j in range(4):
        at = (4 * BLOCKS + 4 + j) * 8
        v4_ref[j : j + 1, :] = v_ref[at : at + 1, :]
        v4_ref[4 + j : 5 + j, :] = v_ref[at + 1 : at + 2, :]


def second_kernel(
    s_ref, up_ref, v_ref, below_ref, own_ref, above_ref, out_ref, v45_ref,
    h0_ref, l0_ref, h1_ref, l1_ref,
):
    for g, ref in enumerate((below_ref, own_ref, above_ref)):
        for j in range(4):
            pair = ref[j : j + 1, :], ref[4 + j : 5 + j, :]
            at = g * 4 + j
            store_tile(v45_ref, at, pair)
            if 1 < at < 10:
                h0_ref[block_at(at), :] = to_column(pair[0])
                l0_ref[block_at(at), :] = to_column(pair[1])
    cols = ((h0_ref, l0_ref), (h1_ref, l1_ref))
    powers(s_ref, up_ref, v45_ref, cols, 1, 2, 1, 3)
    zero = jnp.zeros((1, LANES), F32)
    total = None
    for j in range(4, 8):

        def row(k, part):
            ref, at = (v_ref, k) if k < 4 else (v45_ref, k - 4)
            at = (at * BLOCKS + j) * 8 + part
            return ref[at : at + 1, :]

        def stack(pick, part):
            lines = [row(pick(m), part) for m in range(2 * ITERS)]
            return jnp.concatenate(lines + [zero] * (16 - len(lines)), axis=0)

        lower, upper = (lambda m: m // 2), (lambda m: m - m // 2)
        a, b = (stack(lower, 0), stack(lower, 1)), (stack(upper, 0), stack(upper, 1))
        p, e = times(a[0], b[0])
        term = p, e + (a[0] * b[1] + a[1] * b[0])
        total = term if total is None else plus(total, term)
    total = tidy(lane_total(total))
    diagonal = iota((16, LANES), 0) == iota((16, LANES), 1)
    put(
        out_ref,
        [jnp.sum(jnp.where(diagonal, x, 0.0), axis=0, keepdims=True) for x in total],
    )


def put(ref, pair):
    ref[...] = jnp.zeros((8, LANES), F32)
    ref[0:1, :] = pair[0]
    ref[1:2, :] = pair[1]


def gather_sum(refs):
    acc = refs[0][0:1, :], refs[0][1:2, :]
    for r in refs[1:]:
        acc = plus(acc, (r[0:1, :], r[1:2, :]))
    return tidy(acc)


def sum_kernel(a_ref, b_ref, c_ref, d_ref, out_ref):
    put(out_ref, gather_sum((a_ref, b_ref, c_ref, d_ref)))


def solve_kernel(where_ref, a_ref, b_ref, c_ref, d_ref, v_ref, v45_ref, out_ref):
    at_quad = where_ref[3]
    total = gather_sum((a_ref, b_ref, c_ref, d_ref))
    m = [(total[0][:, k : k + 1], total[1][:, k : k + 1]) for k in range(2 * ITERS)]
    one = jnp.ones((1, 1), F32)
    zero = jnp.zeros((1, 1), F32)
    none = (zero, zero)

    def where(live, a, b):
        return jnp.where(live, a[0], b[0]), jnp.where(live, a[1], b[1])

    sigma = list(m)
    tau = list(m)
    rc = [(one, zero)] + [none] * ITERS
    pc = list(rc)
    xc = [none] * ITERS
    lead = one
    live = m[0][0] > 0.0
    for k in range(ITERS):
        alpha = div(sigma[k], where(live, tau[k + 1], (one, zero)))
        live = live & (alpha[0] > 0.0) & (alpha[0] < LARGEST_STEP)
        alpha = where(live, alpha, none)
        for i in range(k + 1):
            xc[i] = add(xc[i], mul(alpha, pc[i]))
        if k + 1 == ITERS:
            break
        back = neg(alpha)
        fresh = {i: add(sigma[i], mul(back, tau[i + 1])) for i in range(k + 1, 2 * ITERS - k - 1)}
        for i in range(k + 1, 0, -1):
            rc[i] = add(rc[i], mul(back, pc[i - 1]))
        lead = -lead * alpha[0]
        live = live & (lead * fresh[k + 1][0] > 1e-11 * m[0][0])
        beta = div(mul(back, fresh[k + 1]), where(live, sigma[k], (one, zero)))
        beta = where(live, beta, none)
        for i, x in fresh.items():
            tau[i] = add(x, mul(beta, tau[i]))
            sigma[i] = x
        pc = [add(rc[i], mul(beta, pc[i])) for i in range(k + 2)] + [none] * (ITERS - k - 1)
    for g in range(3):
        acc = None
        for k in range(ITERS):
            ref = v_ref if k < 4 else v45_ref
            tile = ref[tile_at((k if k < 4 else k - 4) * BLOCKS + 3 + at_quad + g), :]
            wide = tuple(jnp.broadcast_to(x, (1, LANES)) for x in xc[k])
            term = mul(wide, (tile[0:1], tile[1:2]))
            acc = term if acc is None else plus(acc, term)
        out_ref[g * 8 : g * 8 + 8, :] = jnp.broadcast_to(
            (acc[0] + acc[1]) * (SHRINK / FIRST), (8, LANES)
        )


def final_kernel(pose_ref, b_ref, g_ref, base_ref, scale_ref, out_ref, sum_ref):
    x0 = pose_ref[0:1, :]
    x1 = pose_ref[8:9, :]
    x2 = pose_ref[16:17, :]

    def frame(f, carry):
        rows = pl.ds(pl.multiple_of(f * GROUP, 8), GROUP)
        prod = (
            b_ref[rows, 0:LANES] * x0
            + b_ref[rows, LANES : 2 * LANES] * x1
            + b_ref[rows, 2 * LANES : 3 * LANES] * x2
        )
        x = jnp.sum(prod, axis=1, keepdims=True)
        image = jnp.sum(g_ref[rows, :] * x, axis=0, keepdims=True)
        at = pl.ds(pl.multiple_of(f * 8, 8), 8)
        sum_ref[at, :] = base_ref[at, :] - scale_ref[at, :] * image
        return carry

    lax.fori_loop(0, FD, frame, 0)
    for f in range(FD):
        out_ref[f : f + 1, :] = sum_ref[f * 8 : f * 8 + 1, :]


SMEM = pl.BlockSpec(memory_space=pltpu.SMEM)
VMEM = pl.BlockSpec(memory_space=pltpu.VMEM)


def call(kernel, name, outs, smem, *args, scratch=()):
    return pl.pallas_call(
        kernel,
        name=name,
        out_shape=[jax.ShapeDtypeStruct(s, F32) for s in outs],
        in_specs=[SMEM] * smem + [VMEM] * (len(args) - smem),
        out_specs=[VMEM] * len(outs),
        scratch_shapes=list(scratch),
    )(*args)


def per_device(edge_frames, rotvec, trans, inv_depth, depth_damping, flow, weight, mask):
    f_dev, plocal = inv_depth.shape
    edges = mask.shape[0]
    count = lax.axis_size("frames")
    pixes = lax.axis_size("pix")
    fi = lax.axis_index("frames")
    pi = lax.axis_index("pix")
    spot = jnp.stack([fi * f_dev, pi * plocal, pi % 2, fi % 4]).astype(jnp.int32)

    def shift(block, step):
        return lax.ppermute(
            block, "frames", [(i, i + step) for i in range(count) if 0 <= i + step < count]
        )

    def view(x):
        return x.reshape(edges, 2, plocal // LANES, LANES).transpose(0, 2, 1, 3).reshape(-1, LANES)

    own, down, up = call(
        scatter_kernel, "scatter",
        [(4 * f_dev * SLOTS, plocal), (8 + 4 * SIDE, plocal), (4 * SIDE, plocal)],
        1, spot, edge_frames, view(flow), view(weight), mask,
    )
    from_after = shift(down, -1)
    from_before = shift(up, 1)
    tab, b, bt = call(
        pose_kernel, "pose",
        [(f_dev * SLOTS, LANES), (f_dev * GROUP, 3 * LANES), (192, f_dev * GROUP)],
        1, spot, rotvec, trans,
    )
    keep, send, g, base, scale = call(
        main_kernel, "main",
        [(96, 256), (96, 256), (f_dev * GROUP, plocal), (f_dev * 8, plocal), (f_dev * 8, plocal)],
        1, spot, own, from_after, from_before, inv_depth, depth_damping, tab, b, bt,
        scratch=[
            pltpu.VMEM((4 * FD * 8, plocal), F32),
            pltpu.VMEM((7 * 16, plocal), F32),
            pltpu.VMEM((GROUP, plocal), F32),
            pltpu.VMEM((256, plocal), F32),
            pltpu.VMEM((GROUP, LANES), F32),
            pltpu.VMEM((f_dev * GROUP, 3 * LANES), F32),
            pltpu.VMEM((192, 3 * LANES), F32),
        ],
    )
    got = lax.ppermute(send, "pix", [(i, i ^ 1) for i in range(pixes)])
    both = keep + got
    own_half, rim = both[:48], both[48:]
    both_axes = ("frames", "pix")

    def to_neighbour(flip):
        route = []
        for i in range(count):
            for k in range(pixes):
                to = i + 1 if k % 2 == 0 else i - 1
                if 0 <= to < count:
                    route.append((i * pixes + k, to * pixes + (k ^ flip)))
        return lax.ppermute(rim, both_axes, route)

    own_far = lax.ppermute(own_half, "pix", [(i, i ^ 2) for i in range(pixes)])
    rim_near = to_neighbour(0)
    rim_far = to_neighbour(2)
    (half,) = call(quad_kernel, "half", [(48, 256)], 1, spot, own_half, own_far, rim_near, rim_far)

    def mates(v, step):
        return [v] + [
            lax.ppermute(v, "frames", [(i, i ^ (k * step)) for i in range(count)]) for k in (1, 2, 3)
        ]

    def twin(v):
        return lax.ppermute(v, "pix", [(i, i ^ 1) for i in range(pixes)])

    def halo(v):
        return shift(v, 4), v, shift(v, -4)

    (quad,) = call(place_kernel, "place", [(192, 256)], 1, spot, *mates(half, 1))
    pieces = halo(quad)
    wide = BLOCKS * GROUP
    scratch = [pltpu.VMEM((wide, LANES), F32)] * 4
    s, up, vs, v4 = call(
        first_kernel, "first",
        [(wide, 256), (wide, LANES), (5 * BLOCKS * 8, LANES), (8, LANES)],
        1, spot, *pieces, *[twin(x) for x in pieces], scratch=scratch,
    )
    part, v45 = call(
        second_kernel, "second", [(8, LANES), (3 * BLOCKS * 8, LANES)], 0, s, up, vs, *halo(v4),
        scratch=scratch,
    )
    (part,) = call(sum_kernel, "sum", [(8, LANES)], 0, *mates(part, 4))
    (pose,) = call(solve_kernel, "solve", [(24, LANES)], 1, spot, *mates(part, 16), vs, v45)
    (depth_step,) = call(
        final_kernel, "final", [(f_dev, plocal)], 0, pose, b, g, base, scale,
        scratch=[pltpu.VMEM((f_dev * 8, plocal), F32)],
    )
    pose_step = pose[8, : f_dev * 6].reshape(f_dev, 6).T
    return pose_step, depth_step


def solution(mesh):
    return jax.shard_map(
        per_device,
        mesh=mesh,
        in_specs=(
            P(None, "frames"),
            P(),
            P(),
            P("frames", "pix"),
            P("frames", "pix"),
            P("frames", None, "pix"),
            P("frames", None, "pix"),
            P("frames", "pix"),
        ),
        out_specs=(P(None, "frames"), P("frames", "pix")),
        check_vma=False,
    )
```

```python
import functools
import jax
import jax.numpy as jnp
from jax import lax
from jax.experimental import pallas as pl
from jax.experimental.pallas import tpu as pltpu
from jax.sharding import PartitionSpec as P

ROWS = 48
COLS = 64
RADIUS = 8
ITERS = 6
HIGHEST = lax.Precision.HIGHEST
F32 = jnp.float32
BF16 = jnp.bfloat16
LANES = 128
FD = 16
SLOTS = 16
GROUP = FD * 6
SIDE = RADIUS * (RADIUS + 1) // 2
POSE_REG = 100.0


def iota(shape, dim):
    return lax.broadcasted_iota(jnp.int32, shape, dim)


def thirds(x):
    first = x.astype(BF16)
    rest = x - first.astype(F32)
    second = rest.astype(BF16)
    return first, second, (rest - second.astype(F32)).astype(BF16)


def pair_of(x):
    first = x.astype(BF16)
    return first, (x - first.astype(F32)).astype(BF16)


def dot(a, b):
    return jnp.dot(a, b, preferred_element_type=F32)


def scatter_kernel(where_ref, ef_ref, flow_ref, weight_ref, mask_ref, own_ref, down_ref, up_ref):
    edges = ef_ref.shape[1]
    start = where_ref[0]
    source = ef_ref[0:1, :] - start
    delta = ef_ref[1:2, :] - start - source
    slot = jnp.where(delta < 0, delta + 8, delta + 7)
    own_at = jnp.where((source >= 0) & (source < FD), source * SLOTS + slot, -1)
    j = source + 8
    down_at = jnp.where(source < 0, ((j * (j + 1)) >> 1) + delta - 8 + j, -1)
    j = 23 - source
    up_at = jnp.where(source >= FD, ((j * (j + 1)) >> 1) + slot, -1)
    hot = jnp.concatenate(
        [
            (iota((FD * SLOTS, edges), 0) == own_at).astype(F32),
            (iota((40, edges), 0) == down_at).astype(F32),
            (iota((40, edges), 0) == up_at).astype(F32),
        ],
        axis=0,
    ).astype(BF16)
    down_ref[0:8, :] = jnp.zeros((8, down_ref.shape[1]), F32)
    for chunk in range(mask_ref.shape[1] // LANES):
        lanes = pl.ds(chunk * LANES, LANES)
        live = mask_ref[:, lanes].astype(F32)
        parts = []
        for comp in range(2):
            conf = weight_ref[comp, :, lanes] * live
            parts.append((conf, conf * flow_ref[comp, :, lanes]))
        values = jnp.concatenate([parts[0][0], parts[1][0], parts[0][1], parts[1][1]], axis=1)
        got = sum(
            jnp.dot(hot, piece, preferred_element_type=F32) for piece in reversed(thirds(values))
        )
        for q in range(4):
            cut = got[:, q * LANES : (q + 1) * LANES]
            own_ref[q * 256 : (q + 1) * 256, lanes] = cut[0:256]
            down_ref[8 + q * SIDE : 8 + (q + 1) * SIDE, lanes] = cut[256 : 256 + SIDE]
            up_ref[q * SIDE : (q + 1) * SIDE, lanes] = cut[296 : 296 + SIDE]


def rotation_rows(w):
    x, y, z = w
    zero = jnp.zeros_like(x)
    cross = [[zero, -z, y], [z, zero, -x], [-y, x, zero]]
    sq = x * x + y * y + z * z
    first = 1.0 - sq / 6.0 + sq * sq / 120.0
    second = 0.5 - sq / 24.0 + sq * sq / 720.0
    return [
        [
            float(i == k)
            + first * cross[i][k]
            + second * sum(cross[i][m] * cross[m][k] for m in range(3))
            for k in range(3)
        ]
        for i in range(3)
    ]


def pose_kernel(where_ref, rotvec_ref, trans_ref, tab_ref, b_ref, bt_ref):
    start = where_ref[0]
    frames = rotvec_ref.shape[1]
    pair = iota((1, FD * SLOTS), 1)
    slot = pair & 15
    delta = jnp.where(slot < 8, slot - 8, slot - 7)
    at_source = start + (pair >> 4)
    at_target = jnp.clip(at_source + delta, 0, frames - 1)
    poses = jnp.concatenate([rotvec_ref[...], trans_ref[...], jnp.zeros((2, frames), F32)], axis=0)

    def pick(at):
        hot = (iota((frames, FD * SLOTS), 0) == at).astype(F32)
        return jnp.dot(poses, hot, precision=HIGHEST, preferred_element_type=F32)

    src = pick(at_source)
    tgt = pick(at_target)
    rs = rotation_rows([src[k : k + 1] for k in range(3)])
    rt = rotation_rows([tgt[k : k + 1] for k in range(3)])
    rel = [[sum(rt[i][k] * rs[m][k] for k in range(3)) for m in range(3)] for i in range(3)]
    tr = [
        tgt[3 + i : 4 + i] - sum(rel[i][m] * src[3 + m : 4 + m] for m in range(3)) for i in range(3)
    ]
    corner = [
        [tr[1] * rel[2][m] - tr[2] * rel[1][m] for m in range(3)],
        [tr[2] * rel[0][m] - tr[0] * rel[2][m] for m in range(3)],
        [tr[0] * rel[1][m] - tr[1] * rel[0][m] for m in range(3)],
    ]
    lines = [x for row in rel for x in row] + tr + [x for row in corner for x in row]
    lines = jnp.concatenate(lines + [jnp.zeros((LANES - len(lines), FD * SLOTS), F32)], axis=0)
    tab_ref[...] = lines.T

    lane3 = iota((SLOTS, 3 * LANES), 1)
    row3 = iota((SLOTS, 3 * LANES), 0)
    off3 = jnp.where(row3 < 8, row3 - 8, row3 - 7)

    def build(f, carry):
        frame = f + off3 + FD
        home = (frame >> 4) * LANES + (frame & 15) * 6
        tab = tab_ref[pl.ds(pl.multiple_of(f * SLOTS, SLOTS), SLOTS), :]
        for c in range(6):
            block = jnp.where(lane3 == home + c, 1.0, 0.0)
            for d in range(6):
                if c < 3:
                    at = c * 3 + d if d < 3 else 12 + c * 3 + d - 3
                elif d >= 3:
                    at = (c - 3) * 3 + d - 3
                else:
                    continue
                block = block - jnp.where(
                    lane3 == LANES + f * 6 + d, jnp.broadcast_to(tab[:, at : at + 1], lane3.shape), 0.0
                )
            b_ref[pl.ds(pl.multiple_of(f * GROUP + c * SLOTS, SLOTS), SLOTS), :] = block
        return carry

    lax.fori_loop(0, FD, build, 0)
    for g in range(4):
        cols = slice(g * 384, (g + 1) * 384)
        below = b_ref[cols, 0:LANES].T
        own = b_ref[cols, LANES : 2 * LANES].T
        above = b_ref[cols, 2 * LANES : 3 * LANES].T
        bt_ref[0:48, cols] = below[48:96]
        bt_ref[48:144, cols] = own[0:96]
        bt_ref[144:192, cols] = above[0:48]


def main_kernel(
    where_ref, own_ref, rdown_ref, rup_ref, depth_ref, damp_ref, tab_ref, b_ref, bt_ref,
    keep_ref, send_ref, g_ref, base_ref, scale_ref,
    half_ref, geo_ref, hi_ref, in_ref, q_ref, w_ref, t_ref,
):
    core = where_ref[2]
    plocal = depth_ref.shape[1]
    chunks = plocal // LANES
    row8 = iota((8, plocal), 0)
    for f in range(FD):
        j = 7 - f if f < 8 else f - 8
        base = j * (j + 1) // 2
        for q in range(4):
            if f < 8:
                extra = jnp.where(row8 <= j, rup_ref[q * SIDE + base : q * SIDE + base + 8, :], 0.0)
                at = q * 256 + f * SLOTS
            else:
                first = 8 + q * SIDE + base - 7 + j
                extra = jnp.where(row8 >= 7 - j, rdown_ref[first : first + 8, :], 0.0)
                at = q * 256 + f * SLOTS + 8
            half_ref[(q * FD + f) * 8 : (q * FD + f + 1) * 8, :] = own_ref[at : at + 8, :] + extra
        in_ref[f * 8 : f * 8 + 8, :] = jnp.broadcast_to(depth_ref[f : f + 1, :], (8, plocal))
        in_ref[128 + f * 8 : 136 + f * 8, :] = jnp.broadcast_to(damp_ref[f : f + 1, :], (8, plocal))
    lane = iota((8, LANES), 1)
    row = iota((8, LANES), 0)

    def frame(f, carry, merged):
        eight = pl.ds(pl.multiple_of(f * 8, 8), 8)
        def conf(q, h, lanes):
            if h == merged:
                at = (q * FD + f) * 8
                return half_ref[pl.ds(pl.multiple_of(at, 8), 8), lanes]
            at = q * 256 + f * SLOTS + 8 * h
            return own_ref[pl.ds(pl.multiple_of(at, 8), 8), lanes]

        params = []
        for h in range(2):
            tab = tab_ref[pl.ds(pl.multiple_of(f * SLOTS + 8 * h, 8), 8), :]
            params.append([jnp.broadcast_to(tab[:, k : k + 1], (8, LANES)) for k in range(12)])
        base_all = []
        scale_all = []
        for c in range(chunks):
            lanes = pl.ds(c * LANES, LANES)
            pixel = where_ref[1] + c * LANES + lane
            col = ((pixel & (COLS - 1)).astype(F32) - 0.5 * (COLS - 1)) / COLS
            line = ((pixel >> 6).astype(F32) - 0.5 * (ROWS - 1)) / COLS
            depth = in_ref[eight, lanes]
            curv = 0.0
            grad = 0.0
            for h in range(2):
                r = params[h]
                z = r[6] * col + r[7] * line + r[8] + depth * r[11]
                inv = 1.0 / z
                u = (r[0] * col + r[1] * line + r[2] + depth * r[9]) * inv
                v = (r[3] * col + r[4] * line + r[5] + depth * r[10]) * inv
                s = depth * inv
                su = inv * (r[9] - u * r[11])
                sv = inv * (r[10] - v * r[11])
                cu = conf(0, h, lanes)
                cv = conf(1, h, lanes)
                eu = cu * (col - u) + conf(2, h, lanes)
                ev = cv * (line - v) + conf(3, h, lanes)
                au = cu * su
                av = cv * sv
                curv = curv + au * su + av * sv
                grad = grad - (su * eu + sv * ev)
                for k, x in enumerate((u, v, s, au, av, eu, ev)):
                    geo_ref[k * 16 + 8 * h : k * 16 + 8 * h + 8, lanes] = x
            damp = in_ref[pl.ds(pl.multiple_of(128 + f * 8, 8), 8), lanes]
            total = damp + jnp.sum(curv, axis=0, keepdims=True)
            base = jnp.sum(grad, axis=0, keepdims=True) / total
            scale = 1.0 / jnp.sqrt(total)
            base_ref[eight, lanes] = base
            scale_ref[eight, lanes] = scale
            base_all.append(base)
            scale_all.append(scale)
        cols = {}
        for h in range(2):
            acc = [0.0] * 27
            for c in range(chunks):
                lanes = pl.ds(c * LANES, LANES)
                u, v, s, au, av, eu, ev = [
                    geo_ref[k * 16 + 8 * h : k * 16 + 8 * h + 8, lanes] for k in range(7)
                ]
                cu = conf(0, h, lanes)
                cv = conf(1, h, lanes)
                base = base_all[c]
                scale = scale_all[c]
                hu = -eu - au * base
                hv = -ev - av * base
                uv = u * v
                u1 = 1.0 + u * u
                v1 = 1.0 + v * v

                def pull(pu, pv):
                    spu = s * pu
                    spv = s * pv
                    return (
                        spu,
                        spv,
                        -(u * spu + v * spv),
                        -(uv * pu) - v1 * pv,
                        u1 * pu + uv * pv,
                        u * pv - v * pu,
                    )

                for k, x in enumerate(pull(au * scale, av * scale)):
                    at = pl.ds(pl.multiple_of(f * GROUP + k * SLOTS + 8 * h, 8), 8)
                    g_ref[at, lanes] = x
                    hi_ref[k * SLOTS + 8 * h : k * SLOTS + 8 * h + 8, lanes] = x
                su_ = cu * s
                sv_ = cv * s
                ju = (None, None, None, -uv, u1, -v)
                jv = (None, None, None, -v1, uv, u)
                terms = list(pull(hu, hv))
                a00 = su_ * s
                a11 = sv_ * s
                a02 = -(a00 * u)
                a12 = -(a11 * v)
                a22 = -(a02 * u + a12 * v)
                terms += [a00, a11, a02, a12, a22]
                tu = [su_ * ju[k] for k in (3, 4, 5)]
                tv = [sv_ * jv[k] for k in (3, 4, 5)]
                terms += tu + tv
                terms += [-(u * tu[k] + v * tv[k]) for k in range(3)]
                wu = [cu * ju[k] for k in (3, 4, 5)]
                wv = [cv * jv[k] for k in (3, 4, 5)]
                for a in range(3):
                    for b in range(a, 3):
                        terms.append(wu[a] * ju[3 + b] + wv[a] * jv[3 + b])
                acc = [x + y for x, y in zip(acc, terms)]
            assert len(acc) == len(terms)
            sums = [jnp.sum(x, axis=1, keepdims=True) for x in acc]
            a = {(0, 0): sums[6], (1, 1): sums[7], (0, 2): sums[8], (1, 2): sums[9], (2, 2): sums[10]}
            for k in range(3):
                a[(0, 3 + k)] = sums[11 + k]
                a[(1, 3 + k)] = sums[14 + k]
                a[(2, 3 + k)] = sums[17 + k]
            at = 20
            for x in range(3):
                for y in range(x, 3):
                    a[(3 + x, 3 + y)] = sums[at]
                    at += 1
            for c in range(6):
                block = jnp.zeros((8, LANES), F32)
                for d in range(6):
                    key = (min(c, d), max(c, d))
                    if key == (0, 1):
                        continue
                    block = jnp.where(
                        lane == d * SLOTS + 8 * h + row, jnp.broadcast_to(a[key], (8, LANES)), block
                    )
                q_ref[c * SLOTS + 8 * h : c * SLOTS + 8 * h + 8, :] = block
                cols[(c, h)] = sums[c]
        g = hi_ref[...]
        top, low = pair_of(g)
        both = lax.dot_general(
            jnp.concatenate([top, low], axis=0), top, (((1,), (1,)), ((), ())),
            preferred_element_type=F32,
        )
        m = both[0:GROUP] + both[GROUP:] + both[GROUP:].T
        q = q_ref[:, 0:GROUP] - m
        rows = pl.ds(pl.multiple_of(f * GROUP, 8), GROUP)
        q_top, q_low = pair_of(q)
        b_top, b_low = pair_of(b_ref[rows, :])
        both = dot(jnp.concatenate([q_top, q_low], axis=0), b_top)
        w_ref[rows, :] = both[0:GROUP] + both[GROUP:]
        own_group = slice(LANES, 2 * LANES)
        w_ref[rows, own_group] = w_ref[rows, own_group] + dot(q_top, b_low[:, own_group])
        for c in range(6):
            for h in range(2):
                at = pl.ds(pl.multiple_of(f * GROUP + c * SLOTS + 8 * h, 8), 8)
                w_ref[at, 0:LANES] = jnp.where(
                    lane == LANES - 1, jnp.broadcast_to(cols[(c, h)], (8, LANES)), w_ref[at, 0:LANES]
                )
        return carry

    lax.fori_loop(0, 8, functools.partial(frame, merged=0), 0)
    lax.fori_loop(8, 16, functools.partial(frame, merged=1), 0)
    bt_top, bt_low = pair_of(bt_ref[...])
    w_top, w_low = pair_of(w_ref[...])
    both = dot(jnp.concatenate([bt_top, bt_low], axis=0), w_top)
    t = both[0:192] + both[192:] + dot(bt_top, w_low)
    t_ref[...] = t
    for lo, hi, group, first in ((0, 48, 0, 48), (48, 144, 1, 0), (144, 192, 2, 0)):
        count = hi - lo
        lanes = slice(group * LANES, (group + 1) * LANES)
        square = jnp.concatenate(
            [jnp.zeros((first, LANES), F32)] * (first > 0)
            + [t[lo:hi, lanes], jnp.zeros((LANES - first - count, LANES), F32)],
            axis=0,
        )
        mean = 0.5 * (square + square.T)
        t_ref[lo:hi, lanes] = mean[first : first + count]
    last = iota((48, LANES), 1) == LANES - 1

    def half(core):
        own = slice(48 + 48 * core, 96 + 48 * core)
        rim = slice(0, 48) if core else slice(144, 192)
        group = 0 if core else 2
        mine = jnp.where(last, t[own, 0:LANES], t_ref[own, LANES : 2 * LANES])
        theirs = jnp.where(last, t[rim, 0:LANES], t_ref[rim, group * LANES : (group + 1) * LANES])
        far = t_ref[rim, LANES : 2 * LANES] if core else jnp.zeros((48, LANES), F32)
        return mine, t_ref[own, 2 * LANES :], theirs, far

    def put_half(ref, core):
        for k, x in enumerate(half(core)):
            ref[(k // 2) * 48 : (k // 2 + 1) * 48, (k % 2) * LANES : (k % 2 + 1) * LANES] = x

    @pl.when(core == 0)
    def _():
        put_half(keep_ref, 0)
        put_half(send_ref, 1)

    @pl.when(core == 1)
    def _():
        put_half(keep_ref, 1)
        put_half(send_ref, 0)


def to_row(column):
    return jnp.sum(
        jnp.where(iota((GROUP, LANES), 0) == iota((GROUP, LANES), 1), column, 0.0),
        axis=0,
        keepdims=True,
    )


BLOCKS = 12


def quad_kernel(where_ref, own_ref, own2_ref, rim_ref, rim2_ref, out_ref):
    out_ref[...] = (own_ref[...] + own2_ref[...]) + (rim_ref[...] + rim2_ref[...])


def place_kernel(where_ref, a_ref, b_ref, c_ref, d_ref, out_ref):
    at = where_ref[3]
    for k, ref in enumerate((a_ref, b_ref, c_ref, d_ref)):
        out_ref[pl.ds(pl.multiple_of(48 * (at ^ k), 8), 48), :] = ref[...]


SHRINK = 2.0**-15
FIRST = 2.0**-10
LARGEST_STEP = 1.001 / (POSE_REG * SHRINK)


def halves(x):
    t = 4097.0 * x
    top = t - (t - x)
    return top, x - top


def times(a, b):
    p = a * b
    ah, al = halves(a)
    bh, bl = halves(b)
    return p, ((ah * bh - p) + ah * bl + al * bh) + al * bl


def plus(a, b):
    t = a[0] + b[0]
    back = t - a[0]
    return t, (a[1] + b[1]) + ((a[0] - (t - back)) + (b[0] - back))


def tidy(a):
    t = a[0] + a[1]
    return t, a[1] - (t - a[0])


def mul(a, b):
    p, e = times(a[0], b[0])
    return tidy((p, e + (a[0] * b[1] + a[1] * b[0])))


def add(a, b):
    return tidy(plus(a, b))


def neg(a):
    return -a[0], -a[1]


def div(a, b):
    q = a[0] / b[0]
    rest = add(a, neg(mul((q, jnp.zeros_like(q)), b)))
    return tidy((q, rest[0] / b[0]))


def lane_total(a):
    for step in (64, 32, 16, 8, 4, 2, 1):
        a = plus(a, (pltpu.roll(a[0], step, 1), pltpu.roll(a[1], step, 1)))
    return a


def to_column(row):
    eye = iota((GROUP, LANES), 0) == iota((GROUP, LANES), 1)
    return jnp.broadcast_to(
        jnp.sum(jnp.where(eye, row, 0.0), axis=1, keepdims=True), (GROUP, LANES)
    )


def block_at(j):
    return pl.ds(pl.multiple_of(j * GROUP, 8), GROUP)


def tile_at(j):
    return pl.ds(pl.multiple_of(j * 8, 8), 8)


def product(s_ref, up_ref, high_ref, low_ref, j):
    acc = None
    sources = (
        (s_ref[block_at(j), 0:LANES], j),
        (s_ref[block_at(j - 1), LANES : 2 * LANES], j - 1),
        (up_ref[block_at(j), :], j + 1),
    )
    for s, at in sources:
        high = high_ref[block_at(at), :]
        p, e = times(s, high)
        e = e + s * low_ref[block_at(at), :]
        for r in range(0, GROUP, 8):
            term = p[r : r + 8], e[r : r + 8]
            acc = term if acc is None else plus(acc, term)
    for step in (4, 2, 1):
        acc = plus(acc, (pltpu.roll(acc[0], step, 0), pltpu.roll(acc[1], step, 0)))
    acc = tidy(acc)
    return acc[0] * SHRINK, acc[1] * SHRINK


def store_tile(ref, at, pair):
    row = iota((8, LANES), 0)
    ref[tile_at(at), :] = jnp.where(row == 0, pair[0], jnp.where(row == 1, pair[1], 0.0))


def powers(s_ref, up_ref, v_ref, cols, first, count, edge, base):
    for k in range(count):
        here, there = cols[k % 2], cols[1 - k % 2]

        def one(j, carry):
            pair = product(s_ref, up_ref, here[0], here[1], j)
            store_tile(v_ref, (first + k) * BLOCKS + j, pair)
            there[0][block_at(j), :] = to_column(pair[0][0:1])
            there[1][block_at(j), :] = to_column(pair[1][0:1])
            return carry

        lax.fori_loop(base + k * edge, BLOCKS - base - k * edge, one, 0)


def first_kernel(
    where_ref, p_ref, c_ref, n_ref, p2_ref, c2_ref, n2_ref,
    s_ref, up_ref, v_ref, v4_ref, h0_ref, l0_ref, h1_ref, l1_ref,
):
    core = where_ref[2]
    mine = pl.multiple_of(48 * core, 8)
    theirs = pl.multiple_of(48 - 48 * core, 8)
    diagonal = iota((GROUP, LANES), 0) == iota((GROUP, LANES), 1)
    lane = iota((GROUP, LANES), 1)
    for j in range(BLOCKS):
        rows = slice((j % 4) * 48, (j % 4 + 1) * 48)
        a = (p_ref, c_ref, n_ref)[j // 4]
        b = (p2_ref, c2_ref, n2_ref)[j // 4]
        s_ref[pl.ds(j * GROUP + mine, 48), :] = a[rows, :]
        s_ref[pl.ds(j * GROUP + theirs, 48), :] = b[rows, :]
    zero = jnp.zeros((LANES - GROUP, LANES), F32)

    def prepare(j, carry):
        own = s_ref[block_at(j), 0:LANES]
        rhs = jnp.broadcast_to(own[:, LANES - 1 : LANES], (GROUP, LANES)) * FIRST
        h0_ref[block_at(j), :] = rhs
        l0_ref[block_at(j), :] = jnp.zeros_like(rhs)
        store_tile(v_ref, j, (to_row(rhs), jnp.zeros((1, LANES), F32)))
        s_ref[block_at(j), 0:LANES] = jnp.where(lane < GROUP, own, 0.0) + jnp.where(
            diagonal, POSE_REG, 0.0
        )
        up = jnp.concatenate([s_ref[block_at(j), LANES : 2 * LANES], zero], axis=0).T
        up_ref[block_at(j), :] = up[0:GROUP]
        return carry

    lax.fori_loop(0, BLOCKS, prepare, 0)
    cols = ((h0_ref, l0_ref), (h1_ref, l1_ref))
    powers(s_ref, up_ref, v_ref, cols, 1, 4, 1, 1)
    for j in range(4):
        at = (4 * BLOCKS + 4 + j) * 8
        v4_ref[j : j + 1, :] = v_ref[at : at + 1, :]
        v4_ref[4 + j : 5 + j, :] = v_ref[at + 1 : at + 2, :]


def second_kernel(
    s_ref, up_ref, v_ref, below_ref, own_ref, above_ref, out_ref, v45_ref,
    h0_ref, l0_ref, h1_ref, l1_ref,
):
    for g, ref in enumerate((below_ref, own_ref, above_ref)):
        for j in range(4):
            pair = ref[j : j + 1, :], ref[4 + j : 5 + j, :]
            at = g * 4 + j
            store_tile(v45_ref, at, pair)
            if 1 < at < 10:
                h0_ref[block_at(at), :] = to_column(pair[0])
                l0_ref[block_at(at), :] = to_column(pair[1])
    cols = ((h0_ref, l0_ref), (h1_ref, l1_ref))
    powers(s_ref, up_ref, v45_ref, cols, 1, 2, 1, 3)
    zero = jnp.zeros((1, LANES), F32)
    total = None
    for j in range(4, 8):

        def row(k, part):
            ref, at = (v_ref, k) if k < 4 else (v45_ref, k - 4)
            at = (at * BLOCKS + j) * 8 + part
            return ref[at : at + 1, :]

        def stack(pick, part):
            lines = [row(pick(m), part) for m in range(2 * ITERS)]
            return jnp.concatenate(lines + [zero] * (16 - len(lines)), axis=0)

        lower, upper = (lambda m: m // 2), (lambda m: m - m // 2)
        a, b = (stack(lower, 0), stack(lower, 1)), (stack(upper, 0), stack(upper, 1))
        p, e = times(a[0], b[0])
        term = p, e + (a[0] * b[1] + a[1] * b[0])
        total = term if total is None else plus(total, term)
    total = tidy(lane_total(total))
    diagonal = iota((16, LANES), 0) == iota((16, LANES), 1)
    put(
        out_ref,
        [jnp.sum(jnp.where(diagonal, x, 0.0), axis=0, keepdims=True) for x in total],
    )


def put(ref, pair):
    ref[...] = jnp.zeros((8, LANES), F32)
    ref[0:1, :] = pair[0]
    ref[1:2, :] = pair[1]


def gather_sum(refs):
    acc = refs[0][0:1, :], refs[0][1:2, :]
    for r in refs[1:]:
        acc = plus(acc, (r[0:1, :], r[1:2, :]))
    return tidy(acc)


def sum_kernel(a_ref, b_ref, c_ref, d_ref, out_ref):
    put(out_ref, gather_sum((a_ref, b_ref, c_ref, d_ref)))


def solve_kernel(where_ref, a_ref, b_ref, c_ref, d_ref, v_ref, v45_ref, out_ref):
    at_quad = where_ref[3]
    total = gather_sum((a_ref, b_ref, c_ref, d_ref))
    shape = (8, LANES)
    row = iota(shape, 0)
    lane = iota(shape, 1)
    zero = jnp.zeros(shape, F32)
    unit = jnp.where((row == 1) & (lane == LANES - 1), 1.0, 0.0)

    def where(live, a, b):
        return jnp.where(live, a[0], b[0]), jnp.where(live, a[1], b[1])

    def at(a, r, k):
        return tuple(jnp.broadcast_to(x[r : r + 1, k : k + 1], shape) for x in a)

    x = jnp.where(row == 0, total[0], unit), jnp.where(row == 0, total[1], 0.0)
    y = x
    found = (zero, zero)
    one = (zero + 1.0, zero)
    start = at(x, 0, 0)
    now = start
    lead = one[0]
    live = start[0] > 0.0
    for k in range(ITERS):
        alpha = div(now, where(live, at(y, 0, k + 1), one))
        live = live & (alpha[0] > 0.0) & (alpha[0] < LARGEST_STEP)
        alpha = where(live, alpha, (zero, zero))
        found = add(found, mul(alpha, y))
        if k + 1 == ITERS:
            break
        back = neg(alpha)
        moved = tuple(pltpu.roll(p, LANES - 1, 1) for p in y)
        x = add(x, mul(back, moved))
        fresh = at(x, 0, k + 1)
        lead = -lead * alpha[0]
        live = live & (lead * fresh[0] > 1e-11 * start[0])
        beta = div(mul(back, fresh), where(live, now, one))
        beta = where(live, beta, (zero, zero))
        y = add(x, mul(beta, y))
        now = fresh
    xc = [tuple(p[1:2, LANES - 1 - k : LANES - k] for p in found) for k in range(ITERS)]
    for g in range(3):
        acc = None
        for k in range(ITERS):
            ref = v_ref if k < 4 else v45_ref
            tile = ref[tile_at((k if k < 4 else k - 4) * BLOCKS + 3 + at_quad + g), :]
            wide = tuple(jnp.broadcast_to(x, (1, LANES)) for x in xc[k])
            term = mul(wide, (tile[0:1], tile[1:2]))
            acc = term if acc is None else plus(acc, term)
        out_ref[g * 8 : g * 8 + 8, :] = jnp.broadcast_to(
            (acc[0] + acc[1]) * (SHRINK / FIRST), (8, LANES)
        )


def final_kernel(pose_ref, b_ref, g_ref, base_ref, scale_ref, out_ref, sum_ref):
    x0 = pose_ref[0:1, :]
    x1 = pose_ref[8:9, :]
    x2 = pose_ref[16:17, :]

    def frame(f, carry):
        rows = pl.ds(pl.multiple_of(f * GROUP, 8), GROUP)
        prod = (
            b_ref[rows, 0:LANES] * x0
            + b_ref[rows, LANES : 2 * LANES] * x1
            + b_ref[rows, 2 * LANES : 3 * LANES] * x2
        )
        x = jnp.sum(prod, axis=1, keepdims=True)
        image = jnp.sum(g_ref[rows, :] * x, axis=0, keepdims=True)
        at = pl.ds(pl.multiple_of(f * 8, 8), 8)
        sum_ref[at, :] = base_ref[at, :] - scale_ref[at, :] * image
        return carry

    lax.fori_loop(0, FD, frame, 0)
    for f in range(FD):
        out_ref[f : f + 1, :] = sum_ref[f * 8 : f * 8 + 1, :]


SMEM = pl.BlockSpec(memory_space=pltpu.SMEM)
VMEM = pl.BlockSpec(memory_space=pltpu.VMEM)


def call(kernel, name, outs, smem, *args, scratch=()):
    return pl.pallas_call(
        kernel,
        name=name,
        out_shape=[jax.ShapeDtypeStruct(s, F32) for s in outs],
        in_specs=[SMEM] * smem + [VMEM] * (len(args) - smem),
        out_specs=[VMEM] * len(outs),
        scratch_shapes=list(scratch),
    )(*args)


def per_device(edge_frames, rotvec, trans, inv_depth, depth_damping, flow, weight, mask):
    f_dev, plocal = inv_depth.shape
    count = lax.axis_size("frames")
    pixes = lax.axis_size("pix")
    fi = lax.axis_index("frames")
    pi = lax.axis_index("pix")
    spot = jnp.stack([fi * f_dev, pi * plocal, pi % 2, fi % 4]).astype(jnp.int32)

    def shift(block, step):
        return lax.ppermute(
            block, "frames", [(i, i + step) for i in range(count) if 0 <= i + step < count]
        )

    own, down, up = call(
        scatter_kernel, "scatter",
        [(4 * f_dev * SLOTS, plocal), (8 + 4 * SIDE, plocal), (4 * SIDE, plocal)],
        1, spot, edge_frames, flow.transpose(1, 0, 2), weight.transpose(1, 0, 2), mask,
    )
    from_after = shift(down, -1)
    from_before = shift(up, 1)
    tab, b, bt = call(
        pose_kernel, "pose",
        [(f_dev * SLOTS, LANES), (f_dev * GROUP, 3 * LANES), (192, f_dev * GROUP)],
        1, spot, rotvec, trans,
    )
    keep, send, g, base, scale = call(
        main_kernel, "main",
        [(96, 256), (96, 256), (f_dev * GROUP, plocal), (f_dev * 8, plocal), (f_dev * 8, plocal)],
        1, spot, own, from_after, from_before, inv_depth, depth_damping, tab, b, bt,
        scratch=[
            pltpu.VMEM((4 * FD * 8, plocal), F32),
            pltpu.VMEM((7 * 16, plocal), F32),
            pltpu.VMEM((GROUP, plocal), F32),
            pltpu.VMEM((256, plocal), F32),
            pltpu.VMEM((GROUP, LANES), F32),
            pltpu.VMEM((f_dev * GROUP, 3 * LANES), F32),
            pltpu.VMEM((192, 3 * LANES), F32),
        ],
    )
    got = lax.ppermute(send, "pix", [(i, i ^ 1) for i in range(pixes)])
    both = keep + got
    own_half, rim = both[:48], both[48:]
    both_axes = ("frames", "pix")

    def to_neighbour(flip):
        route = []
        for i in range(count):
            for k in range(pixes):
                to = i + 1 if k % 2 == 0 else i - 1
                if 0 <= to < count:
                    route.append((i * pixes + k, to * pixes + (k ^ flip)))
        return lax.ppermute(rim, both_axes, route)

    own_far = lax.ppermute(own_half, "pix", [(i, i ^ 2) for i in range(pixes)])
    rim_near = to_neighbour(0)
    rim_far = to_neighbour(2)
    (half,) = call(quad_kernel, "half", [(48, 256)], 1, spot, own_half, own_far, rim_near, rim_far)

    def mates(v, step):
        return [v] + [
            lax.ppermute(v, "frames", [(i, i ^ (k * step)) for i in range(count)]) for k in (1, 2, 3)
        ]

    def twin(v):
        return lax.ppermute(v, "pix", [(i, i ^ 1) for i in range(pixes)])

    def halo(v):
        return shift(v, 4), v, shift(v, -4)

    (quad,) = call(place_kernel, "place", [(192, 256)], 1, spot, *mates(half, 1))
    pieces = halo(quad)
    wide = BLOCKS * GROUP
    scratch = [pltpu.VMEM((wide, LANES), F32)] * 4
    s, up, vs, v4 = call(
        first_kernel, "first",
        [(wide, 256), (wide, LANES), (5 * BLOCKS * 8, LANES), (8, LANES)],
        1, spot, *pieces, *[twin(x) for x in pieces], scratch=scratch,
    )
    part, v45 = call(
        second_kernel, "second", [(8, LANES), (3 * BLOCKS * 8, LANES)], 0, s, up, vs, *halo(v4),
        scratch=scratch,
    )
    (part,) = call(sum_kernel, "sum", [(8, LANES)], 0, *mates(part, 4))
    (pose,) = call(solve_kernel, "solve", [(24, LANES)], 1, spot, *mates(part, 16), vs, v45)
    (depth_step,) = call(
        final_kernel, "final", [(f_dev, plocal)], 0, pose, b, g, base, scale,
        scratch=[pltpu.VMEM((f_dev * 8, plocal), F32)],
    )
    pose_step = pose[8, : f_dev * 6].reshape(f_dev, 6).T
    return pose_step, depth_step


def solution(mesh):
    return jax.shard_map(
        per_device,
        mesh=mesh,
        in_specs=(
            P(None, "frames"),
            P(),
            P(),
            P("frames", "pix"),
            P("frames", "pix"),
            P("frames", None, "pix"),
            P("frames", None, "pix"),
            P("frames", "pix"),
        ),
        out_specs=(P(None, "frames"), P("frames", "pix")),
        check_vma=False,
    )
```

```python
import functools
import jax
import jax.numpy as jnp
from jax import lax
from jax.experimental import pallas as pl
from jax.experimental.pallas import tpu as pltpu
from jax.sharding import PartitionSpec as P

ROWS = 48
COLS = 64
RADIUS = 8
ITERS = 6
HIGHEST = lax.Precision.HIGHEST
F32 = jnp.float32
BF16 = jnp.bfloat16
LANES = 128
FD = 16
SLOTS = 16
GROUP = FD * 6
SIDE = RADIUS * (RADIUS + 1) // 2
POSE_REG = 100.0


def iota(shape, dim):
    return lax.broadcasted_iota(jnp.int32, shape, dim)


def thirds(x):
    first = x.astype(BF16)
    rest = x - first.astype(F32)
    second = rest.astype(BF16)
    return first, second, (rest - second.astype(F32)).astype(BF16)


def pair_of(x):
    first = x.astype(BF16)
    return first, (x - first.astype(F32)).astype(BF16)


def dot(a, b):
    return jnp.dot(a, b, preferred_element_type=F32)


def scatter_kernel(where_ref, ef_ref, flow_ref, weight_ref, mask_ref, own_ref, down_ref, up_ref):
    edges = ef_ref.shape[1]
    start = where_ref[0]
    source = ef_ref[0:1, :] - start
    delta = ef_ref[1:2, :] - start - source
    slot = jnp.where(delta < 0, delta + 8, delta + 7)
    own_at = jnp.where((source >= 0) & (source < FD), source * SLOTS + slot, -1)
    j = source + 8
    down_at = jnp.where(source < 0, ((j * (j + 1)) >> 1) + delta - 8 + j, -1)
    j = 23 - source
    up_at = jnp.where(source >= FD, ((j * (j + 1)) >> 1) + slot, -1)
    hot = jnp.concatenate(
        [
            (iota((FD * SLOTS, edges), 0) == own_at).astype(F32),
            (iota((40, edges), 0) == down_at).astype(F32),
            (iota((40, edges), 0) == up_at).astype(F32),
        ],
        axis=0,
    ).astype(BF16)
    down_ref[0:8, :] = jnp.zeros((8, down_ref.shape[1]), F32)
    for chunk in range(mask_ref.shape[1] // LANES):
        lanes = pl.ds(chunk * LANES, LANES)
        live = mask_ref[:, lanes].astype(F32)
        parts = []
        for comp in range(2):
            conf = weight_ref[comp, :, lanes] * live
            parts.append((conf, conf * flow_ref[comp, :, lanes]))
        values = jnp.concatenate([parts[0][0], parts[1][0], parts[0][1], parts[1][1]], axis=1)
        got = sum(
            jnp.dot(hot, piece, preferred_element_type=F32) for piece in reversed(thirds(values))
        )
        for q in range(4):
            cut = got[:, q * LANES : (q + 1) * LANES]
            own_ref[q * 256 : (q + 1) * 256, lanes] = cut[0:256]
            down_ref[8 + q * SIDE : 8 + (q + 1) * SIDE, lanes] = cut[256 : 256 + SIDE]
            up_ref[q * SIDE : (q + 1) * SIDE, lanes] = cut[296 : 296 + SIDE]


def rotation_rows(w):
    x, y, z = w
    zero = jnp.zeros_like(x)
    cross = [[zero, -z, y], [z, zero, -x], [-y, x, zero]]
    sq = x * x + y * y + z * z
    first = 1.0 - sq / 6.0 + sq * sq / 120.0
    second = 0.5 - sq / 24.0 + sq * sq / 720.0
    return [
        [
            float(i == k)
            + first * cross[i][k]
            + second * sum(cross[i][m] * cross[m][k] for m in range(3))
            for k in range(3)
        ]
        for i in range(3)
    ]


def pose_kernel(where_ref, rotvec_ref, trans_ref, tab_ref, b_ref, bt_ref):
    start = where_ref[0]
    frames = rotvec_ref.shape[1]
    pair = iota((1, FD * SLOTS), 1)
    slot = pair & 15
    delta = jnp.where(slot < 8, slot - 8, slot - 7)
    at_source = start + (pair >> 4)
    at_target = jnp.clip(at_source + delta, 0, frames - 1)
    poses = jnp.concatenate([rotvec_ref[...], trans_ref[...], jnp.zeros((2, frames), F32)], axis=0)

    def pick(at):
        hot = (iota((frames, FD * SLOTS), 0) == at).astype(F32)
        return jnp.dot(poses, hot, precision=HIGHEST, preferred_element_type=F32)

    src = pick(at_source)
    tgt = pick(at_target)
    rs = rotation_rows([src[k : k + 1] for k in range(3)])
    rt = rotation_rows([tgt[k : k + 1] for k in range(3)])
    rel = [[sum(rt[i][k] * rs[m][k] for k in range(3)) for m in range(3)] for i in range(3)]
    tr = [
        tgt[3 + i : 4 + i] - sum(rel[i][m] * src[3 + m : 4 + m] for m in range(3)) for i in range(3)
    ]
    corner = [
        [tr[1] * rel[2][m] - tr[2] * rel[1][m] for m in range(3)],
        [tr[2] * rel[0][m] - tr[0] * rel[2][m] for m in range(3)],
        [tr[0] * rel[1][m] - tr[1] * rel[0][m] for m in range(3)],
    ]
    lines = [x for row in rel for x in row] + tr + [x for row in corner for x in row]
    lines = jnp.concatenate(lines + [jnp.zeros((LANES - len(lines), FD * SLOTS), F32)], axis=0)
    tab_ref[...] = lines.T

    lane3 = iota((SLOTS, 3 * LANES), 1)
    row3 = iota((SLOTS, 3 * LANES), 0)
    off3 = jnp.where(row3 < 8, row3 - 8, row3 - 7)

    def build(f, carry):
        frame = f + off3 + FD
        home = (frame >> 4) * LANES + (frame & 15) * 6
        tab = tab_ref[pl.ds(pl.multiple_of(f * SLOTS, SLOTS), SLOTS), :]
        for c in range(6):
            block = jnp.where(lane3 == home + c, 1.0, 0.0)
            for d in range(6):
                if c < 3:
                    at = c * 3 + d if d < 3 else 12 + c * 3 + d - 3
                elif d >= 3:
                    at = (c - 3) * 3 + d - 3
                else:
                    continue
                block = block - jnp.where(
                    lane3 == LANES + f * 6 + d, jnp.broadcast_to(tab[:, at : at + 1], lane3.shape), 0.0
                )
            b_ref[pl.ds(pl.multiple_of(f * GROUP + c * SLOTS, SLOTS), SLOTS), :] = block
        return carry

    lax.fori_loop(0, FD, build, 0)
    for g in range(4):
        cols = slice(g * 384, (g + 1) * 384)
        below = b_ref[cols, 0:LANES].T
        own = b_ref[cols, LANES : 2 * LANES].T
        above = b_ref[cols, 2 * LANES : 3 * LANES].T
        bt_ref[0:48, cols] = below[48:96]
        bt_ref[48:144, cols] = own[0:96]
        bt_ref[144:192, cols] = above[0:48]


def coords(first, chunk):
    pixel = first + chunk * LANES + iota((8, LANES), 1)
    col = ((pixel & (COLS - 1)).astype(F32) - 0.5 * (COLS - 1)) / COLS
    line = ((pixel >> 6).astype(F32) - 0.5 * (ROWS - 1)) / COLS
    return col, line


def pull(u, v, s, uv, u1, v1, pu, pv):
    spu = s * pu
    spv = s * pv
    return (
        spu,
        spv,
        -(u * spu + v * spv),
        -(uv * pu) - v1 * pv,
        u1 * pu + uv * pv,
        u * pv - v * pu,
    )


def pose_sums(u, v, s, cu, cv, eu, ev):
    uv = u * v
    u1 = 1.0 + u * u
    v1 = 1.0 + v * v
    terms = list(pull(u, v, s, uv, u1, v1, -eu, -ev))
    su_ = cu * s
    sv_ = cv * s
    ju = (-uv, u1, -v)
    jv = (-v1, uv, u)
    a00 = su_ * s
    a11 = sv_ * s
    a02 = -(a00 * u)
    a12 = -(a11 * v)
    terms += [a00, a11, a02, a12, -(a02 * u + a12 * v)]
    tu = [su_ * x for x in ju]
    tv = [sv_ * x for x in jv]
    terms += tu + tv
    terms += [-(u * x + v * y) for x, y in zip(tu, tv)]
    wu = [cu * x for x in ju]
    wv = [cv * x for x in jv]
    for a in range(3):
        for b in range(a, 3):
            terms.append(wu[a] * ju[b] + wv[a] * jv[b])
    return terms


def diagonal_rows(acc, h):
    lane = iota((8, LANES), 1)
    row = iota((8, LANES), 0)
    sums = [jnp.broadcast_to(jnp.sum(x, axis=1, keepdims=True), (8, LANES)) for x in acc]
    a = {(0, 0): 6, (1, 1): 7, (0, 2): 8, (1, 2): 9, (2, 2): 10}
    for k in range(3):
        a[(0, 3 + k)] = 11 + k
        a[(1, 3 + k)] = 14 + k
        a[(2, 3 + k)] = 17 + k
    at = 20
    for x in range(3):
        for y in range(x, 3):
            a[(3 + x, 3 + y)] = at
            at += 1
    tiles = []
    for c in range(6):
        tile = jnp.where(lane == LANES - 1, sums[c], 0.0)
        for d in range(6):
            key = (min(c, d), max(c, d))
            if key != (0, 1):
                tile = jnp.where(lane == d * SLOTS + 8 * h + row, sums[a[key]], tile)
        tiles.append(tile)
    return tiles


def early_kernel(
    where_ref, own_ref, depth_ref, tab_ref, geo_ref, curv_ref, grad_ref, block_ref, in_ref
):
    plocal = depth_ref.shape[1]
    chunks = plocal // LANES
    for f in range(FD):
        in_ref[f * 8 : f * 8 + 8, :] = jnp.broadcast_to(depth_ref[f : f + 1, :], (8, plocal))

    def frame(f, carry):
        eight = pl.ds(pl.multiple_of(f * 8, 8), 8)
        for h in range(2):
            tab = tab_ref[pl.ds(pl.multiple_of(f * SLOTS + 8 * h, 8), 8), :]
            r = [jnp.broadcast_to(tab[:, k : k + 1], (8, LANES)) for k in range(12)]
            acc = [0.0] * 26
            for c in range(chunks):
                lanes = pl.ds(c * LANES, LANES)
                col, line = coords(where_ref[1], c)
                depth = in_ref[eight, lanes]

                def at(q):
                    return pl.ds(pl.multiple_of(q * 256 + f * SLOTS + 8 * h, 8), 8)

                cu, cv, fu, fv = [own_ref[at(q), lanes] for q in range(4)]
                inv = 1.0 / (r[6] * col + r[7] * line + r[8] + depth * r[11])
                u = (r[0] * col + r[1] * line + r[2] + depth * r[9]) * inv
                v = (r[3] * col + r[4] * line + r[5] + depth * r[10]) * inv
                su = inv * (r[9] - u * r[11])
                sv = inv * (r[10] - v * r[11])
                eu = cu * (col - u) + fu
                ev = cv * (line - v) + fv
                au = cu * su
                av = cv * sv
                curv = au * su + av * sv
                grad = -(su * eu + sv * ev)
                if h:
                    curv = curv + curv_ref[eight, lanes]
                    grad = grad + grad_ref[eight, lanes]
                curv_ref[eight, lanes] = curv
                grad_ref[eight, lanes] = grad
                for q, x in enumerate((u, v, inv, au, av)):
                    geo_ref[at(q), lanes] = x
                acc = [x + y for x, y in zip(acc, pose_sums(u, v, depth * inv, cu, cv, eu, ev))]
            for c, tile in enumerate(diagonal_rows(acc, h)):
                block_ref[pl.ds(pl.multiple_of(f * GROUP + c * SLOTS + 8 * h, 8), 8), :] = tile
        return carry

    lax.fori_loop(0, FD, frame, 0)


def main_kernel(
    where_ref, rdown_ref, rup_ref, geo_ref, curv_ref, grad_ref, block_ref, depth_ref, damp_ref, tab_ref,
    b_ref, bt_ref,
    keep_ref, send_ref, g_ref, base_ref, scale_ref,
    half_ref, hi_ref, in_ref, q_ref, w_ref, t_ref,
):
    core = where_ref[2]
    plocal = depth_ref.shape[1]
    chunks = plocal // LANES
    row8 = iota((8, plocal), 0)
    for f in range(FD):
        j = 7 - f if f < 8 else f - 8
        base = j * (j + 1) // 2
        for q in range(4):
            if f < 8:
                first = q * SIDE + base
                extra = jnp.where(row8 <= j, rup_ref[first : first + 8, :], 0.0)
            else:
                first = 8 + q * SIDE + base - 7 + j
                extra = jnp.where(row8 >= 7 - j, rdown_ref[first : first + 8, :], 0.0)
            half_ref[(q * FD + f) * 8 : (q * FD + f + 1) * 8, :] = extra
        in_ref[f * 8 : f * 8 + 8, :] = jnp.broadcast_to(depth_ref[f : f + 1, :], (8, plocal))
        in_ref[128 + f * 8 : 136 + f * 8, :] = jnp.broadcast_to(damp_ref[f : f + 1, :], (8, plocal))
    lane = iota((8, LANES), 1)

    def frame(f, carry, merged):
        eight = pl.ds(pl.multiple_of(f * 8, 8), 8)
        tab = tab_ref[pl.ds(pl.multiple_of(f * SLOTS + 8 * merged, 8), 8), :]
        t0, t1, t2 = [jnp.broadcast_to(tab[:, k : k + 1], (8, LANES)) for k in (9, 10, 11)]
        acc = [0.0] * 26
        for c in range(chunks):
            lanes = pl.ds(c * LANES, LANES)
            col, line = coords(where_ref[1], c)
            depth = in_ref[eight, lanes]

            def geo(q, h):
                return geo_ref[pl.ds(pl.multiple_of(q * 256 + f * SLOTS + 8 * h, 8), 8), lanes]

            cu, cv, fu, fv = [
                half_ref[pl.ds(pl.multiple_of((q * FD + f) * 8, 8), 8), lanes] for q in range(4)
            ]
            u, v, inv = [geo(q, merged) for q in range(3)]
            su = inv * (t0 - u * t2)
            sv = inv * (t1 - v * t2)
            eu = cu * (col - u) + fu
            ev = cv * (line - v) + fv
            au = cu * su
            av = cv * sv
            acc = [x + y for x, y in zip(acc, pose_sums(u, v, depth * inv, cu, cv, eu, ev))]
            curv = curv_ref[eight, lanes] + (au * su + av * sv)
            grad = grad_ref[eight, lanes] - (su * eu + sv * ev)
            total = in_ref[pl.ds(pl.multiple_of(128 + f * 8, 8), 8), lanes] + jnp.sum(
                curv, axis=0, keepdims=True
            )
            base = jnp.sum(grad, axis=0, keepdims=True) / total
            root = jnp.sqrt(total)
            scale = 1.0 / root
            base_ref[eight, lanes] = base
            scale_ref[eight, lanes] = scale
            lifted = base * root
            hi_ref[GROUP : GROUP + 8, lanes] = lifted
            hi_ref[GROUP + 8 : GROUP + 16, lanes] = lifted - lifted.astype(BF16).astype(F32)
            for h in range(2):
                if h != merged:
                    u, v, inv = [geo(q, h) for q in range(3)]
                    gu, gv = geo(3, h), geo(4, h)
                else:
                    u, v, inv = [geo(q, h) for q in range(3)]
                    gu, gv = geo(3, h) + au, geo(4, h) + av
                rows = pull(
                    u, v, depth * inv, u * v, 1.0 + u * u, 1.0 + v * v, gu * scale, gv * scale
                )
                for k, x in enumerate(rows):
                    g_ref[pl.ds(pl.multiple_of(f * GROUP + k * SLOTS + 8 * h, 8), 8), lanes] = x
                    hi_ref[k * SLOTS + 8 * h : k * SLOTS + 8 * h + 8, lanes] = x
        rows = pl.ds(pl.multiple_of(f * GROUP, 8), GROUP)
        q_ref[...] = block_ref[rows, :]
        for c, tile in enumerate(diagonal_rows(acc, merged)):
            at = slice(c * SLOTS + 8 * merged, c * SLOTS + 8 * merged + 8)
            q_ref[at, :] = q_ref[at, :] + tile
        g = hi_ref[...]
        top, low = pair_of(g)
        both = lax.dot_general(
            jnp.concatenate([top[0:GROUP], low[0:GROUP]], axis=0), top, (((1,), (1,)), ((), ())),
            preferred_element_type=F32,
        )
        m = both[0:GROUP, 0:GROUP] + both[GROUP:, 0:GROUP] + both[GROUP:, 0:GROUP].T
        vec = q_ref[:, LANES - 1 : LANES] - (
            both[0:GROUP, GROUP : GROUP + 1]
            + both[GROUP:, GROUP : GROUP + 1]
            + both[0:GROUP, GROUP + 8 : GROUP + 9]
        )
        q = q_ref[:, 0:GROUP] - m
        q_top, q_low = pair_of(q)
        b_top, b_low = pair_of(b_ref[rows, :])
        both = dot(jnp.concatenate([q_top, q_low], axis=0), b_top)
        w = both[0:GROUP] + both[GROUP:]
        w_ref[rows, 0:LANES] = jnp.where(
            iota((GROUP, LANES), 1) == LANES - 1, jnp.broadcast_to(vec, (GROUP, LANES)), w[:, 0:LANES]
        )
        w_ref[rows, LANES : 2 * LANES] = w[:, LANES : 2 * LANES] + dot(q_top, b_low[:, LANES : 2 * LANES])
        w_ref[rows, 2 * LANES :] = w[:, 2 * LANES :]
        return carry

    lax.fori_loop(0, 8, functools.partial(frame, merged=0), 0)
    lax.fori_loop(8, 16, functools.partial(frame, merged=1), 0)
    bt_top, bt_low = pair_of(bt_ref[...])
    w_top, w_low = pair_of(w_ref[...])
    both = dot(jnp.concatenate([bt_top, bt_low], axis=0), w_top)
    t = both[0:192] + both[192:] + dot(bt_top, w_low)
    t_ref[...] = t
    for lo, hi, group, first in ((0, 48, 0, 48), (48, 144, 1, 0), (144, 192, 2, 0)):
        count = hi - lo
        lanes = slice(group * LANES, (group + 1) * LANES)
        square = jnp.concatenate(
            [jnp.zeros((first, LANES), F32)] * (first > 0)
            + [t[lo:hi, lanes], jnp.zeros((LANES - first - count, LANES), F32)],
            axis=0,
        )
        mean = 0.5 * (square + square.T)
        t_ref[lo:hi, lanes] = mean[first : first + count]
    last = iota((48, LANES), 1) == LANES - 1

    def half(core):
        own = slice(48 + 48 * core, 96 + 48 * core)
        rim = slice(0, 48) if core else slice(144, 192)
        group = 0 if core else 2
        mine = jnp.where(last, t[own, 0:LANES], t_ref[own, LANES : 2 * LANES])
        theirs = jnp.where(last, t[rim, 0:LANES], t_ref[rim, group * LANES : (group + 1) * LANES])
        far = t_ref[rim, LANES : 2 * LANES] if core else jnp.zeros((48, LANES), F32)
        return mine, t_ref[own, 2 * LANES :], theirs, far

    def put_half(ref, core):
        for k, x in enumerate(half(core)):
            ref[(k // 2) * 48 : (k // 2 + 1) * 48, (k % 2) * LANES : (k % 2 + 1) * LANES] = x

    @pl.when(core == 0)
    def _():
        put_half(keep_ref, 0)
        put_half(send_ref, 1)

    @pl.when(core == 1)
    def _():
        put_half(keep_ref, 1)
        put_half(send_ref, 0)


def to_row(column):
    return jnp.sum(
        jnp.where(iota((GROUP, LANES), 0) == iota((GROUP, LANES), 1), column, 0.0),
        axis=0,
        keepdims=True,
    )


BLOCKS = 12


def quad_kernel(where_ref, own_ref, own2_ref, rim_ref, rim2_ref, out_ref):
    out_ref[...] = (own_ref[...] + own2_ref[...]) + (rim_ref[...] + rim2_ref[...])


def place_kernel(where_ref, a_ref, b_ref, c_ref, d_ref, out_ref):
    at = where_ref[3]
    for k, ref in enumerate((a_ref, b_ref, c_ref, d_ref)):
        out_ref[pl.ds(pl.multiple_of(48 * (at ^ k), 8), 48), :] = ref[...]


SHRINK = 2.0**-15
FIRST = 2.0**-10
LARGEST_STEP = 1.001 / (POSE_REG * SHRINK)


def halves(x):
    t = 4097.0 * x
    top = t - (t - x)
    return top, x - top


def times(a, b):
    p = a * b
    ah, al = halves(a)
    bh, bl = halves(b)
    return p, ((ah * bh - p) + ah * bl + al * bh) + al * bl


def plus(a, b):
    t = a[0] + b[0]
    back = t - a[0]
    return t, (a[1] + b[1]) + ((a[0] - (t - back)) + (b[0] - back))


def tidy(a):
    t = a[0] + a[1]
    return t, a[1] - (t - a[0])


def mul(a, b):
    p, e = times(a[0], b[0])
    return tidy((p, e + (a[0] * b[1] + a[1] * b[0])))


def add(a, b):
    return tidy(plus(a, b))


def neg(a):
    return -a[0], -a[1]


def div(a, b):
    q = a[0] / b[0]
    rest = add(a, neg(mul((q, jnp.zeros_like(q)), b)))
    return tidy((q, rest[0] / b[0]))


def lane_total(a):
    for step in (64, 32, 16, 8, 4, 2, 1):
        a = plus(a, (pltpu.roll(a[0], step, 1), pltpu.roll(a[1], step, 1)))
    return a


def to_column(row):
    eye = iota((GROUP, LANES), 0) == iota((GROUP, LANES), 1)
    return jnp.broadcast_to(
        jnp.sum(jnp.where(eye, row, 0.0), axis=1, keepdims=True), (GROUP, LANES)
    )


def block_at(j):
    return pl.ds(pl.multiple_of(j * GROUP, 8), GROUP)


def tile_at(j):
    return pl.ds(pl.multiple_of(j * 8, 8), 8)


def product(s_ref, up_ref, high_ref, low_ref, j):
    acc = None
    sources = (
        (s_ref[block_at(j), 0:LANES], j),
        (s_ref[block_at(j - 1), LANES : 2 * LANES], j - 1),
        (up_ref[block_at(j), :], j + 1),
    )
    for s, at in sources:
        high = high_ref[block_at(at), :]
        p, e = times(s, high)
        e = e + s * low_ref[block_at(at), :]
        for r in range(0, GROUP, 8):
            term = p[r : r + 8], e[r : r + 8]
            acc = term if acc is None else plus(acc, term)
    for step in (4, 2, 1):
        acc = plus(acc, (pltpu.roll(acc[0], step, 0), pltpu.roll(acc[1], step, 0)))
    acc = tidy(acc)
    return acc[0] * SHRINK, acc[1] * SHRINK


def store_tile(ref, at, pair):
    row = iota((8, LANES), 0)
    ref[tile_at(at), :] = jnp.where(row == 0, pair[0], jnp.where(row == 1, pair[1], 0.0))


def powers(s_ref, up_ref, v_ref, cols, first, count, edge, base):
    for k in range(count):
        here, there = cols[k % 2], cols[1 - k % 2]

        def one(j, carry):
            pair = product(s_ref, up_ref, here[0], here[1], j)
            store_tile(v_ref, (first + k) * BLOCKS + j, pair)
            there[0][block_at(j), :] = to_column(pair[0][0:1])
            there[1][block_at(j), :] = to_column(pair[1][0:1])
            return carry

        lax.fori_loop(base + k * edge, BLOCKS - base - k * edge, one, 0)


def first_kernel(
    where_ref, p_ref, c_ref, n_ref, p2_ref, c2_ref, n2_ref,
    s_ref, up_ref, v_ref, v4_ref, h0_ref, l0_ref, h1_ref, l1_ref,
):
    core = where_ref[2]
    mine = pl.multiple_of(48 * core, 8)
    theirs = pl.multiple_of(48 - 48 * core, 8)
    diagonal = iota((GROUP, LANES), 0) == iota((GROUP, LANES), 1)
    lane = iota((GROUP, LANES), 1)
    for j in range(BLOCKS):
        rows = slice((j % 4) * 48, (j % 4 + 1) * 48)
        a = (p_ref, c_ref, n_ref)[j // 4]
        b = (p2_ref, c2_ref, n2_ref)[j // 4]
        s_ref[pl.ds(j * GROUP + mine, 48), :] = a[rows, :]
        s_ref[pl.ds(j * GROUP + theirs, 48), :] = b[rows, :]
    zero = jnp.zeros((LANES - GROUP, LANES), F32)

    def prepare(j, carry):
        own = s_ref[block_at(j), 0:LANES]
        rhs = jnp.broadcast_to(own[:, LANES - 1 : LANES], (GROUP, LANES)) * FIRST
        h0_ref[block_at(j), :] = rhs
        l0_ref[block_at(j), :] = jnp.zeros_like(rhs)
        store_tile(v_ref, j, (to_row(rhs), jnp.zeros((1, LANES), F32)))
        s_ref[block_at(j), 0:LANES] = jnp.where(lane < GROUP, own, 0.0) + jnp.where(
            diagonal, POSE_REG, 0.0
        )
        up = jnp.concatenate([s_ref[block_at(j), LANES : 2 * LANES], zero], axis=0).T
        up_ref[block_at(j), :] = up[0:GROUP]
        return carry

    lax.fori_loop(0, BLOCKS, prepare, 0)
    cols = ((h0_ref, l0_ref), (h1_ref, l1_ref))
    powers(s_ref, up_ref, v_ref, cols, 1, 4, 1, 1)
    for j in range(4):
        at = (4 * BLOCKS + 4 + j) * 8
        v4_ref[j : j + 1, :] = v_ref[at : at + 1, :]
        v4_ref[4 + j : 5 + j, :] = v_ref[at + 1 : at + 2, :]


def second_kernel(
    s_ref, up_ref, v_ref, below_ref, own_ref, above_ref, out_ref, v45_ref,
    h0_ref, l0_ref, h1_ref, l1_ref,
):
    for g, ref in enumerate((below_ref, own_ref, above_ref)):
        for j in range(4):
            pair = ref[j : j + 1, :], ref[4 + j : 5 + j, :]
            at = g * 4 + j
            store_tile(v45_ref, at, pair)
            if 1 < at < 10:
                h0_ref[block_at(at), :] = to_column(pair[0])
                l0_ref[block_at(at), :] = to_column(pair[1])
    cols = ((h0_ref, l0_ref), (h1_ref, l1_ref))
    powers(s_ref, up_ref, v45_ref, cols, 1, 2, 1, 3)
    zero = jnp.zeros((1, LANES), F32)
    total = None
    for j in range(4, 8):

        def row(k, part):
            ref, at = (v_ref, k) if k < 4 else (v45_ref, k - 4)
            at = (at * BLOCKS + j) * 8 + part
            return ref[at : at + 1, :]

        def stack(pick, part):
            lines = [row(pick(m), part) for m in range(2 * ITERS)]
            return jnp.concatenate(lines + [zero] * (16 - len(lines)), axis=0)

        lower, upper = (lambda m: m // 2), (lambda m: m - m // 2)
        a, b = (stack(lower, 0), stack(lower, 1)), (stack(upper, 0), stack(upper, 1))
        p, e = times(a[0], b[0])
        term = p, e + (a[0] * b[1] + a[1] * b[0])
        total = term if total is None else plus(total, term)
    total = tidy(lane_total(total))
    diagonal = iota((16, LANES), 0) == iota((16, LANES), 1)
    put(
        out_ref,
        [jnp.sum(jnp.where(diagonal, x, 0.0), axis=0, keepdims=True) for x in total],
    )


def put(ref, pair):
    ref[...] = jnp.zeros((8, LANES), F32)
    ref[0:1, :] = pair[0]
    ref[1:2, :] = pair[1]


def gather_sum(refs):
    acc = refs[0][0:1, :], refs[0][1:2, :]
    for r in refs[1:]:
        acc = plus(acc, (r[0:1, :], r[1:2, :]))
    return tidy(acc)


def sum_kernel(a_ref, b_ref, c_ref, d_ref, out_ref):
    put(out_ref, gather_sum((a_ref, b_ref, c_ref, d_ref)))


def solve_kernel(
    where_ref, a_ref, b_ref, c_ref, d_ref, v_ref, v45_ref, base_ref, scale_ref, move_hbm, g_hbm,
    pose_ref, out_ref, sum_ref, move_ref, g_ref, sems,
):
    copies = [
        pltpu.make_async_copy(move_hbm, move_ref, sems.at[0]),
        pltpu.make_async_copy(g_hbm, g_ref, sems.at[1]),
    ]
    for copy in copies:
        copy.start()
    at_quad = where_ref[3]
    total = gather_sum((a_ref, b_ref, c_ref, d_ref))
    shape = (8, LANES)
    row = iota(shape, 0)
    lane = iota(shape, 1)
    zero = jnp.zeros(shape, F32)
    unit = jnp.where((row == 1) & (lane == LANES - 1), 1.0, 0.0)

    def where(live, a, b):
        return jnp.where(live, a[0], b[0]), jnp.where(live, a[1], b[1])

    def at(a, r, k):
        return tuple(jnp.broadcast_to(x[r : r + 1, k : k + 1], shape) for x in a)

    x = jnp.where(row == 0, total[0], unit), jnp.where(row == 0, total[1], 0.0)
    y = x
    found = (zero, zero)
    one = (zero + 1.0, zero)
    start = at(x, 0, 0)
    now = start
    lead = one[0]
    live = start[0] > 0.0
    for k in range(ITERS):
        alpha = div(now, where(live, at(y, 0, k + 1), one))
        live = live & (alpha[0] > 0.0) & (alpha[0] < LARGEST_STEP)
        alpha = where(live, alpha, (zero, zero))
        found = add(found, mul(alpha, y))
        if k + 1 == ITERS:
            break
        back = neg(alpha)
        moved = tuple(pltpu.roll(p, LANES - 1, 1) for p in y)
        x = add(x, mul(back, moved))
        fresh = at(x, 0, k + 1)
        lead = -lead * alpha[0]
        live = live & (lead * fresh[0] > 1e-11 * start[0])
        beta = div(mul(back, fresh), where(live, now, one))
        beta = where(live, beta, (zero, zero))
        y = add(x, mul(beta, y))
        now = fresh
    xc = [tuple(p[1:2, LANES - 1 - k : LANES - k] for p in found) for k in range(ITERS)]
    poses = []
    for g in range(3):
        acc = None
        for k in range(ITERS):
            ref = v_ref if k < 4 else v45_ref
            tile = ref[tile_at((k if k < 4 else k - 4) * BLOCKS + 3 + at_quad + g), :]
            wide = tuple(jnp.broadcast_to(x, (1, LANES)) for x in xc[k])
            term = mul(wide, (tile[0:1], tile[1:2]))
            acc = term if acc is None else plus(acc, term)
        poses.append((acc[0] + acc[1]) * (SHRINK / FIRST))
    column = to_column(poses[1])
    r = iota((GROUP, LANES), 0)
    l = iota((GROUP, LANES), 1)
    for c in range(6):
        line = jnp.sum(jnp.where(r == l * 6 + c, column, 0.0), axis=0, keepdims=True)
        pose_ref[c : c + 1, :] = line[:, 0:FD]
    for copy in copies:
        copy.wait()

    def frame(f, carry):
        rows = pl.ds(pl.multiple_of(f * GROUP, 8), GROUP)
        prod = (
            move_ref[rows, 0:LANES] * poses[0]
            + move_ref[rows, LANES : 2 * LANES] * poses[1]
            + move_ref[rows, 2 * LANES : 3 * LANES] * poses[2]
        )
        x = jnp.sum(prod, axis=1, keepdims=True)
        image = jnp.sum(g_ref[rows, :] * x, axis=0, keepdims=True)
        at = tile_at(f)
        sum_ref[at, :] = base_ref[at, :] - scale_ref[at, :] * image
        return carry

    lax.fori_loop(0, FD, frame, 0)
    for f in range(FD):
        out_ref[f : f + 1, :] = sum_ref[f * 8 : f * 8 + 1, :]


SMEM = pl.BlockSpec(memory_space=pltpu.SMEM)
VMEM = pl.BlockSpec(memory_space=pltpu.VMEM)
ANY = pl.BlockSpec(memory_space=pl.ANY)


def call(kernel, name, outs, smem, *args, scratch=(), hbm=0):
    return pl.pallas_call(
        kernel,
        name=name,
        out_shape=[jax.ShapeDtypeStruct(s, F32) for s in outs],
        in_specs=[SMEM] * smem + [VMEM] * (len(args) - smem - hbm) + [ANY] * hbm,
        out_specs=[VMEM] * len(outs),
        scratch_shapes=list(scratch),
    )(*args)


def per_device(edge_frames, rotvec, trans, inv_depth, depth_damping, flow, weight, mask):
    f_dev, plocal = inv_depth.shape
    count = lax.axis_size("frames")
    pixes = lax.axis_size("pix")
    fi = lax.axis_index("frames")
    pi = lax.axis_index("pix")
    spot = jnp.stack([fi * f_dev, pi * plocal, pi % 2, fi % 4]).astype(jnp.int32)

    def shift(block, step):
        return lax.ppermute(
            block, "frames", [(i, i + step) for i in range(count) if 0 <= i + step < count]
        )

    own, down, up = call(
        scatter_kernel, "scatter",
        [(4 * f_dev * SLOTS, plocal), (8 + 4 * SIDE, plocal), (4 * SIDE, plocal)],
        1, spot, edge_frames, flow.transpose(1, 0, 2), weight.transpose(1, 0, 2), mask,
    )
    from_after = shift(down, -1)
    from_before = shift(up, 1)
    tab, b, bt = call(
        pose_kernel, "pose",
        [(f_dev * SLOTS, LANES), (f_dev * GROUP, 3 * LANES), (192, f_dev * GROUP)],
        1, spot, rotvec, trans,
    )
    pairs = f_dev * SLOTS
    geo, curv, grad, block = call(
        early_kernel, "early",
        [(5 * pairs, plocal), (f_dev * 8, plocal), (f_dev * 8, plocal), (f_dev * GROUP, LANES)],
        1, spot, own, inv_depth, tab, scratch=[pltpu.VMEM((f_dev * 8, plocal), F32)],
    )
    keep, send, g, base, scale = call(
        main_kernel, "main",
        [(96, 256), (96, 256), (f_dev * GROUP, plocal), (f_dev * 8, plocal), (f_dev * 8, plocal)],
        1, spot, from_after, from_before, geo, curv, grad, block, inv_depth, depth_damping, tab, b, bt,
        scratch=[
            pltpu.VMEM((4 * FD * 8, plocal), F32),
            pltpu.VMEM((GROUP + 16, plocal), F32),
            pltpu.VMEM((256, plocal), F32),
            pltpu.VMEM((GROUP, LANES), F32),
            pltpu.VMEM((f_dev * GROUP, 3 * LANES), F32),
            pltpu.VMEM((192, 3 * LANES), F32),
        ],
    )
    got = lax.ppermute(send, "pix", [(i, i ^ 1) for i in range(pixes)])
    both = keep + got
    own_half, rim = both[:48], both[48:]
    both_axes = ("frames", "pix")

    def to_neighbour(flip):
        route = []
        for i in range(count):
            for k in range(pixes):
                to = i + 1 if k % 2 == 0 else i - 1
                if 0 <= to < count:
                    route.append((i * pixes + k, to * pixes + (k ^ flip)))
        return lax.ppermute(rim, both_axes, route)

    own_far = lax.ppermute(own_half, "pix", [(i, i ^ 2) for i in range(pixes)])
    rim_near = to_neighbour(0)
    rim_far = to_neighbour(2)
    (half,) = call(quad_kernel, "half", [(48, 256)], 1, spot, own_half, own_far, rim_near, rim_far)

    def mates(v, step):
        return [v] + [
            lax.ppermute(v, "frames", [(i, i ^ (k * step)) for i in range(count)]) for k in (1, 2, 3)
        ]

    def twin(v):
        return lax.ppermute(v, "pix", [(i, i ^ 1) for i in range(pixes)])

    def halo(v):
        return shift(v, 4), v, shift(v, -4)

    (quad,) = call(place_kernel, "place", [(192, 256)], 1, spot, *mates(half, 1))
    pieces = halo(quad)
    wide = BLOCKS * GROUP
    scratch = [pltpu.VMEM((wide, LANES), F32)] * 4
    s, up, vs, v4 = call(
        first_kernel, "first",
        [(wide, 256), (wide, LANES), (5 * BLOCKS * 8, LANES), (8, LANES)],
        1, spot, *pieces, *[twin(x) for x in pieces], scratch=scratch,
    )
    part, v45 = call(
        second_kernel, "second", [(8, LANES), (3 * BLOCKS * 8, LANES)], 0, s, up, vs, *halo(v4),
        scratch=scratch,
    )
    (part,) = call(sum_kernel, "sum", [(8, LANES)], 0, *mates(part, 4))
    pose_step, depth_step = call(
        solve_kernel, "solve", [(6, f_dev), (f_dev, plocal)], 1, spot, *mates(part, 16), vs, v45,
        base, scale, b, g,
        scratch=[
            pltpu.VMEM((f_dev * 8, plocal), F32),
            pltpu.VMEM((f_dev * GROUP, 3 * LANES), F32),
            pltpu.VMEM((f_dev * GROUP, plocal), F32),
            pltpu.SemaphoreType.DMA((2,)),
        ],
        hbm=2,
    )
    return pose_step, depth_step


def solution(mesh):
    return jax.shard_map(
        per_device,
        mesh=mesh,
        in_specs=(
            P(None, "frames"),
            P(),
            P(),
            P("frames", "pix"),
            P("frames", "pix"),
            P("frames", None, "pix"),
            P("frames", None, "pix"),
            P("frames", "pix"),
        ),
        out_specs=(P(None, "frames"), P("frames", "pix")),
        check_vma=False,
    )
```

```python
import functools
import jax
import jax.numpy as jnp
from jax import lax
from jax.experimental import pallas as pl
from jax.experimental.pallas import tpu as pltpu
from jax.sharding import PartitionSpec as P

ROWS = 48
COLS = 64
RADIUS = 8
ITERS = 6
HIGHEST = lax.Precision.HIGHEST
F32 = jnp.float32
BF16 = jnp.bfloat16
LANES = 128
FD = 16
SLOTS = 16
GROUP = FD * 6
SIDE = RADIUS * (RADIUS + 1) // 2
POSE_REG = 100.0


def iota(shape, dim):
    return lax.broadcasted_iota(jnp.int32, shape, dim)


def thirds(x):
    first = x.astype(BF16)
    rest = x - first.astype(F32)
    second = rest.astype(BF16)
    return first, second, (rest - second.astype(F32)).astype(BF16)


def pair_of(x):
    first = x.astype(BF16)
    return first, (x - first.astype(F32)).astype(BF16)


def dot(a, b):
    return jnp.dot(a, b, preferred_element_type=F32)


def spread(where_ref, ef_ref, flow_ref, weight_ref, mask_ref, rims, write):
    edges = ef_ref.shape[1]
    start = where_ref[0]
    source = ef_ref[0:1, :] - start
    delta = ef_ref[1:2, :] - start - source
    slot = jnp.where(delta < 0, delta + 8, delta + 7)
    if rims:
        j = source + 8
        down_at = jnp.where(source < 0, ((j * (j + 1)) >> 1) + delta - 8 + j, -1)
        j = 23 - source
        up_at = jnp.where(source >= FD, ((j * (j + 1)) >> 1) + slot, -1)
        row = iota((40, edges), 0)
        hot = jnp.concatenate([(row == down_at).astype(F32), (row == up_at).astype(F32)], axis=0)
    else:
        own_at = jnp.where((source >= 0) & (source < FD), source * SLOTS + slot, -1)
        hot = (iota((FD * SLOTS, edges), 0) == own_at).astype(F32)
    hot = hot.astype(BF16)
    for chunk in range(mask_ref.shape[1] // LANES):
        lanes = pl.ds(chunk * LANES, LANES)
        live = mask_ref[:, lanes].astype(F32)
        parts = []
        for comp in range(2):
            conf = weight_ref[comp, :, lanes] * live
            parts.append((conf, conf * flow_ref[comp, :, lanes]))
        values = jnp.concatenate([parts[0][0], parts[1][0], parts[0][1], parts[1][1]], axis=1)
        got = sum(dot(hot, piece) for piece in reversed(thirds(values)))
        for q in range(4):
            write(q, lanes, got[:, q * LANES : (q + 1) * LANES])


def rim_kernel(where_ref, ef_ref, flow_ref, weight_ref, mask_ref, down_ref, up_ref):
    down_ref[0:8, :] = jnp.zeros((8, down_ref.shape[1]), F32)

    def write(q, lanes, cut):
        down_ref[8 + q * SIDE : 8 + (q + 1) * SIDE, lanes] = cut[0:SIDE]
        up_ref[q * SIDE : (q + 1) * SIDE, lanes] = cut[40 : 40 + SIDE]

    spread(where_ref, ef_ref, flow_ref, weight_ref, mask_ref, True, write)


def own_kernel(where_ref, ef_ref, flow_ref, weight_ref, mask_ref, own_ref):
    def write(q, lanes, cut):
        own_ref[q * 256 : (q + 1) * 256, lanes] = cut

    spread(where_ref, ef_ref, flow_ref, weight_ref, mask_ref, False, write)


def rotation_rows(w):
    x, y, z = w
    zero = jnp.zeros_like(x)
    cross = [[zero, -z, y], [z, zero, -x], [-y, x, zero]]
    sq = x * x + y * y + z * z
    first = 1.0 - sq / 6.0 + sq * sq / 120.0
    second = 0.5 - sq / 24.0 + sq * sq / 720.0
    return [
        [
            float(i == k)
            + first * cross[i][k]
            + second * sum(cross[i][m] * cross[m][k] for m in range(3))
            for k in range(3)
        ]
        for i in range(3)
    ]


def pose_kernel(where_ref, rotvec_ref, trans_ref, tab_ref, b_ref, bt_ref):
    start = where_ref[0]
    frames = rotvec_ref.shape[1]
    pair = iota((1, FD * SLOTS), 1)
    slot = pair & 15
    delta = jnp.where(slot < 8, slot - 8, slot - 7)
    at_source = start + (pair >> 4)
    at_target = jnp.clip(at_source + delta, 0, frames - 1)
    poses = jnp.concatenate([rotvec_ref[...], trans_ref[...], jnp.zeros((2, frames), F32)], axis=0)

    def pick(at):
        hot = (iota((frames, FD * SLOTS), 0) == at).astype(F32)
        return jnp.dot(poses, hot, precision=HIGHEST, preferred_element_type=F32)

    src = pick(at_source)
    tgt = pick(at_target)
    rs = rotation_rows([src[k : k + 1] for k in range(3)])
    rt = rotation_rows([tgt[k : k + 1] for k in range(3)])
    rel = [[sum(rt[i][k] * rs[m][k] for k in range(3)) for m in range(3)] for i in range(3)]
    tr = [
        tgt[3 + i : 4 + i] - sum(rel[i][m] * src[3 + m : 4 + m] for m in range(3)) for i in range(3)
    ]
    corner = [
        [tr[1] * rel[2][m] - tr[2] * rel[1][m] for m in range(3)],
        [tr[2] * rel[0][m] - tr[0] * rel[2][m] for m in range(3)],
        [tr[0] * rel[1][m] - tr[1] * rel[0][m] for m in range(3)],
    ]
    lines = [x for row in rel for x in row] + tr + [x for row in corner for x in row]
    lines = jnp.concatenate(lines + [jnp.zeros((LANES - len(lines), FD * SLOTS), F32)], axis=0)
    tab_ref[...] = lines.T

    lane3 = iota((SLOTS, 3 * LANES), 1)
    row3 = iota((SLOTS, 3 * LANES), 0)
    off3 = jnp.where(row3 < 8, row3 - 8, row3 - 7)

    def build(f, carry):
        frame = f + off3 + FD
        home = (frame >> 4) * LANES + (frame & 15) * 6
        tab = tab_ref[pl.ds(pl.multiple_of(f * SLOTS, SLOTS), SLOTS), :]
        for c in range(6):
            block = jnp.where(lane3 == home + c, 1.0, 0.0)
            for d in range(6):
                if c < 3:
                    at = c * 3 + d if d < 3 else 12 + c * 3 + d - 3
                elif d >= 3:
                    at = (c - 3) * 3 + d - 3
                else:
                    continue
                block = block - jnp.where(
                    lane3 == LANES + f * 6 + d, jnp.broadcast_to(tab[:, at : at + 1], lane3.shape), 0.0
                )
            b_ref[pl.ds(pl.multiple_of(f * GROUP + c * SLOTS, SLOTS), SLOTS), :] = block
        return carry

    lax.fori_loop(0, FD, build, 0)
    for g in range(4):
        cols = slice(g * 384, (g + 1) * 384)
        below = b_ref[cols, 0:LANES].T
        own = b_ref[cols, LANES : 2 * LANES].T
        above = b_ref[cols, 2 * LANES : 3 * LANES].T
        bt_ref[0:48, cols] = below[48:96]
        bt_ref[48:144, cols] = own[0:96]
        bt_ref[144:192, cols] = above[0:48]


def coords(first, chunk):
    pixel = first + chunk * LANES + iota((8, LANES), 1)
    col = ((pixel & (COLS - 1)).astype(F32) - 0.5 * (COLS - 1)) / COLS
    line = ((pixel >> 6).astype(F32) - 0.5 * (ROWS - 1)) / COLS
    return col, line


def pull(u, v, s, uv, u1, v1, pu, pv):
    spu = s * pu
    spv = s * pv
    return (
        spu,
        spv,
        -(u * spu + v * spv),
        -(uv * pu) - v1 * pv,
        u1 * pu + uv * pv,
        u * pv - v * pu,
    )


def pose_sums(u, v, s, cu, cv, eu, ev):
    uv = u * v
    u1 = 1.0 + u * u
    v1 = 1.0 + v * v
    terms = list(pull(u, v, s, uv, u1, v1, -eu, -ev))
    su_ = cu * s
    sv_ = cv * s
    ju = (-uv, u1, -v)
    jv = (-v1, uv, u)
    a00 = su_ * s
    a11 = sv_ * s
    a02 = -(a00 * u)
    a12 = -(a11 * v)
    terms += [a00, a11, a02, a12, -(a02 * u + a12 * v)]
    tu = [su_ * x for x in ju]
    tv = [sv_ * x for x in jv]
    terms += tu + tv
    terms += [-(u * x + v * y) for x, y in zip(tu, tv)]
    wu = [cu * x for x in ju]
    wv = [cv * x for x in jv]
    for a in range(3):
        for b in range(a, 3):
            terms.append(wu[a] * ju[b] + wv[a] * jv[b])
    return terms


def diagonal_rows(acc, h):
    lane = iota((8, LANES), 1)
    row = iota((8, LANES), 0)
    sums = [jnp.broadcast_to(jnp.sum(x, axis=1, keepdims=True), (8, LANES)) for x in acc]
    a = {(0, 0): 6, (1, 1): 7, (0, 2): 8, (1, 2): 9, (2, 2): 10}
    for k in range(3):
        a[(0, 3 + k)] = 11 + k
        a[(1, 3 + k)] = 14 + k
        a[(2, 3 + k)] = 17 + k
    at = 20
    for x in range(3):
        for y in range(x, 3):
            a[(3 + x, 3 + y)] = at
            at += 1
    tiles = []
    for c in range(6):
        tile = jnp.where(lane == LANES - 1, sums[c], 0.0)
        for d in range(6):
            key = (min(c, d), max(c, d))
            if key != (0, 1):
                tile = jnp.where(lane == d * SLOTS + 8 * h + row, sums[a[key]], tile)
        tiles.append(tile)
    return tiles


def early_kernel(
    where_ref, own_ref, depth_ref, tab_ref, geo_ref, curv_ref, grad_ref, block_ref, in_ref
):
    plocal = depth_ref.shape[1]
    chunks = plocal // LANES
    for f in range(FD):
        in_ref[f * 8 : f * 8 + 8, :] = jnp.broadcast_to(depth_ref[f : f + 1, :], (8, plocal))

    def frame(f, carry):
        eight = pl.ds(pl.multiple_of(f * 8, 8), 8)
        for h in range(2):
            tab = tab_ref[pl.ds(pl.multiple_of(f * SLOTS + 8 * h, 8), 8), :]
            r = [jnp.broadcast_to(tab[:, k : k + 1], (8, LANES)) for k in range(12)]
            acc = [0.0] * 26
            for c in range(chunks):
                lanes = pl.ds(c * LANES, LANES)
                col, line = coords(where_ref[1], c)
                depth = in_ref[eight, lanes]

                def at(q):
                    return pl.ds(pl.multiple_of(q * 256 + f * SLOTS + 8 * h, 8), 8)

                cu, cv, fu, fv = [own_ref[at(q), lanes] for q in range(4)]
                inv = 1.0 / (r[6] * col + r[7] * line + r[8] + depth * r[11])
                u = (r[0] * col + r[1] * line + r[2] + depth * r[9]) * inv
                v = (r[3] * col + r[4] * line + r[5] + depth * r[10]) * inv
                su = inv * (r[9] - u * r[11])
                sv = inv * (r[10] - v * r[11])
                eu = cu * (col - u) + fu
                ev = cv * (line - v) + fv
                au = cu * su
                av = cv * sv
                curv = au * su + av * sv
                grad = -(su * eu + sv * ev)
                if h:
                    curv = curv + curv_ref[eight, lanes]
                    grad = grad + grad_ref[eight, lanes]
                curv_ref[eight, lanes] = curv
                grad_ref[eight, lanes] = grad
                for q, x in enumerate((u, v, inv, au, av)):
                    row = pl.multiple_of((f * 5 + q) * SLOTS + 8 * h, 8)
                    geo_ref[pl.ds(row, 8), lanes] = x
                acc = [x + y for x, y in zip(acc, pose_sums(u, v, depth * inv, cu, cv, eu, ev))]
            for c, tile in enumerate(diagonal_rows(acc, h)):
                block_ref[pl.ds(pl.multiple_of(f * GROUP + c * SLOTS + 8 * h, 8), 8), :] = tile
        return carry

    lax.fori_loop(0, FD, frame, 0)


def main_kernel(
    where_ref, rdown_ref, rup_ref, curv_ref, grad_ref, block_ref, depth_ref, damp_ref, tab_ref,
    geo_hbm, b_hbm, bt_hbm,
    keep_ref, send_ref, base_ref, scale_ref, g_hbm,
    half_ref, hi_ref, in_ref, q_ref, w_ref, t_ref, geo_ref, b_ref, bt_ref, g_ref,
    geo_sems, b_sems, g_sems, bt_sem,
):
    def piece(src, dst, sems, f, rows):
        at = pl.ds(pl.multiple_of(f * rows, 8), rows)
        return pltpu.make_async_copy(src.at[at, :], dst.at[at, :], sems.at[f])

    for f in range(FD):
        piece(geo_hbm, geo_ref, geo_sems, f, 5 * SLOTS).start()
        piece(b_hbm, b_ref, b_sems, f, GROUP).start()
    bt_copy = pltpu.make_async_copy(bt_hbm, bt_ref, bt_sem.at[0])
    bt_copy.start()
    core = where_ref[2]
    plocal = depth_ref.shape[1]
    chunks = plocal // LANES
    row8 = iota((8, plocal), 0)
    for f in range(FD):
        j = 7 - f if f < 8 else f - 8
        base = j * (j + 1) // 2
        for q in range(4):
            if f < 8:
                first = q * SIDE + base
                extra = jnp.where(row8 <= j, rup_ref[first : first + 8, :], 0.0)
            else:
                first = 8 + q * SIDE + base - 7 + j
                extra = jnp.where(row8 >= 7 - j, rdown_ref[first : first + 8, :], 0.0)
            half_ref[(q * FD + f) * 8 : (q * FD + f + 1) * 8, :] = extra
        in_ref[f * 8 : f * 8 + 8, :] = jnp.broadcast_to(depth_ref[f : f + 1, :], (8, plocal))
        in_ref[128 + f * 8 : 136 + f * 8, :] = jnp.broadcast_to(damp_ref[f : f + 1, :], (8, plocal))
    lane = iota((8, LANES), 1)

    def frame(f, carry, merged):
        eight = pl.ds(pl.multiple_of(f * 8, 8), 8)
        piece(geo_hbm, geo_ref, geo_sems, f, 5 * SLOTS).wait()
        piece(b_hbm, b_ref, b_sems, f, GROUP).wait()
        tab = tab_ref[pl.ds(pl.multiple_of(f * SLOTS + 8 * merged, 8), 8), :]
        t0, t1, t2 = [jnp.broadcast_to(tab[:, k : k + 1], (8, LANES)) for k in (9, 10, 11)]
        acc = [0.0] * 26
        for c in range(chunks):
            lanes = pl.ds(c * LANES, LANES)
            col, line = coords(where_ref[1], c)
            depth = in_ref[eight, lanes]

            def geo(q, h):
                return geo_ref[pl.ds(pl.multiple_of((f * 5 + q) * SLOTS + 8 * h, 8), 8), lanes]

            cu, cv, fu, fv = [
                half_ref[pl.ds(pl.multiple_of((q * FD + f) * 8, 8), 8), lanes] for q in range(4)
            ]
            u, v, inv = [geo(q, merged) for q in range(3)]
            su = inv * (t0 - u * t2)
            sv = inv * (t1 - v * t2)
            eu = cu * (col - u) + fu
            ev = cv * (line - v) + fv
            au = cu * su
            av = cv * sv
            acc = [x + y for x, y in zip(acc, pose_sums(u, v, depth * inv, cu, cv, eu, ev))]
            curv = curv_ref[eight, lanes] + (au * su + av * sv)
            grad = grad_ref[eight, lanes] - (su * eu + sv * ev)
            total = in_ref[pl.ds(pl.multiple_of(128 + f * 8, 8), 8), lanes] + jnp.sum(
                curv, axis=0, keepdims=True
            )
            base = jnp.sum(grad, axis=0, keepdims=True) / total
            root = jnp.sqrt(total)
            scale = 1.0 / root
            base_ref[eight, lanes] = base
            scale_ref[eight, lanes] = scale
            lifted = base * root
            hi_ref[GROUP : GROUP + 8, lanes] = lifted
            hi_ref[GROUP + 8 : GROUP + 16, lanes] = lifted - lifted.astype(BF16).astype(F32)
            for h in range(2):
                if h != merged:
                    u, v, inv = [geo(q, h) for q in range(3)]
                    gu, gv = geo(3, h), geo(4, h)
                else:
                    u, v, inv = [geo(q, h) for q in range(3)]
                    gu, gv = geo(3, h) + au, geo(4, h) + av
                rows = pull(
                    u, v, depth * inv, u * v, 1.0 + u * u, 1.0 + v * v, gu * scale, gv * scale
                )
                for k, x in enumerate(rows):
                    g_ref[pl.ds(pl.multiple_of(f * GROUP + k * SLOTS + 8 * h, 8), 8), lanes] = x
                    hi_ref[k * SLOTS + 8 * h : k * SLOTS + 8 * h + 8, lanes] = x
        piece(g_ref, g_hbm, g_sems, f, GROUP).start()
        rows = pl.ds(pl.multiple_of(f * GROUP, 8), GROUP)
        q_ref[...] = block_ref[rows, :]
        for c, tile in enumerate(diagonal_rows(acc, merged)):
            at = slice(c * SLOTS + 8 * merged, c * SLOTS + 8 * merged + 8)
            q_ref[at, :] = q_ref[at, :] + tile
        g = hi_ref[...]
        top, low = pair_of(g)
        both = lax.dot_general(
            jnp.concatenate([top[0:GROUP], low[0:GROUP]], axis=0), top, (((1,), (1,)), ((), ())),
            preferred_element_type=F32,
        )
        m = both[0:GROUP, 0:GROUP] + both[GROUP:, 0:GROUP] + both[GROUP:, 0:GROUP].T
        vec = q_ref[:, LANES - 1 : LANES] - (
            both[0:GROUP, GROUP : GROUP + 1]
            + both[GROUP:, GROUP : GROUP + 1]
            + both[0:GROUP, GROUP + 8 : GROUP + 9]
        )
        q = q_ref[:, 0:GROUP] - m
        q_top, q_low = pair_of(q)
        b_top, b_low = pair_of(b_ref[rows, :])
        both = dot(jnp.concatenate([q_top, q_low], axis=0), b_top)
        w = both[0:GROUP] + both[GROUP:]
        w_ref[rows, 0:LANES] = jnp.where(
            iota((GROUP, LANES), 1) == LANES - 1, jnp.broadcast_to(vec, (GROUP, LANES)), w[:, 0:LANES]
        )
        w_ref[rows, LANES : 2 * LANES] = w[:, LANES : 2 * LANES] + dot(q_top, b_low[:, LANES : 2 * LANES])
        w_ref[rows, 2 * LANES :] = w[:, 2 * LANES :]
        return carry

    lax.fori_loop(0, 8, functools.partial(frame, merged=0), 0)
    lax.fori_loop(8, 16, functools.partial(frame, merged=1), 0)
    bt_copy.wait()
    bt_top, bt_low = pair_of(bt_ref[...])
    w_top, w_low = pair_of(w_ref[...])
    both = dot(jnp.concatenate([bt_top, bt_low], axis=0), w_top)
    t = both[0:192] + both[192:] + dot(bt_top, w_low)
    t_ref[...] = t
    for lo, hi, group, first in ((0, 48, 0, 48), (48, 144, 1, 0), (144, 192, 2, 0)):
        count = hi - lo
        lanes = slice(group * LANES, (group + 1) * LANES)
        square = jnp.concatenate(
            [jnp.zeros((first, LANES), F32)] * (first > 0)
            + [t[lo:hi, lanes], jnp.zeros((LANES - first - count, LANES), F32)],
            axis=0,
        )
        mean = 0.5 * (square + square.T)
        t_ref[lo:hi, lanes] = mean[first : first + count]
    last = iota((48, LANES), 1) == LANES - 1

    def half(core):
        own = slice(48 + 48 * core, 96 + 48 * core)
        rim = slice(0, 48) if core else slice(144, 192)
        group = 0 if core else 2
        mine = jnp.where(last, t[own, 0:LANES], t_ref[own, LANES : 2 * LANES])
        theirs = jnp.where(last, t[rim, 0:LANES], t_ref[rim, group * LANES : (group + 1) * LANES])
        far = t_ref[rim, LANES : 2 * LANES] if core else jnp.zeros((48, LANES), F32)
        return mine, t_ref[own, 2 * LANES :], theirs, far

    def put_half(ref, core):
        for k, x in enumerate(half(core)):
            ref[(k // 2) * 48 : (k // 2 + 1) * 48, (k % 2) * LANES : (k % 2 + 1) * LANES] = x

    @pl.when(core == 0)
    def _():
        put_half(keep_ref, 0)
        put_half(send_ref, 1)

    @pl.when(core == 1)
    def _():
        put_half(keep_ref, 1)
        put_half(send_ref, 0)

    for f in range(FD):
        piece(g_ref, g_hbm, g_sems, f, GROUP).wait()


def to_row(column):
    return jnp.sum(
        jnp.where(iota((GROUP, LANES), 0) == iota((GROUP, LANES), 1), column, 0.0),
        axis=0,
        keepdims=True,
    )


BLOCKS = 12


def place_kernel(where_ref, a_ref, b_ref, c_ref, d_ref, out_ref):
    at = where_ref[3]
    for k, ref in enumerate((a_ref, b_ref, c_ref, d_ref)):
        out_ref[pl.ds(pl.multiple_of(48 * (at ^ k), 8), 48), :] = ref[...]


SHRINK = 2.0**-15
FIRST = 2.0**-10
LARGEST_STEP = 1.001 / (POSE_REG * SHRINK)


def halves(x):
    t = 4097.0 * x
    top = t - (t - x)
    return top, x - top


def times(a, b):
    p = a * b
    ah, al = halves(a)
    bh, bl = halves(b)
    return p, ((ah * bh - p) + ah * bl + al * bh) + al * bl


def plus(a, b):
    t = a[0] + b[0]
    back = t - a[0]
    return t, (a[1] + b[1]) + ((a[0] - (t - back)) + (b[0] - back))


def tidy(a):
    t = a[0] + a[1]
    return t, a[1] - (t - a[0])


def mul(a, b):
    p, e = times(a[0], b[0])
    return tidy((p, e + (a[0] * b[1] + a[1] * b[0])))


def add(a, b):
    return tidy(plus(a, b))


def neg(a):
    return -a[0], -a[1]


def div(a, b):
    q = a[0] / b[0]
    rest = add(a, neg(mul((q, jnp.zeros_like(q)), b)))
    return tidy((q, rest[0] / b[0]))


def lane_total(a):
    for step in (64, 32, 16, 8, 4, 2, 1):
        a = plus(a, (pltpu.roll(a[0], step, 1), pltpu.roll(a[1], step, 1)))
    return a


def to_column(row):
    eye = iota((GROUP, LANES), 0) == iota((GROUP, LANES), 1)
    return jnp.broadcast_to(
        jnp.sum(jnp.where(eye, row, 0.0), axis=1, keepdims=True), (GROUP, LANES)
    )


def block_at(j):
    return pl.ds(pl.multiple_of(j * GROUP, 8), GROUP)


def tile_at(j):
    return pl.ds(pl.multiple_of(j * 8, 8), 8)


def product(s_ref, up_ref, high_ref, low_ref, j):
    acc = None
    sources = (
        (s_ref[block_at(j), 0:LANES], j),
        (s_ref[block_at(j - 1), LANES : 2 * LANES], j - 1),
        (up_ref[block_at(j), :], j + 1),
    )
    for s, at in sources:
        high = high_ref[block_at(at), :]
        p, e = times(s, high)
        e = e + s * low_ref[block_at(at), :]
        for r in range(0, GROUP, 8):
            term = p[r : r + 8], e[r : r + 8]
            acc = term if acc is None else plus(acc, term)
    for step in (4, 2, 1):
        acc = plus(acc, (pltpu.roll(acc[0], step, 0), pltpu.roll(acc[1], step, 0)))
    acc = tidy(acc)
    return acc[0] * SHRINK, acc[1] * SHRINK


def store_tile(ref, at, pair):
    row = iota((8, LANES), 0)
    ref[tile_at(at), :] = jnp.where(row == 0, pair[0], jnp.where(row == 1, pair[1], 0.0))


def powers(s_ref, up_ref, v_ref, cols, first, count, edge, base):
    for k in range(count):
        here, there = cols[k % 2], cols[1 - k % 2]

        def one(j, carry):
            pair = product(s_ref, up_ref, here[0], here[1], j)
            store_tile(v_ref, (first + k) * BLOCKS + j, pair)
            there[0][block_at(j), :] = to_column(pair[0][0:1])
            there[1][block_at(j), :] = to_column(pair[1][0:1])
            return carry

        lax.fori_loop(base + k * edge, BLOCKS - base - k * edge, one, 0)


def first_kernel(
    where_ref, p_ref, c_ref, n_ref, p2_ref, c2_ref, n2_ref,
    s_ref, up_ref, v_ref, v4_ref, h0_ref, l0_ref, h1_ref, l1_ref,
):
    core = where_ref[2]
    mine = pl.multiple_of(48 * core, 8)
    theirs = pl.multiple_of(48 - 48 * core, 8)
    diagonal = iota((GROUP, LANES), 0) == iota((GROUP, LANES), 1)
    lane = iota((GROUP, LANES), 1)
    for j in range(BLOCKS):
        rows = slice((j % 4) * 48, (j % 4 + 1) * 48)
        a = (p_ref, c_ref, n_ref)[j // 4]
        b = (p2_ref, c2_ref, n2_ref)[j // 4]
        s_ref[pl.ds(j * GROUP + mine, 48), :] = a[rows, :]
        s_ref[pl.ds(j * GROUP + theirs, 48), :] = b[rows, :]
    zero = jnp.zeros((LANES - GROUP, LANES), F32)

    def prepare(j, carry):
        own = s_ref[block_at(j), 0:LANES]
        rhs = jnp.broadcast_to(own[:, LANES - 1 : LANES], (GROUP, LANES)) * FIRST
        h0_ref[block_at(j), :] = rhs
        l0_ref[block_at(j), :] = jnp.zeros_like(rhs)
        store_tile(v_ref, j, (to_row(rhs), jnp.zeros((1, LANES), F32)))
        s_ref[block_at(j), 0:LANES] = jnp.where(lane < GROUP, own, 0.0) + jnp.where(
            diagonal, POSE_REG, 0.0
        )
        up = jnp.concatenate([s_ref[block_at(j), LANES : 2 * LANES], zero], axis=0).T
        up_ref[block_at(j), :] = up[0:GROUP]
        return carry

    lax.fori_loop(0, BLOCKS, prepare, 0)
    cols = ((h0_ref, l0_ref), (h1_ref, l1_ref))
    powers(s_ref, up_ref, v_ref, cols, 1, 4, 1, 1)
    for j in range(4):
        at = (4 * BLOCKS + 4 + j) * 8
        v4_ref[j : j + 1, :] = v_ref[at : at + 1, :]
        v4_ref[4 + j : 5 + j, :] = v_ref[at + 1 : at + 2, :]


def second_kernel(
    s_ref, up_ref, v_ref, below_ref, own_ref, above_ref, out_ref, v45_ref,
    h0_ref, l0_ref, h1_ref, l1_ref,
):
    for g, ref in enumerate((below_ref, own_ref, above_ref)):
        for j in range(4):
            pair = ref[j : j + 1, :], ref[4 + j : 5 + j, :]
            at = g * 4 + j
            store_tile(v45_ref, at, pair)
            if 1 < at < 10:
                h0_ref[block_at(at), :] = to_column(pair[0])
                l0_ref[block_at(at), :] = to_column(pair[1])
    cols = ((h0_ref, l0_ref), (h1_ref, l1_ref))
    powers(s_ref, up_ref, v45_ref, cols, 1, 2, 1, 3)
    zero = jnp.zeros((1, LANES), F32)
    total = None
    for j in range(4, 8):

        def row(k, part):
            ref, at = (v_ref, k) if k < 4 else (v45_ref, k - 4)
            at = (at * BLOCKS + j) * 8 + part
            return ref[at : at + 1, :]

        def stack(pick, part):
            lines = [row(pick(m), part) for m in range(2 * ITERS)]
            return jnp.concatenate(lines + [zero] * (16 - len(lines)), axis=0)

        lower, upper = (lambda m: m // 2), (lambda m: m - m // 2)
        a, b = (stack(lower, 0), stack(lower, 1)), (stack(upper, 0), stack(upper, 1))
        p, e = times(a[0], b[0])
        term = p, e + (a[0] * b[1] + a[1] * b[0])
        total = term if total is None else plus(total, term)
    total = tidy(lane_total(total))
    diagonal = iota((16, LANES), 0) == iota((16, LANES), 1)
    put(
        out_ref,
        [jnp.sum(jnp.where(diagonal, x, 0.0), axis=0, keepdims=True) for x in total],
    )


def put(ref, pair):
    ref[...] = jnp.zeros((8, LANES), F32)
    ref[0:1, :] = pair[0]
    ref[1:2, :] = pair[1]


def gather_sum(refs):
    acc = refs[0][0:1, :], refs[0][1:2, :]
    for r in refs[1:]:
        acc = plus(acc, (r[0:1, :], r[1:2, :]))
    return tidy(acc)


def sum_kernel(a_ref, b_ref, c_ref, d_ref, out_ref):
    put(out_ref, gather_sum((a_ref, b_ref, c_ref, d_ref)))


def solve_kernel(
    where_ref, a_ref, b_ref, c_ref, d_ref, v_ref, v45_ref, base_ref, scale_ref, move_hbm, g_hbm,
    pose_ref, out_ref, sum_ref, move_ref, g_ref, sems,
):
    copies = [
        pltpu.make_async_copy(move_hbm, move_ref, sems.at[0]),
        pltpu.make_async_copy(g_hbm, g_ref, sems.at[1]),
    ]
    for copy in copies:
        copy.start()
    at_quad = where_ref[3]
    total = gather_sum((a_ref, b_ref, c_ref, d_ref))
    shape = (8, LANES)
    row = iota(shape, 0)
    lane = iota(shape, 1)
    zero = jnp.zeros(shape, F32)
    unit = jnp.where((row == 1) & (lane == LANES - 1), 1.0, 0.0)

    def where(live, a, b):
        return jnp.where(live, a[0], b[0]), jnp.where(live, a[1], b[1])

    def at(a, r, k):
        return tuple(jnp.broadcast_to(x[r : r + 1, k : k + 1], shape) for x in a)

    x = jnp.where(row == 0, total[0], unit), jnp.where(row == 0, total[1], 0.0)
    y = x
    found = (zero, zero)
    one = (zero + 1.0, zero)
    start = at(x, 0, 0)
    now = start
    lead = one[0]
    live = start[0] > 0.0
    for k in range(ITERS):
        alpha = div(now, where(live, at(y, 0, k + 1), one))
        live = live & (alpha[0] > 0.0) & (alpha[0] < LARGEST_STEP)
        alpha = where(live, alpha, (zero, zero))
        found = add(found, mul(alpha, y))
        if k + 1 == ITERS:
            break
        back = neg(alpha)
        moved = tuple(pltpu.roll(p, LANES - 1, 1) for p in y)
        x = add(x, mul(back, moved))
        fresh = at(x, 0, k + 1)
        lead = -lead * alpha[0]
        live = live & (lead * fresh[0] > 1e-11 * start[0])
        beta = div(mul(back, fresh), where(live, now, one))
        beta = where(live, beta, (zero, zero))
        y = add(x, mul(beta, y))
        now = fresh
    xc = [tuple(p[1:2, LANES - 1 - k : LANES - k] for p in found) for k in range(ITERS)]
    poses = []
    for g in range(3):
        acc = None
        for k in range(ITERS):
            ref = v_ref if k < 4 else v45_ref
            tile = ref[tile_at((k if k < 4 else k - 4) * BLOCKS + 3 + at_quad + g), :]
            wide = tuple(jnp.broadcast_to(x, (1, LANES)) for x in xc[k])
            term = mul(wide, (tile[0:1], tile[1:2]))
            acc = term if acc is None else plus(acc, term)
        poses.append((acc[0] + acc[1]) * (SHRINK / FIRST))
    column = to_column(poses[1])
    r = iota((GROUP, LANES), 0)
    l = iota((GROUP, LANES), 1)
    for c in range(6):
        line = jnp.sum(jnp.where(r == l * 6 + c, column, 0.0), axis=0, keepdims=True)
        pose_ref[c : c + 1, :] = line[:, 0:FD]
    for copy in copies:
        copy.wait()

    def frame(f, carry):
        rows = pl.ds(pl.multiple_of(f * GROUP, 8), GROUP)
        prod = (
            move_ref[rows, 0:LANES] * poses[0]
            + move_ref[rows, LANES : 2 * LANES] * poses[1]
            + move_ref[rows, 2 * LANES : 3 * LANES] * poses[2]
        )
        x = jnp.sum(prod, axis=1, keepdims=True)
        image = jnp.sum(g_ref[rows, :] * x, axis=0, keepdims=True)
        at = tile_at(f)
        sum_ref[at, :] = base_ref[at, :] - scale_ref[at, :] * image
        return carry

    lax.fori_loop(0, FD, frame, 0)
    for f in range(FD):
        out_ref[f : f + 1, :] = sum_ref[f * 8 : f * 8 + 1, :]


SMEM = pl.BlockSpec(memory_space=pltpu.SMEM)
VMEM = pl.BlockSpec(memory_space=pltpu.VMEM)
ANY = pl.BlockSpec(memory_space=pl.ANY)


def call(kernel, name, outs, smem, *args, scratch=(), hbm=0, hbm_out=0):
    return pl.pallas_call(
        kernel,
        name=name,
        out_shape=[jax.ShapeDtypeStruct(s, F32) for s in outs],
        in_specs=[SMEM] * smem + [VMEM] * (len(args) - smem - hbm) + [ANY] * hbm,
        out_specs=[VMEM] * (len(outs) - hbm_out) + [ANY] * hbm_out,
        scratch_shapes=list(scratch),
    )(*args)


def per_device(edge_frames, rotvec, trans, inv_depth, depth_damping, flow, weight, mask):
    f_dev, plocal = inv_depth.shape
    count = lax.axis_size("frames")
    pixes = lax.axis_size("pix")
    fi = lax.axis_index("frames")
    pi = lax.axis_index("pix")
    spot = jnp.stack([fi * f_dev, pi * plocal, pi % 2, fi % 4]).astype(jnp.int32)

    def shift(block, step):
        return lax.ppermute(
            block, "frames", [(i, i + step) for i in range(count) if 0 <= i + step < count]
        )

    edges = (edge_frames, flow.transpose(1, 0, 2), weight.transpose(1, 0, 2), mask)
    down, up = call(
        rim_kernel, "rim", [(8 + 4 * SIDE, plocal), (4 * SIDE, plocal)], 1, spot, *edges
    )
    from_after = shift(down, -1)
    from_before = shift(up, 1)
    (own,) = call(own_kernel, "own", [(4 * f_dev * SLOTS, plocal)], 1, spot, *edges)
    tab, b, bt = call(
        pose_kernel, "pose",
        [(f_dev * SLOTS, LANES), (f_dev * GROUP, 3 * LANES), (192, f_dev * GROUP)],
        1, spot, rotvec, trans,
    )
    pairs = f_dev * SLOTS
    geo, curv, grad, block = call(
        early_kernel, "early",
        [(5 * pairs, plocal), (f_dev * 8, plocal), (f_dev * 8, plocal), (f_dev * GROUP, LANES)],
        1, spot, own, inv_depth, tab, scratch=[pltpu.VMEM((f_dev * 8, plocal), F32)],
    )
    keep, send, base, scale, g = call(
        main_kernel, "main",
        [(96, 256), (96, 256), (f_dev * 8, plocal), (f_dev * 8, plocal), (f_dev * GROUP, plocal)],
        1, spot, from_after, from_before, curv, grad, block, inv_depth, depth_damping, tab, geo, b, bt,
        hbm=3, hbm_out=1,
        scratch=[
            pltpu.VMEM((4 * FD * 8, plocal), F32),
            pltpu.VMEM((GROUP + 16, plocal), F32),
            pltpu.VMEM((256, plocal), F32),
            pltpu.VMEM((GROUP, LANES), F32),
            pltpu.VMEM((f_dev * GROUP, 3 * LANES), F32),
            pltpu.VMEM((192, 3 * LANES), F32),
            pltpu.VMEM((5 * pairs, plocal), F32),
            pltpu.VMEM((f_dev * GROUP, 3 * LANES), F32),
            pltpu.VMEM((192, f_dev * GROUP), F32),
            pltpu.VMEM((f_dev * GROUP, plocal), F32),
            pltpu.SemaphoreType.DMA((f_dev,)),
            pltpu.SemaphoreType.DMA((f_dev,)),
            pltpu.SemaphoreType.DMA((f_dev,)),
            pltpu.SemaphoreType.DMA((1,)),
        ],
    )
    got = lax.ppermute(send, "pix", [(i, i ^ 1) for i in range(pixes)])
    both = keep + got
    own_half, rim = both[:48], both[48:]
    both_axes = ("frames", "pix")

    def to_neighbour(flip):
        route = []
        for i in range(count):
            for k in range(pixes):
                to = i + 1 if k % 2 == 0 else i - 1
                if 0 <= to < count:
                    route.append((i * pixes + k, to * pixes + (k ^ flip)))
        return lax.ppermute(rim, both_axes, route)

    own_far = lax.ppermute(own_half, "pix", [(i, i ^ 2) for i in range(pixes)])
    rim_near = to_neighbour(0)
    rim_far = to_neighbour(2)
    half = (own_half + own_far) + (rim_near + rim_far)

    def mates(v, step):
        return [v] + [
            lax.ppermute(v, "frames", [(i, i ^ (k * step)) for i in range(count)]) for k in (1, 2, 3)
        ]

    def twin(v):
        return lax.ppermute(v, "pix", [(i, i ^ 1) for i in range(pixes)])

    def halo(v):
        return shift(v, 4), v, shift(v, -4)

    (quad,) = call(place_kernel, "place", [(192, 256)], 1, spot, *mates(half, 1))
    pieces = halo(quad)
    wide = BLOCKS * GROUP
    scratch = [pltpu.VMEM((wide, LANES), F32)] * 4
    s, up, vs, v4 = call(
        first_kernel, "first",
        [(wide, 256), (wide, LANES), (5 * BLOCKS * 8, LANES), (8, LANES)],
        1, spot, *pieces, *[twin(x) for x in pieces], scratch=scratch,
    )
    part, v45 = call(
        second_kernel, "second", [(8, LANES), (3 * BLOCKS * 8, LANES)], 0, s, up, vs, *halo(v4),
        scratch=scratch,
    )
    (part,) = call(sum_kernel, "sum", [(8, LANES)], 0, *mates(part, 4))
    pose_step, depth_step = call(
        solve_kernel, "solve", [(6, f_dev), (f_dev, plocal)], 1, spot, *mates(part, 16), vs, v45,
        base, scale, b, g,
        scratch=[
            pltpu.VMEM((f_dev * 8, plocal), F32),
            pltpu.VMEM((f_dev * GROUP, 3 * LANES), F32),
            pltpu.VMEM((f_dev * GROUP, plocal), F32),
            pltpu.SemaphoreType.DMA((2,)),
        ],
        hbm=2,
    )
    return pose_step, depth_step


def solution(mesh):
    return jax.shard_map(
        per_device,
        mesh=mesh,
        in_specs=(
            P(None, "frames"),
            P(),
            P(),
            P("frames", "pix"),
            P("frames", "pix"),
            P("frames", None, "pix"),
            P("frames", None, "pix"),
            P("frames", "pix"),
        ),
        out_specs=(P(None, "frames"), P("frames", "pix")),
        check_vma=False,
    )
```

```python
import functools
import jax
import jax.numpy as jnp
from jax import lax
from jax.experimental import pallas as pl
from jax.experimental.pallas import tpu as pltpu
from jax.sharding import PartitionSpec as P

ROWS = 48
COLS = 64
RADIUS = 8
ITERS = 6
HIGHEST = lax.Precision.HIGHEST
F32 = jnp.float32
BF16 = jnp.bfloat16
LANES = 128
FD = 16
SLOTS = 16
GROUP = FD * 6
SIDE = RADIUS * (RADIUS + 1) // 2
POSE_REG = 100.0


def iota(shape, dim):
    return lax.broadcasted_iota(jnp.int32, shape, dim)


def thirds(x):
    first = x.astype(BF16)
    rest = x - first.astype(F32)
    second = rest.astype(BF16)
    return first, second, (rest - second.astype(F32)).astype(BF16)


def pair_of(x):
    first = x.astype(BF16)
    return first, (x - first.astype(F32)).astype(BF16)


def dot(a, b):
    return jnp.dot(a, b, preferred_element_type=F32)


def spread(where_ref, ef_ref, flow_ref, weight_ref, mask_ref, rims, write):
    edges = ef_ref.shape[1]
    start = where_ref[0]
    source = ef_ref[0:1, :] - start
    delta = ef_ref[1:2, :] - start - source
    slot = jnp.where(delta < 0, delta + 8, delta + 7)
    if rims:
        j = source + 8
        down_at = jnp.where(source < 0, ((j * (j + 1)) >> 1) + delta - 8 + j, -1)
        j = 23 - source
        up_at = jnp.where(source >= FD, ((j * (j + 1)) >> 1) + slot, -1)
        row = iota((40, edges), 0)
        hot = jnp.concatenate([(row == down_at).astype(F32), (row == up_at).astype(F32)], axis=0)
    else:
        own_at = jnp.where((source >= 0) & (source < FD), source * SLOTS + slot, -1)
        hot = (iota((FD * SLOTS, edges), 0) == own_at).astype(F32)
    hot = hot.astype(BF16)
    for chunk in range(mask_ref.shape[1] // LANES):
        lanes = pl.ds(chunk * LANES, LANES)
        live = mask_ref[:, lanes].astype(F32)
        parts = []
        for comp in range(2):
            conf = weight_ref[comp, :, lanes] * live
            parts.append((conf, conf * flow_ref[comp, :, lanes]))
        values = jnp.concatenate([parts[0][0], parts[1][0], parts[0][1], parts[1][1]], axis=1)
        got = sum(dot(hot, piece) for piece in reversed(thirds(values)))
        for q in range(4):
            write(q, lanes, got[:, q * LANES : (q + 1) * LANES])


def rim_kernel(where_ref, ef_ref, flow_ref, weight_ref, mask_ref, down_ref, up_ref):
    down_ref[0:8, :] = jnp.zeros((8, down_ref.shape[1]), F32)

    def write(q, lanes, cut):
        down_ref[8 + q * SIDE : 8 + (q + 1) * SIDE, lanes] = cut[0:SIDE]
        up_ref[q * SIDE : (q + 1) * SIDE, lanes] = cut[40 : 40 + SIDE]

    spread(where_ref, ef_ref, flow_ref, weight_ref, mask_ref, True, write)


def own_kernel(where_ref, ef_ref, flow_ref, weight_ref, mask_ref, own_ref):
    def write(q, lanes, cut):
        own_ref[q * 256 : (q + 1) * 256, lanes] = cut

    spread(where_ref, ef_ref, flow_ref, weight_ref, mask_ref, False, write)


def rotation_rows(w):
    x, y, z = w
    zero = jnp.zeros_like(x)
    cross = [[zero, -z, y], [z, zero, -x], [-y, x, zero]]
    sq = x * x + y * y + z * z
    first = 1.0 - sq / 6.0 + sq * sq / 120.0
    second = 0.5 - sq / 24.0 + sq * sq / 720.0
    return [
        [
            float(i == k)
            + first * cross[i][k]
            + second * sum(cross[i][m] * cross[m][k] for m in range(3))
            for k in range(3)
        ]
        for i in range(3)
    ]


def pose_kernel(where_ref, rotvec_ref, trans_ref, tab_ref, b_ref, bt_ref):
    start = where_ref[0]
    frames = rotvec_ref.shape[1]
    pair = iota((1, FD * SLOTS), 1)
    slot = pair & 15
    delta = jnp.where(slot < 8, slot - 8, slot - 7)
    at_source = start + (pair >> 4)
    at_target = jnp.clip(at_source + delta, 0, frames - 1)
    poses = jnp.concatenate([rotvec_ref[...], trans_ref[...], jnp.zeros((2, frames), F32)], axis=0)

    def pick(at):
        hot = (iota((frames, FD * SLOTS), 0) == at).astype(F32)
        return jnp.dot(poses, hot, precision=HIGHEST, preferred_element_type=F32)

    src = pick(at_source)
    tgt = pick(at_target)
    rs = rotation_rows([src[k : k + 1] for k in range(3)])
    rt = rotation_rows([tgt[k : k + 1] for k in range(3)])
    rel = [[sum(rt[i][k] * rs[m][k] for k in range(3)) for m in range(3)] for i in range(3)]
    tr = [
        tgt[3 + i : 4 + i] - sum(rel[i][m] * src[3 + m : 4 + m] for m in range(3)) for i in range(3)
    ]
    corner = [
        [tr[1] * rel[2][m] - tr[2] * rel[1][m] for m in range(3)],
        [tr[2] * rel[0][m] - tr[0] * rel[2][m] for m in range(3)],
        [tr[0] * rel[1][m] - tr[1] * rel[0][m] for m in range(3)],
    ]
    lines = [x for row in rel for x in row] + tr + [x for row in corner for x in row]
    lines = jnp.concatenate(lines + [jnp.zeros((LANES - len(lines), FD * SLOTS), F32)], axis=0)
    tab_ref[...] = lines.T

    lane3 = iota((SLOTS, 3 * LANES), 1)
    row3 = iota((SLOTS, 3 * LANES), 0)
    off3 = jnp.where(row3 < 8, row3 - 8, row3 - 7)

    def build(f, carry):
        frame = f + off3 + FD
        home = (frame >> 4) * LANES + (frame & 15) * 6
        tab = tab_ref[pl.ds(pl.multiple_of(f * SLOTS, SLOTS), SLOTS), :]
        for c in range(6):
            block = jnp.where(lane3 == home + c, 1.0, 0.0)
            for d in range(6):
                if c < 3:
                    at = c * 3 + d if d < 3 else 12 + c * 3 + d - 3
                elif d >= 3:
                    at = (c - 3) * 3 + d - 3
                else:
                    continue
                block = block - jnp.where(
                    lane3 == LANES + f * 6 + d, jnp.broadcast_to(tab[:, at : at + 1], lane3.shape), 0.0
                )
            b_ref[pl.ds(pl.multiple_of(f * GROUP + c * SLOTS, SLOTS), SLOTS), :] = block
        return carry

    lax.fori_loop(0, FD, build, 0)
    for g in range(4):
        cols = slice(g * 384, (g + 1) * 384)
        below = b_ref[cols, 0:LANES].T
        own = b_ref[cols, LANES : 2 * LANES].T
        above = b_ref[cols, 2 * LANES : 3 * LANES].T
        bt_ref[0:48, cols] = below[48:96]
        bt_ref[48:144, cols] = own[0:96]
        bt_ref[144:192, cols] = above[0:48]


def coords(first, chunk):
    pixel = first + chunk * LANES + iota((8, LANES), 1)
    col = ((pixel & (COLS - 1)).astype(F32) - 0.5 * (COLS - 1)) / COLS
    line = ((pixel >> 6).astype(F32) - 0.5 * (ROWS - 1)) / COLS
    return col, line


def pull(u, v, s, uv, u1, v1, pu, pv):
    spu = s * pu
    spv = s * pv
    return (
        spu,
        spv,
        -(u * spu + v * spv),
        -(uv * pu) - v1 * pv,
        u1 * pu + uv * pv,
        u * pv - v * pu,
    )


def pose_sums(u, v, s, cu, cv, eu, ev):
    uv = u * v
    u1 = 1.0 + u * u
    v1 = 1.0 + v * v
    terms = list(pull(u, v, s, uv, u1, v1, -eu, -ev))
    su_ = cu * s
    sv_ = cv * s
    ju = (-uv, u1, -v)
    jv = (-v1, uv, u)
    a00 = su_ * s
    a11 = sv_ * s
    a02 = -(a00 * u)
    a12 = -(a11 * v)
    terms += [a00, a11, a02, a12, -(a02 * u + a12 * v)]
    tu = [su_ * x for x in ju]
    tv = [sv_ * x for x in jv]
    terms += tu + tv
    terms += [-(u * x + v * y) for x, y in zip(tu, tv)]
    wu = [cu * x for x in ju]
    wv = [cv * x for x in jv]
    for a in range(3):
        for b in range(a, 3):
            terms.append(wu[a] * ju[b] + wv[a] * jv[b])
    return terms


def diagonal_rows(acc, h):
    lane = iota((8, LANES), 1)
    row = iota((8, LANES), 0)
    sums = [jnp.broadcast_to(jnp.sum(x, axis=1, keepdims=True), (8, LANES)) for x in acc]
    a = {(0, 0): 6, (1, 1): 7, (0, 2): 8, (1, 2): 9, (2, 2): 10}
    for k in range(3):
        a[(0, 3 + k)] = 11 + k
        a[(1, 3 + k)] = 14 + k
        a[(2, 3 + k)] = 17 + k
    at = 20
    for x in range(3):
        for y in range(x, 3):
            a[(3 + x, 3 + y)] = at
            at += 1
    tiles = []
    for c in range(6):
        tile = jnp.where(lane == LANES - 1, sums[c], 0.0)
        for d in range(6):
            key = (min(c, d), max(c, d))
            if key != (0, 1):
                tile = jnp.where(lane == d * SLOTS + 8 * h + row, sums[a[key]], tile)
        tiles.append(tile)
    return tiles


def early_kernel(
    where_ref, own_ref, depth_ref, tab_ref, geo_ref, curv_ref, grad_ref, block_ref, in_ref
):
    plocal = depth_ref.shape[1]
    chunks = plocal // LANES
    for f in range(FD):
        in_ref[f * 8 : f * 8 + 8, :] = jnp.broadcast_to(depth_ref[f : f + 1, :], (8, plocal))

    def frame(f, carry):
        eight = pl.ds(pl.multiple_of(f * 8, 8), 8)
        for h in range(2):
            tab = tab_ref[pl.ds(pl.multiple_of(f * SLOTS + 8 * h, 8), 8), :]
            r = [jnp.broadcast_to(tab[:, k : k + 1], (8, LANES)) for k in range(12)]
            acc = [0.0] * 26
            for c in range(chunks):
                lanes = pl.ds(c * LANES, LANES)
                col, line = coords(where_ref[1], c)
                depth = in_ref[eight, lanes]

                def at(q):
                    return pl.ds(pl.multiple_of(q * 256 + f * SLOTS + 8 * h, 8), 8)

                cu, cv, fu, fv = [own_ref[at(q), lanes] for q in range(4)]
                inv = 1.0 / (r[6] * col + r[7] * line + r[8] + depth * r[11])
                u = (r[0] * col + r[1] * line + r[2] + depth * r[9]) * inv
                v = (r[3] * col + r[4] * line + r[5] + depth * r[10]) * inv
                su = inv * (r[9] - u * r[11])
                sv = inv * (r[10] - v * r[11])
                eu = cu * (col - u) + fu
                ev = cv * (line - v) + fv
                au = cu * su
                av = cv * sv
                curv = au * su + av * sv
                grad = -(su * eu + sv * ev)
                if h:
                    curv = curv + curv_ref[eight, lanes]
                    grad = grad + grad_ref[eight, lanes]
                curv_ref[eight, lanes] = curv
                grad_ref[eight, lanes] = grad
                for q, x in enumerate((u, v, inv, au, av)):
                    row = pl.multiple_of((f * 5 + q) * SLOTS + 8 * h, 8)
                    geo_ref[pl.ds(row, 8), lanes] = x
                acc = [x + y for x, y in zip(acc, pose_sums(u, v, depth * inv, cu, cv, eu, ev))]
            for c, tile in enumerate(diagonal_rows(acc, h)):
                block_ref[pl.ds(pl.multiple_of(f * GROUP + c * SLOTS + 8 * h, 8), 8), :] = tile
        return carry

    lax.fori_loop(0, FD, frame, 0)


def main_kernel(
    where_ref, rdown_ref, rup_ref, curv_ref, grad_ref, block_ref, depth_ref, damp_ref, tab_ref,
    geo_hbm, b_hbm, bt_hbm,
    keep_ref, send_ref, base_ref, scale_ref, g_hbm,
    half_ref, hi0_ref, hi1_ref, in_ref, q0_ref, q1_ref, w_ref, t_ref, geo_ref, b_ref, bt_ref, g_ref,
    geo_sems, b_sems, g_sems, bt_sem,
):
    def piece(src, dst, sems, f, rows):
        at = pl.ds(pl.multiple_of(f * rows, 8), rows)
        return pltpu.make_async_copy(src.at[at, :], dst.at[at, :], sems.at[f])

    for f in range(FD):
        piece(geo_hbm, geo_ref, geo_sems, f, 5 * SLOTS).start()
        piece(b_hbm, b_ref, b_sems, f, GROUP).start()
    bt_copy = pltpu.make_async_copy(bt_hbm, bt_ref, bt_sem.at[0])
    bt_copy.start()
    core = where_ref[2]
    plocal = depth_ref.shape[1]
    chunks = plocal // LANES
    row8 = iota((8, plocal), 0)
    for f in range(FD):
        j = 7 - f if f < 8 else f - 8
        base = j * (j + 1) // 2
        for q in range(4):
            if f < 8:
                first = q * SIDE + base
                extra = jnp.where(row8 <= j, rup_ref[first : first + 8, :], 0.0)
            else:
                first = 8 + q * SIDE + base - 7 + j
                extra = jnp.where(row8 >= 7 - j, rdown_ref[first : first + 8, :], 0.0)
            half_ref[(q * FD + f) * 8 : (q * FD + f + 1) * 8, :] = extra
        in_ref[f * 8 : f * 8 + 8, :] = jnp.broadcast_to(depth_ref[f : f + 1, :], (8, plocal))
        in_ref[128 + f * 8 : 136 + f * 8, :] = jnp.broadcast_to(damp_ref[f : f + 1, :], (8, plocal))
    lane = iota((8, LANES), 1)

    def tiles(f, merged, hi_ref, q_ref):
        eight = pl.ds(pl.multiple_of(f * 8, 8), 8)
        tab = tab_ref[pl.ds(pl.multiple_of(f * SLOTS + 8 * merged, 8), 8), :]
        t0, t1, t2 = [jnp.broadcast_to(tab[:, k : k + 1], (8, LANES)) for k in (9, 10, 11)]
        acc = [0.0] * 26
        for c in range(chunks):
            lanes = pl.ds(c * LANES, LANES)
            col, line = coords(where_ref[1], c)
            depth = in_ref[eight, lanes]

            def geo(q, h):
                return geo_ref[pl.ds(pl.multiple_of((f * 5 + q) * SLOTS + 8 * h, 8), 8), lanes]

            cu, cv, fu, fv = [
                half_ref[pl.ds(pl.multiple_of((q * FD + f) * 8, 8), 8), lanes] for q in range(4)
            ]
            u, v, inv = [geo(q, merged) for q in range(3)]
            su = inv * (t0 - u * t2)
            sv = inv * (t1 - v * t2)
            eu = cu * (col - u) + fu
            ev = cv * (line - v) + fv
            au = cu * su
            av = cv * sv
            acc = [x + y for x, y in zip(acc, pose_sums(u, v, depth * inv, cu, cv, eu, ev))]
            curv = curv_ref[eight, lanes] + (au * su + av * sv)
            grad = grad_ref[eight, lanes] - (su * eu + sv * ev)
            total = in_ref[pl.ds(pl.multiple_of(128 + f * 8, 8), 8), lanes] + jnp.sum(
                curv, axis=0, keepdims=True
            )
            base = jnp.sum(grad, axis=0, keepdims=True) / total
            root = jnp.sqrt(total)
            scale = 1.0 / root
            base_ref[eight, lanes] = base
            scale_ref[eight, lanes] = scale
            lifted = base * root
            hi_ref[GROUP : GROUP + 8, lanes] = lifted
            hi_ref[GROUP + 8 : GROUP + 16, lanes] = lifted - lifted.astype(BF16).astype(F32)
            for h in range(2):
                if h != merged:
                    u, v, inv = [geo(q, h) for q in range(3)]
                    gu, gv = geo(3, h), geo(4, h)
                else:
                    u, v, inv = [geo(q, h) for q in range(3)]
                    gu, gv = geo(3, h) + au, geo(4, h) + av
                rows = pull(
                    u, v, depth * inv, u * v, 1.0 + u * u, 1.0 + v * v, gu * scale, gv * scale
                )
                for k, x in enumerate(rows):
                    g_ref[pl.ds(pl.multiple_of(f * GROUP + k * SLOTS + 8 * h, 8), 8), lanes] = x
                    hi_ref[k * SLOTS + 8 * h : k * SLOTS + 8 * h + 8, lanes] = x
        q_ref[...] = block_ref[pl.ds(pl.multiple_of(f * GROUP, 8), GROUP), :]
        for c, tile in enumerate(diagonal_rows(acc, merged)):
            at = slice(c * SLOTS + 8 * merged, c * SLOTS + 8 * merged + 8)
            q_ref[at, :] = q_ref[at, :] + tile

    def matmuls(f, hi_ref, q_ref):
        rows = pl.ds(pl.multiple_of(f * GROUP, 8), GROUP)
        g = hi_ref[...]
        top, low = pair_of(g)
        both = lax.dot_general(
            jnp.concatenate([top[0:GROUP], low[0:GROUP]], axis=0), top, (((1,), (1,)), ((), ())),
            preferred_element_type=F32,
        )
        m = both[0:GROUP, 0:GROUP] + both[GROUP:, 0:GROUP] + both[GROUP:, 0:GROUP].T
        vec = q_ref[:, LANES - 1 : LANES] - (
            both[0:GROUP, GROUP : GROUP + 1]
            + both[GROUP:, GROUP : GROUP + 1]
            + both[0:GROUP, GROUP + 8 : GROUP + 9]
        )
        q = q_ref[:, 0:GROUP] - m
        q_top, q_low = pair_of(q)
        b_top, b_low = pair_of(b_ref[rows, :])
        both = dot(jnp.concatenate([q_top, q_low], axis=0), b_top)
        w = both[0:GROUP] + both[GROUP:]
        w_ref[rows, 0:LANES] = jnp.where(
            iota((GROUP, LANES), 1) == LANES - 1, jnp.broadcast_to(vec, (GROUP, LANES)), w[:, 0:LANES]
        )
        w_ref[rows, LANES : 2 * LANES] = w[:, LANES : 2 * LANES] + dot(q_top, b_low[:, LANES : 2 * LANES])
        w_ref[rows, 2 * LANES :] = w[:, 2 * LANES :]

    def frames(i, carry, merged):
        work = ((2 * i, hi0_ref, q0_ref), (2 * i + 1, hi1_ref, q1_ref))
        for f, _, _ in work:
            piece(geo_hbm, geo_ref, geo_sems, f, 5 * SLOTS).wait()
            piece(b_hbm, b_ref, b_sems, f, GROUP).wait()
        for f, hi_ref, q_ref in work:
            tiles(f, merged, hi_ref, q_ref)
        for f, hi_ref, q_ref in work:
            matmuls(f, hi_ref, q_ref)
        for f, _, _ in work:
            piece(g_ref, g_hbm, g_sems, f, GROUP).start()
        return carry

    lax.fori_loop(0, 4, functools.partial(frames, merged=0), 0)
    lax.fori_loop(4, 8, functools.partial(frames, merged=1), 0)
    bt_copy.wait()
    bt_top, bt_low = pair_of(bt_ref[...])
    w_top, w_low = pair_of(w_ref[...])
    both = dot(jnp.concatenate([bt_top, bt_low], axis=0), w_top)
    t = both[0:192] + both[192:] + dot(bt_top, w_low)
    t_ref[...] = t
    for lo, hi, group, first in ((0, 48, 0, 48), (48, 144, 1, 0), (144, 192, 2, 0)):
        count = hi - lo
        lanes = slice(group * LANES, (group + 1) * LANES)
        square = jnp.concatenate(
            [jnp.zeros((first, LANES), F32)] * (first > 0)
            + [t[lo:hi, lanes], jnp.zeros((LANES - first - count, LANES), F32)],
            axis=0,
        )
        mean = 0.5 * (square + square.T)
        t_ref[lo:hi, lanes] = mean[first : first + count]
    last = iota((48, LANES), 1) == LANES - 1

    def half(core):
        own = slice(48 + 48 * core, 96 + 48 * core)
        rim = slice(0, 48) if core else slice(144, 192)
        group = 0 if core else 2
        mine = jnp.where(last, t[own, 0:LANES], t_ref[own, LANES : 2 * LANES])
        theirs = jnp.where(last, t[rim, 0:LANES], t_ref[rim, group * LANES : (group + 1) * LANES])
        far = t_ref[rim, LANES : 2 * LANES] if core else jnp.zeros((48, LANES), F32)
        return mine, t_ref[own, 2 * LANES :], theirs, far

    def put_half(ref, core):
        for k, x in enumerate(half(core)):
            ref[(k // 2) * 48 : (k // 2 + 1) * 48, (k % 2) * LANES : (k % 2 + 1) * LANES] = x

    @pl.when(core == 0)
    def _():
        put_half(keep_ref, 0)
        put_half(send_ref, 1)

    @pl.when(core == 1)
    def _():
        put_half(keep_ref, 1)
        put_half(send_ref, 0)

    for f in range(FD):
        piece(g_ref, g_hbm, g_sems, f, GROUP).wait()


def to_row(column):
    return jnp.sum(
        jnp.where(iota((GROUP, LANES), 0) == iota((GROUP, LANES), 1), column, 0.0),
        axis=0,
        keepdims=True,
    )


BLOCKS = 12


def place_kernel(where_ref, a_ref, b_ref, c_ref, d_ref, out_ref):
    at = where_ref[3]
    for k, ref in enumerate((a_ref, b_ref, c_ref, d_ref)):
        out_ref[pl.ds(pl.multiple_of(48 * (at ^ k), 8), 48), :] = ref[...]


SHRINK = 2.0**-15
FIRST = 2.0**-10
LARGEST_STEP = 1.001 / (POSE_REG * SHRINK)


def halves(x):
    t = 4097.0 * x
    top = t - (t - x)
    return top, x - top


def times(a, b):
    p = a * b
    ah, al = halves(a)
    bh, bl = halves(b)
    return p, ((ah * bh - p) + ah * bl + al * bh) + al * bl


def plus(a, b):
    t = a[0] + b[0]
    back = t - a[0]
    return t, (a[1] + b[1]) + ((a[0] - (t - back)) + (b[0] - back))


def tidy(a):
    t = a[0] + a[1]
    return t, a[1] - (t - a[0])


def mul(a, b):
    p, e = times(a[0], b[0])
    return tidy((p, e + (a[0] * b[1] + a[1] * b[0])))


def add(a, b):
    return tidy(plus(a, b))


def neg(a):
    return -a[0], -a[1]


def div(a, b):
    q = a[0] / b[0]
    rest = add(a, neg(mul((q, jnp.zeros_like(q)), b)))
    return tidy((q, rest[0] / b[0]))


def lane_total(a):
    for step in (64, 32, 16, 8, 4, 2, 1):
        a = plus(a, (pltpu.roll(a[0], step, 1), pltpu.roll(a[1], step, 1)))
    return a


def to_column(row):
    eye = iota((GROUP, LANES), 0) == iota((GROUP, LANES), 1)
    return jnp.broadcast_to(
        jnp.sum(jnp.where(eye, row, 0.0), axis=1, keepdims=True), (GROUP, LANES)
    )


def block_at(j):
    return pl.ds(pl.multiple_of(j * GROUP, 8), GROUP)


def tile_at(j):
    return pl.ds(pl.multiple_of(j * 8, 8), 8)


def product(s_ref, up_ref, col, split, j):
    acc = None
    lower, upper = slice(0, LANES), slice(LANES, 2 * LANES)
    sources = ((s_ref, lower, j, j), (s_ref, upper, j - 1, j - 1), (up_ref, slice(0, LANES), j, j + 1))
    for n, (ref, lanes, row, at) in enumerate(sources):
        s = ref[block_at(row), lanes]
        if split is None:
            sh, sl = halves(s)
        else:
            sh, sl = [x[block_at(row), lanes] for x in (split[2:] if n == 2 else split[:2])]
        high, low, hh, hl = [x[block_at(at), :] for x in col]
        p = s * high
        e = (((sh * hh - p) + sh * hl + sl * hh) + sl * hl) + s * low
        for r in range(0, GROUP, 8):
            term = p[r : r + 8], e[r : r + 8]
            acc = term if acc is None else plus(acc, term)
    for step in (4, 2, 1):
        acc = plus(acc, (pltpu.roll(acc[0], step, 0), pltpu.roll(acc[1], step, 0)))
    acc = tidy(acc)
    return acc[0] * SHRINK, acc[1] * SHRINK


def put_column(col, j, high, low):
    col[0][block_at(j), :] = high
    col[1][block_at(j), :] = low
    col[2][block_at(j), :], col[3][block_at(j), :] = halves(high)


def store_tile(ref, at, pair):
    row = iota((8, LANES), 0)
    ref[tile_at(at), :] = jnp.where(row == 0, pair[0], jnp.where(row == 1, pair[1], 0.0))


def powers(s_ref, up_ref, v_ref, cols, split, first, count, edge, base):
    for k in range(count):
        here, there = cols[k % 2], cols[1 - k % 2]

        def one(j, carry):
            pair = product(s_ref, up_ref, here, split, j)
            store_tile(v_ref, (first + k) * BLOCKS + j, pair)
            put_column(there, j, to_column(pair[0][0:1]), to_column(pair[1][0:1]))
            return carry

        lax.fori_loop(base + k * edge, BLOCKS - base - k * edge, one, 0)


def first_kernel(
    where_ref, p_ref, c_ref, n_ref, p2_ref, c2_ref, n2_ref,
    s_ref, up_ref, v_ref, v4_ref, *scratch,
):
    cols = scratch[0:4], scratch[4:8]
    split = scratch[8:12]
    core = where_ref[2]
    mine = pl.multiple_of(48 * core, 8)
    theirs = pl.multiple_of(48 - 48 * core, 8)
    diagonal = iota((GROUP, LANES), 0) == iota((GROUP, LANES), 1)
    lane = iota((GROUP, LANES), 1)
    for j in range(BLOCKS):
        rows = slice((j % 4) * 48, (j % 4 + 1) * 48)
        a = (p_ref, c_ref, n_ref)[j // 4]
        b = (p2_ref, c2_ref, n2_ref)[j // 4]
        s_ref[pl.ds(j * GROUP + mine, 48), :] = a[rows, :]
        s_ref[pl.ds(j * GROUP + theirs, 48), :] = b[rows, :]
    zero = jnp.zeros((LANES - GROUP, LANES), F32)

    def prepare(j, carry):
        own = s_ref[block_at(j), 0:LANES]
        rhs = jnp.broadcast_to(own[:, LANES - 1 : LANES], (GROUP, LANES)) * FIRST
        put_column(cols[0], j, rhs, jnp.zeros_like(rhs))
        store_tile(v_ref, j, (to_row(rhs), jnp.zeros((1, LANES), F32)))
        s_ref[block_at(j), 0:LANES] = jnp.where(lane < GROUP, own, 0.0) + jnp.where(
            diagonal, POSE_REG, 0.0
        )
        up = jnp.concatenate([s_ref[block_at(j), LANES : 2 * LANES], zero], axis=0).T
        up_ref[block_at(j), :] = up[0:GROUP]
        split[0][block_at(j), :], split[1][block_at(j), :] = halves(s_ref[block_at(j), :])
        split[2][block_at(j), :], split[3][block_at(j), :] = halves(up[0:GROUP])
        return carry

    lax.fori_loop(0, BLOCKS, prepare, 0)
    powers(s_ref, up_ref, v_ref, cols, split, 1, 4, 1, 1)
    for j in range(4):
        at = (4 * BLOCKS + 4 + j) * 8
        v4_ref[j : j + 1, :] = v_ref[at : at + 1, :]
        v4_ref[4 + j : 5 + j, :] = v_ref[at + 1 : at + 2, :]


def second_kernel(
    s_ref, up_ref, v_ref, below_ref, own_ref, above_ref, out_ref, v45_ref, *scratch,
):
    cols = scratch[0:4], scratch[4:8]
    for g, ref in enumerate((below_ref, own_ref, above_ref)):
        for j in range(4):
            pair = ref[j : j + 1, :], ref[4 + j : 5 + j, :]
            at = g * 4 + j
            store_tile(v45_ref, at, pair)
            if 1 < at < 10:
                put_column(cols[0], at, to_column(pair[0]), to_column(pair[1]))
    powers(s_ref, up_ref, v45_ref, cols, None, 1, 2, 1, 3)
    zero = jnp.zeros((1, LANES), F32)
    total = None
    for j in range(4, 8):

        def row(k, part):
            ref, at = (v_ref, k) if k < 4 else (v45_ref, k - 4)
            at = (at * BLOCKS + j) * 8 + part
            return ref[at : at + 1, :]

        def stack(pick, part):
            lines = [row(pick(m), part) for m in range(2 * ITERS)]
            return jnp.concatenate(lines + [zero] * (16 - len(lines)), axis=0)

        lower, upper = (lambda m: m // 2), (lambda m: m - m // 2)
        a, b = (stack(lower, 0), stack(lower, 1)), (stack(upper, 0), stack(upper, 1))
        p, e = times(a[0], b[0])
        term = p, e + (a[0] * b[1] + a[1] * b[0])
        total = term if total is None else plus(total, term)
    total = tidy(lane_total(total))
    diagonal = iota((16, LANES), 0) == iota((16, LANES), 1)
    put(
        out_ref,
        [jnp.sum(jnp.where(diagonal, x, 0.0), axis=0, keepdims=True) for x in total],
    )


def put(ref, pair):
    ref[...] = jnp.zeros((8, LANES), F32)
    ref[0:1, :] = pair[0]
    ref[1:2, :] = pair[1]


def gather_sum(refs):
    acc = refs[0][0:1, :], refs[0][1:2, :]
    for r in refs[1:]:
        acc = plus(acc, (r[0:1, :], r[1:2, :]))
    return tidy(acc)


def sum_kernel(a_ref, b_ref, c_ref, d_ref, out_ref):
    put(out_ref, gather_sum((a_ref, b_ref, c_ref, d_ref)))


def solve_kernel(
    where_ref, a_ref, b_ref, c_ref, d_ref, v_ref, v45_ref, base_ref, scale_ref, move_hbm, g_hbm,
    pose_ref, out_ref, sum_ref, move_ref, g_ref, sems,
):
    copies = [
        pltpu.make_async_copy(move_hbm, move_ref, sems.at[0]),
        pltpu.make_async_copy(g_hbm, g_ref, sems.at[1]),
    ]
    for copy in copies:
        copy.start()
    at_quad = where_ref[3]
    total = gather_sum((a_ref, b_ref, c_ref, d_ref))
    shape = (8, LANES)
    row = iota(shape, 0)
    lane = iota(shape, 1)
    zero = jnp.zeros(shape, F32)
    unit = jnp.where((row == 1) & (lane == LANES - 1), 1.0, 0.0)

    def where(live, a, b):
        return jnp.where(live, a[0], b[0]), jnp.where(live, a[1], b[1])

    def at(a, r, k):
        return tuple(jnp.broadcast_to(x[r : r + 1, k : k + 1], shape) for x in a)

    x = jnp.where(row == 0, total[0], unit), jnp.where(row == 0, total[1], 0.0)
    y = x
    found = (zero, zero)
    one = (zero + 1.0, zero)
    start = at(x, 0, 0)
    now = start
    lead = one[0]
    live = start[0] > 0.0
    for k in range(ITERS):
        alpha = div(now, where(live, at(y, 0, k + 1), one))
        live = live & (alpha[0] > 0.0) & (alpha[0] < LARGEST_STEP)
        alpha = where(live, alpha, (zero, zero))
        found = add(found, mul(alpha, y))
        if k + 1 == ITERS:
            break
        back = neg(alpha)
        moved = tuple(pltpu.roll(p, LANES - 1, 1) for p in y)
        x = add(x, mul(back, moved))
        fresh = at(x, 0, k + 1)
        lead = -lead * alpha[0]
        live = live & (lead * fresh[0] > 1e-11 * start[0])
        beta = div(mul(back, fresh), where(live, now, one))
        beta = where(live, beta, (zero, zero))
        y = add(x, mul(beta, y))
        now = fresh
    xc = [tuple(p[1:2, LANES - 1 - k : LANES - k] for p in found) for k in range(ITERS)]
    poses = []
    for g in range(3):
        acc = None
        for k in range(ITERS):
            ref = v_ref if k < 4 else v45_ref
            tile = ref[tile_at((k if k < 4 else k - 4) * BLOCKS + 3 + at_quad + g), :]
            wide = tuple(jnp.broadcast_to(x, (1, LANES)) for x in xc[k])
            term = mul(wide, (tile[0:1], tile[1:2]))
            acc = term if acc is None else plus(acc, term)
        poses.append((acc[0] + acc[1]) * (SHRINK / FIRST))
    column = to_column(poses[1])
    r = iota((GROUP, LANES), 0)
    l = iota((GROUP, LANES), 1)
    for c in range(6):
        line = jnp.sum(jnp.where(r == l * 6 + c, column, 0.0), axis=0, keepdims=True)
        pose_ref[c : c + 1, :] = line[:, 0:FD]
    for copy in copies:
        copy.wait()

    def frame(f, carry):
        rows = pl.ds(pl.multiple_of(f * GROUP, 8), GROUP)
        prod = (
            move_ref[rows, 0:LANES] * poses[0]
            + move_ref[rows, LANES : 2 * LANES] * poses[1]
            + move_ref[rows, 2 * LANES : 3 * LANES] * poses[2]
        )
        x = jnp.sum(prod, axis=1, keepdims=True)
        image = jnp.sum(g_ref[rows, :] * x, axis=0, keepdims=True)
        at = tile_at(f)
        sum_ref[at, :] = base_ref[at, :] - scale_ref[at, :] * image
        return carry

    lax.fori_loop(0, FD, frame, 0)
    for f in range(FD):
        out_ref[f : f + 1, :] = sum_ref[f * 8 : f * 8 + 1, :]


SMEM = pl.BlockSpec(memory_space=pltpu.SMEM)
VMEM = pl.BlockSpec(memory_space=pltpu.VMEM)
ANY = pl.BlockSpec(memory_space=pl.ANY)


def call(kernel, name, outs, smem, *args, scratch=(), hbm=0, hbm_out=0):
    return pl.pallas_call(
        kernel,
        name=name,
        out_shape=[jax.ShapeDtypeStruct(s, F32) for s in outs],
        in_specs=[SMEM] * smem + [VMEM] * (len(args) - smem - hbm) + [ANY] * hbm,
        out_specs=[VMEM] * (len(outs) - hbm_out) + [ANY] * hbm_out,
        scratch_shapes=list(scratch),
    )(*args)


def per_device(edge_frames, rotvec, trans, inv_depth, depth_damping, flow, weight, mask):
    f_dev, plocal = inv_depth.shape
    count = lax.axis_size("frames")
    pixes = lax.axis_size("pix")
    fi = lax.axis_index("frames")
    pi = lax.axis_index("pix")
    spot = jnp.stack([fi * f_dev, pi * plocal, pi % 2, fi % 4]).astype(jnp.int32)

    def shift(block, step):
        return lax.ppermute(
            block, "frames", [(i, i + step) for i in range(count) if 0 <= i + step < count]
        )

    edges = (edge_frames, flow.transpose(1, 0, 2), weight.transpose(1, 0, 2), mask)
    down, up = call(
        rim_kernel, "rim", [(8 + 4 * SIDE, plocal), (4 * SIDE, plocal)], 1, spot, *edges
    )
    from_after = shift(down, -1)
    from_before = shift(up, 1)
    (own,) = call(own_kernel, "own", [(4 * f_dev * SLOTS, plocal)], 1, spot, *edges)
    tab, b, bt = call(
        pose_kernel, "pose",
        [(f_dev * SLOTS, LANES), (f_dev * GROUP, 3 * LANES), (192, f_dev * GROUP)],
        1, spot, rotvec, trans,
    )
    pairs = f_dev * SLOTS
    geo, curv, grad, block = call(
        early_kernel, "early",
        [(5 * pairs, plocal), (f_dev * 8, plocal), (f_dev * 8, plocal), (f_dev * GROUP, LANES)],
        1, spot, own, inv_depth, tab, scratch=[pltpu.VMEM((f_dev * 8, plocal), F32)],
    )
    keep, send, base, scale, g = call(
        main_kernel, "main",
        [(96, 256), (96, 256), (f_dev * 8, plocal), (f_dev * 8, plocal), (f_dev * GROUP, plocal)],
        1, spot, from_after, from_before, curv, grad, block, inv_depth, depth_damping, tab, geo, b, bt,
        hbm=3, hbm_out=1,
        scratch=[
            pltpu.VMEM((4 * FD * 8, plocal), F32),
            pltpu.VMEM((GROUP + 16, plocal), F32),
            pltpu.VMEM((GROUP + 16, plocal), F32),
            pltpu.VMEM((256, plocal), F32),
            pltpu.VMEM((GROUP, LANES), F32),
            pltpu.VMEM((GROUP, LANES), F32),
            pltpu.VMEM((f_dev * GROUP, 3 * LANES), F32),
            pltpu.VMEM((192, 3 * LANES), F32),
            pltpu.VMEM((5 * pairs, plocal), F32),
            pltpu.VMEM((f_dev * GROUP, 3 * LANES), F32),
            pltpu.VMEM((192, f_dev * GROUP), F32),
            pltpu.VMEM((f_dev * GROUP, plocal), F32),
            pltpu.SemaphoreType.DMA((f_dev,)),
            pltpu.SemaphoreType.DMA((f_dev,)),
            pltpu.SemaphoreType.DMA((f_dev,)),
            pltpu.SemaphoreType.DMA((1,)),
        ],
    )
    got = lax.ppermute(send, "pix", [(i, i ^ 1) for i in range(pixes)])
    both = keep + got
    own_half, rim = both[:48], both[48:]
    both_axes = ("frames", "pix")

    def to_neighbour(flip):
        route = []
        for i in range(count):
            for k in range(pixes):
                to = i + 1 if k % 2 == 0 else i - 1
                if 0 <= to < count:
                    route.append((i * pixes + k, to * pixes + (k ^ flip)))
        return lax.ppermute(rim, both_axes, route)

    own_far = lax.ppermute(own_half, "pix", [(i, i ^ 2) for i in range(pixes)])
    rim_near = to_neighbour(0)
    rim_far = to_neighbour(2)
    half = (own_half + own_far) + (rim_near + rim_far)

    def mates(v, step):
        return [v] + [
            lax.ppermute(v, "frames", [(i, i ^ (k * step)) for i in range(count)]) for k in (1, 2, 3)
        ]

    def twin(v):
        return lax.ppermute(v, "pix", [(i, i ^ 1) for i in range(pixes)])

    def halo(v):
        return shift(v, 4), v, shift(v, -4)

    (quad,) = call(place_kernel, "place", [(192, 256)], 1, spot, *mates(half, 1))
    pieces = halo(quad)
    wide = BLOCKS * GROUP
    columns = [pltpu.VMEM((wide, LANES), F32)] * 8
    split = [pltpu.VMEM((wide, 2 * LANES), F32)] * 2 + [pltpu.VMEM((wide, LANES), F32)] * 2
    s, up, vs, v4 = call(
        first_kernel, "first",
        [(wide, 256), (wide, LANES), (5 * BLOCKS * 8, LANES), (8, LANES)],
        1, spot, *pieces, *[twin(x) for x in pieces], scratch=columns + split,
    )
    part, v45 = call(
        second_kernel, "second", [(8, LANES), (3 * BLOCKS * 8, LANES)], 0, s, up, vs, *halo(v4),
        scratch=columns,
    )
    (part,) = call(sum_kernel, "sum", [(8, LANES)], 0, *mates(part, 4))
    pose_step, depth_step = call(
        solve_kernel, "solve", [(6, f_dev), (f_dev, plocal)], 1, spot, *mates(part, 16), vs, v45,
        base, scale, b, g,
        scratch=[
            pltpu.VMEM((f_dev * 8, plocal), F32),
            pltpu.VMEM((f_dev * GROUP, 3 * LANES), F32),
            pltpu.VMEM((f_dev * GROUP, plocal), F32),
            pltpu.SemaphoreType.DMA((2,)),
        ],
        hbm=2,
    )
    return pose_step, depth_step


def solution(mesh):
    return jax.shard_map(
        per_device,
        mesh=mesh,
        in_specs=(
            P(None, "frames"),
            P(),
            P(),
            P("frames", "pix"),
            P("frames", "pix"),
            P("frames", None, "pix"),
            P("frames", None, "pix"),
            P("frames", "pix"),
        ),
        out_specs=(P(None, "frames"), P("frames", "pix")),
        check_vma=False,
    )
```

```python
import functools
import jax
import jax.numpy as jnp
from jax import lax
from jax.experimental import pallas as pl
from jax.experimental.pallas import tpu as pltpu
from jax.sharding import PartitionSpec as P

ROWS = 48
COLS = 64
RADIUS = 8
ITERS = 6
HIGHEST = lax.Precision.HIGHEST
F32 = jnp.float32
BF16 = jnp.bfloat16
LANES = 128
FD = 16
SLOTS = 16
GROUP = FD * 6
SIDE = RADIUS * (RADIUS + 1) // 2
POSE_REG = 100.0


def iota(shape, dim):
    return lax.broadcasted_iota(jnp.int32, shape, dim)


def thirds(x):
    first = x.astype(BF16)
    rest = x - first.astype(F32)
    second = rest.astype(BF16)
    return first, second, (rest - second.astype(F32)).astype(BF16)


def pair_of(x):
    first = x.astype(BF16)
    return first, (x - first.astype(F32)).astype(BF16)


def dot(a, b):
    return jnp.dot(a, b, preferred_element_type=F32)


def spread(where_ref, ef_ref, flow_ref, weight_ref, mask_ref, rims, write):
    edges = ef_ref.shape[1]
    start = where_ref[0]
    source = ef_ref[0:1, :] - start
    delta = ef_ref[1:2, :] - start - source
    slot = jnp.where(delta < 0, delta + 8, delta + 7)
    if rims:
        j = source + 8
        down_at = jnp.where(source < 0, ((j * (j + 1)) >> 1) + delta - 8 + j, -1)
        j = 23 - source
        up_at = jnp.where(source >= FD, ((j * (j + 1)) >> 1) + slot, -1)
        row = iota((40, edges), 0)
        hot = jnp.concatenate([(row == down_at).astype(F32), (row == up_at).astype(F32)], axis=0)
    else:
        own_at = jnp.where((source >= 0) & (source < FD), source * SLOTS + slot, -1)
        hot = (iota((FD * SLOTS, edges), 0) == own_at).astype(F32)
    hot = hot.astype(BF16)
    for chunk in range(mask_ref.shape[1] // LANES):
        lanes = pl.ds(chunk * LANES, LANES)
        live = mask_ref[:, lanes].astype(F32)
        parts = []
        for comp in range(2):
            conf = weight_ref[comp, :, lanes] * live
            parts.append((conf, conf * flow_ref[comp, :, lanes]))
        values = jnp.concatenate([parts[0][0], parts[1][0], parts[0][1], parts[1][1]], axis=1)
        got = sum(dot(hot, piece) for piece in reversed(thirds(values)))
        for q in range(4):
            write(q, lanes, got[:, q * LANES : (q + 1) * LANES])


def rim_kernel(where_ref, ef_ref, flow_ref, weight_ref, mask_ref, down_ref, up_ref):
    down_ref[0:8, :] = jnp.zeros((8, down_ref.shape[1]), F32)

    def write(q, lanes, cut):
        down_ref[8 + q * SIDE : 8 + (q + 1) * SIDE, lanes] = cut[0:SIDE]
        up_ref[q * SIDE : (q + 1) * SIDE, lanes] = cut[40 : 40 + SIDE]

    spread(where_ref, ef_ref, flow_ref, weight_ref, mask_ref, True, write)


def rotation_rows(w):
    x, y, z = w
    zero = jnp.zeros_like(x)
    cross = [[zero, -z, y], [z, zero, -x], [-y, x, zero]]
    sq = x * x + y * y + z * z
    first = 1.0 - sq / 6.0 + sq * sq / 120.0
    second = 0.5 - sq / 24.0 + sq * sq / 720.0
    return [
        [
            float(i == k)
            + first * cross[i][k]
            + second * sum(cross[i][m] * cross[m][k] for m in range(3))
            for k in range(3)
        ]
        for i in range(3)
    ]


def pose_kernel(where_ref, rotvec_ref, trans_ref, tab_ref, b_ref, bt_ref):
    start = where_ref[0]
    frames = rotvec_ref.shape[1]
    pair = iota((1, FD * SLOTS), 1)
    slot = pair & 15
    delta = jnp.where(slot < 8, slot - 8, slot - 7)
    at_source = start + (pair >> 4)
    at_target = jnp.clip(at_source + delta, 0, frames - 1)
    poses = jnp.concatenate([rotvec_ref[...], trans_ref[...], jnp.zeros((2, frames), F32)], axis=0)
    first = start - RADIUS
    poses = pltpu.roll(poses, (2 * frames - first) % frames, 1)[:, 0:LANES]

    def pick(at):
        hot = (iota((LANES, FD * SLOTS), 0) == at - first).astype(F32)
        return jnp.dot(poses, hot, precision=HIGHEST, preferred_element_type=F32)

    src = pick(at_source)
    tgt = pick(at_target)
    rs = rotation_rows([src[k : k + 1] for k in range(3)])
    rt = rotation_rows([tgt[k : k + 1] for k in range(3)])
    rel = [[sum(rt[i][k] * rs[m][k] for k in range(3)) for m in range(3)] for i in range(3)]
    tr = [
        tgt[3 + i : 4 + i] - sum(rel[i][m] * src[3 + m : 4 + m] for m in range(3)) for i in range(3)
    ]
    corner = [
        [tr[1] * rel[2][m] - tr[2] * rel[1][m] for m in range(3)],
        [tr[2] * rel[0][m] - tr[0] * rel[2][m] for m in range(3)],
        [tr[0] * rel[1][m] - tr[1] * rel[0][m] for m in range(3)],
    ]
    lines = [x for row in rel for x in row] + tr + [x for row in corner for x in row]
    lines = jnp.concatenate(lines + [jnp.zeros((LANES - len(lines), FD * SLOTS), F32)], axis=0)
    tab_ref[...] = lines.T

    lane3 = iota((SLOTS, 3 * LANES), 1)
    row3 = iota((SLOTS, 3 * LANES), 0)
    off3 = jnp.where(row3 < 8, row3 - 8, row3 - 7)

    def build(f, carry):
        frame = f + off3 + FD
        home = (frame >> 4) * LANES + (frame & 15) * 6
        tab = tab_ref[pl.ds(pl.multiple_of(f * SLOTS, SLOTS), SLOTS), :]
        for c in range(6):
            block = jnp.where(lane3 == home + c, 1.0, 0.0)
            for d in range(6):
                if c < 3:
                    at = c * 3 + d if d < 3 else 12 + c * 3 + d - 3
                elif d >= 3:
                    at = (c - 3) * 3 + d - 3
                else:
                    continue
                block = block - jnp.where(
                    lane3 == LANES + f * 6 + d, jnp.broadcast_to(tab[:, at : at + 1], lane3.shape), 0.0
                )
            b_ref[pl.ds(pl.multiple_of(f * GROUP + c * SLOTS, SLOTS), SLOTS), :] = block
        return carry

    lax.fori_loop(0, FD, build, 0)
    for g in range(4):
        cols = slice(g * 384, (g + 1) * 384)
        below = b_ref[cols, 0:LANES].T
        own = b_ref[cols, LANES : 2 * LANES].T
        above = b_ref[cols, 2 * LANES : 3 * LANES].T
        bt_ref[0:48, cols] = below[48:96]
        bt_ref[48:144, cols] = own[0:96]
        bt_ref[144:192, cols] = above[0:48]


def coords(first, chunk):
    pixel = first + chunk * LANES + iota((8, LANES), 1)
    col = ((pixel & (COLS - 1)).astype(F32) - 0.5 * (COLS - 1)) / COLS
    line = ((pixel >> 6).astype(F32) - 0.5 * (ROWS - 1)) / COLS
    return col, line


def pull(u, v, s, uv, u1, v1, pu, pv):
    spu = s * pu
    spv = s * pv
    return (
        spu,
        spv,
        -(u * spu + v * spv),
        -(uv * pu) - v1 * pv,
        u1 * pu + uv * pv,
        u * pv - v * pu,
    )


def pose_sums(u, v, s, cu, cv, eu, ev):
    uv = u * v
    u1 = 1.0 + u * u
    v1 = 1.0 + v * v
    terms = list(pull(u, v, s, uv, u1, v1, -eu, -ev))
    su_ = cu * s
    sv_ = cv * s
    ju = (-uv, u1, -v)
    jv = (-v1, uv, u)
    a00 = su_ * s
    a11 = sv_ * s
    a02 = -(a00 * u)
    a12 = -(a11 * v)
    terms += [a00, a11, a02, a12, -(a02 * u + a12 * v)]
    tu = [su_ * x for x in ju]
    tv = [sv_ * x for x in jv]
    terms += tu + tv
    terms += [-(u * x + v * y) for x, y in zip(tu, tv)]
    wu = [cu * x for x in ju]
    wv = [cv * x for x in jv]
    for a in range(3):
        for b in range(a, 3):
            terms.append(wu[a] * ju[b] + wv[a] * jv[b])
    return terms


def diagonal_rows(acc, h):
    lane = iota((8, LANES), 1)
    row = iota((8, LANES), 0)
    sums = [jnp.broadcast_to(jnp.sum(x, axis=1, keepdims=True), (8, LANES)) for x in acc]
    a = {(0, 0): 6, (1, 1): 7, (0, 2): 8, (1, 2): 9, (2, 2): 10}
    for k in range(3):
        a[(0, 3 + k)] = 11 + k
        a[(1, 3 + k)] = 14 + k
        a[(2, 3 + k)] = 17 + k
    at = 20
    for x in range(3):
        for y in range(x, 3):
            a[(3 + x, 3 + y)] = at
            at += 1
    tiles = []
    for c in range(6):
        tile = jnp.where(lane == LANES - 1, sums[c], 0.0)
        for d in range(6):
            key = (min(c, d), max(c, d))
            if key != (0, 1):
                tile = jnp.where(lane == d * SLOTS + 8 * h + row, sums[a[key]], tile)
        tiles.append(tile)
    return tiles


def early_kernel(
    where_ref, ef_ref, flow_ref, weight_ref, mask_ref, depth_ref, tab_ref,
    geo_ref, curv_ref, grad_ref, block_ref, in_ref, own_ref,
):
    def write(q, lanes, cut):
        own_ref[q * 256 : (q + 1) * 256, lanes] = cut

    spread(where_ref, ef_ref, flow_ref, weight_ref, mask_ref, False, write)
    plocal = depth_ref.shape[1]
    chunks = plocal // LANES
    for f in range(FD):
        in_ref[f * 8 : f * 8 + 8, :] = jnp.broadcast_to(depth_ref[f : f + 1, :], (8, plocal))

    def frame(f, carry):
        eight = pl.ds(pl.multiple_of(f * 8, 8), 8)
        for h in range(2):
            tab = tab_ref[pl.ds(pl.multiple_of(f * SLOTS + 8 * h, 8), 8), :]
            r = [jnp.broadcast_to(tab[:, k : k + 1], (8, LANES)) for k in range(12)]
            acc = [0.0] * 26
            for c in range(chunks):
                lanes = pl.ds(c * LANES, LANES)
                col, line = coords(where_ref[1], c)
                depth = in_ref[eight, lanes]

                def at(q):
                    return pl.ds(pl.multiple_of(q * 256 + f * SLOTS + 8 * h, 8), 8)

                cu, cv, fu, fv = [own_ref[at(q), lanes] for q in range(4)]
                inv = 1.0 / (r[6] * col + r[7] * line + r[8] + depth * r[11])
                u = (r[0] * col + r[1] * line + r[2] + depth * r[9]) * inv
                v = (r[3] * col + r[4] * line + r[5] + depth * r[10]) * inv
                su = inv * (r[9] - u * r[11])
                sv = inv * (r[10] - v * r[11])
                eu = cu * (col - u) + fu
                ev = cv * (line - v) + fv
                au = cu * su
                av = cv * sv
                curv = au * su + av * sv
                grad = -(su * eu + sv * ev)
                if h:
                    curv = curv + curv_ref[eight, lanes]
                    grad = grad + grad_ref[eight, lanes]
                curv_ref[eight, lanes] = curv
                grad_ref[eight, lanes] = grad
                for q, x in enumerate((u, v, inv, au, av)):
                    row = pl.multiple_of((f * 5 + q) * SLOTS + 8 * h, 8)
                    geo_ref[pl.ds(row, 8), lanes] = x
                acc = [x + y for x, y in zip(acc, pose_sums(u, v, depth * inv, cu, cv, eu, ev))]
            for c, tile in enumerate(diagonal_rows(acc, h)):
                block_ref[pl.ds(pl.multiple_of(f * GROUP + c * SLOTS + 8 * h, 8), 8), :] = tile
        return carry

    lax.fori_loop(0, FD, frame, 0)


def main_kernel(
    where_ref, rdown_ref, rup_ref, curv_ref, grad_ref, block_ref, depth_ref, damp_ref, tab_ref,
    geo_hbm, b_hbm, bt_hbm,
    keep_ref, send_ref, base_ref, scale_ref, g_hbm,
    half_ref, hi0_ref, hi1_ref, in_ref, q0_ref, q1_ref, w_ref, t_ref, geo_ref, b_ref, bt_ref, g_ref,
    geo_sems, b_sems, g_sems, bt_sem,
):
    def piece(src, dst, sems, f, rows):
        at = pl.ds(pl.multiple_of(f * rows, 8), rows)
        return pltpu.make_async_copy(src.at[at, :], dst.at[at, :], sems.at[f])

    for f in range(FD):
        piece(geo_hbm, geo_ref, geo_sems, f, 5 * SLOTS).start()
        piece(b_hbm, b_ref, b_sems, f, GROUP).start()
    bt_copy = pltpu.make_async_copy(bt_hbm, bt_ref, bt_sem.at[0])
    bt_copy.start()
    core = where_ref[2]
    plocal = depth_ref.shape[1]
    chunks = plocal // LANES
    row8 = iota((8, plocal), 0)
    for f in range(FD):
        j = 7 - f if f < 8 else f - 8
        base = j * (j + 1) // 2
        for q in range(4):
            if f < 8:
                first = q * SIDE + base
                extra = jnp.where(row8 <= j, rup_ref[first : first + 8, :], 0.0)
            else:
                first = 8 + q * SIDE + base - 7 + j
                extra = jnp.where(row8 >= 7 - j, rdown_ref[first : first + 8, :], 0.0)
            half_ref[(q * FD + f) * 8 : (q * FD + f + 1) * 8, :] = extra
        in_ref[f * 8 : f * 8 + 8, :] = jnp.broadcast_to(depth_ref[f : f + 1, :], (8, plocal))
        in_ref[128 + f * 8 : 136 + f * 8, :] = jnp.broadcast_to(damp_ref[f : f + 1, :], (8, plocal))
    lane = iota((8, LANES), 1)

    def tiles(f, merged, hi_ref, q_ref):
        eight = pl.ds(pl.multiple_of(f * 8, 8), 8)
        tab = tab_ref[pl.ds(pl.multiple_of(f * SLOTS + 8 * merged, 8), 8), :]
        t0, t1, t2 = [jnp.broadcast_to(tab[:, k : k + 1], (8, LANES)) for k in (9, 10, 11)]
        acc = [0.0] * 26
        for c in range(chunks):
            lanes = pl.ds(c * LANES, LANES)
            col, line = coords(where_ref[1], c)
            depth = in_ref[eight, lanes]

            def geo(q, h):
                return geo_ref[pl.ds(pl.multiple_of((f * 5 + q) * SLOTS + 8 * h, 8), 8), lanes]

            cu, cv, fu, fv = [
                half_ref[pl.ds(pl.multiple_of((q * FD + f) * 8, 8), 8), lanes] for q in range(4)
            ]
            u, v, inv = [geo(q, merged) for q in range(3)]
            su = inv * (t0 - u * t2)
            sv = inv * (t1 - v * t2)
            eu = cu * (col - u) + fu
            ev = cv * (line - v) + fv
            au = cu * su
            av = cv * sv
            acc = [x + y for x, y in zip(acc, pose_sums(u, v, depth * inv, cu, cv, eu, ev))]
            curv = curv_ref[eight, lanes] + (au * su + av * sv)
            grad = grad_ref[eight, lanes] - (su * eu + sv * ev)
            total = in_ref[pl.ds(pl.multiple_of(128 + f * 8, 8), 8), lanes] + jnp.sum(
                curv, axis=0, keepdims=True
            )
            base = jnp.sum(grad, axis=0, keepdims=True) / total
            root = jnp.sqrt(total)
            scale = 1.0 / root
            base_ref[eight, lanes] = base
            scale_ref[eight, lanes] = scale
            lifted = base * root
            hi_ref[GROUP : GROUP + 8, lanes] = lifted
            hi_ref[GROUP + 8 : GROUP + 16, lanes] = lifted - lifted.astype(BF16).astype(F32)
            for h in range(2):
                if h != merged:
                    u, v, inv = [geo(q, h) for q in range(3)]
                    gu, gv = geo(3, h), geo(4, h)
                else:
                    u, v, inv = [geo(q, h) for q in range(3)]
                    gu, gv = geo(3, h) + au, geo(4, h) + av
                rows = pull(
                    u, v, depth * inv, u * v, 1.0 + u * u, 1.0 + v * v, gu * scale, gv * scale
                )
                for k, x in enumerate(rows):
                    g_ref[pl.ds(pl.multiple_of(f * GROUP + k * SLOTS + 8 * h, 8), 8), lanes] = x
                    hi_ref[k * SLOTS + 8 * h : k * SLOTS + 8 * h + 8, lanes] = x
        q_ref[...] = block_ref[pl.ds(pl.multiple_of(f * GROUP, 8), GROUP), :]
        for c, tile in enumerate(diagonal_rows(acc, merged)):
            at = slice(c * SLOTS + 8 * merged, c * SLOTS + 8 * merged + 8)
            q_ref[at, :] = q_ref[at, :] + tile

    def matmuls(f, hi_ref, q_ref):
        rows = pl.ds(pl.multiple_of(f * GROUP, 8), GROUP)
        g = hi_ref[...]
        top, low = pair_of(g)
        both = lax.dot_general(
            jnp.concatenate([top[0:GROUP], low[0:GROUP]], axis=0), top, (((1,), (1,)), ((), ())),
            preferred_element_type=F32,
        )
        m = both[0:GROUP, 0:GROUP] + both[GROUP:, 0:GROUP] + both[GROUP:, 0:GROUP].T
        vec = q_ref[:, LANES - 1 : LANES] - (
            both[0:GROUP, GROUP : GROUP + 1]
            + both[GROUP:, GROUP : GROUP + 1]
            + both[0:GROUP, GROUP + 8 : GROUP + 9]
        )
        q = q_ref[:, 0:GROUP] - m
        q_top, q_low = pair_of(q)
        b_top, b_low = pair_of(b_ref[rows, :])
        both = dot(jnp.concatenate([q_top, q_low], axis=0), b_top)
        w = both[0:GROUP] + both[GROUP:]
        w_ref[rows, 0:LANES] = jnp.where(
            iota((GROUP, LANES), 1) == LANES - 1, jnp.broadcast_to(vec, (GROUP, LANES)), w[:, 0:LANES]
        )
        w_ref[rows, LANES : 2 * LANES] = w[:, LANES : 2 * LANES] + dot(q_top, b_low[:, LANES : 2 * LANES])
        w_ref[rows, 2 * LANES :] = w[:, 2 * LANES :]

    def frames(i, carry, merged):
        work = ((2 * i, hi0_ref, q0_ref), (2 * i + 1, hi1_ref, q1_ref))
        for f, _, _ in work:
            piece(geo_hbm, geo_ref, geo_sems, f, 5 * SLOTS).wait()
            piece(b_hbm, b_ref, b_sems, f, GROUP).wait()
        for f, hi_ref, q_ref in work:
            tiles(f, merged, hi_ref, q_ref)
        for f, hi_ref, q_ref in work:
            matmuls(f, hi_ref, q_ref)
        for f, _, _ in work:
            piece(g_ref, g_hbm, g_sems, f, GROUP).start()
        return carry

    lax.fori_loop(0, 4, functools.partial(frames, merged=0), 0)
    lax.fori_loop(4, 8, functools.partial(frames, merged=1), 0)
    bt_copy.wait()
    bt_top, bt_low = pair_of(bt_ref[...])
    w_top, w_low = pair_of(w_ref[...])
    both = dot(jnp.concatenate([bt_top, bt_low], axis=0), w_top)
    t = both[0:192] + both[192:] + dot(bt_top, w_low)
    t_ref[...] = t
    for lo, hi, group, first in ((0, 48, 0, 48), (48, 144, 1, 0), (144, 192, 2, 0)):
        count = hi - lo
        lanes = slice(group * LANES, (group + 1) * LANES)
        square = jnp.concatenate(
            [jnp.zeros((first, LANES), F32)] * (first > 0)
            + [t[lo:hi, lanes], jnp.zeros((LANES - first - count, LANES), F32)],
            axis=0,
        )
        mean = 0.5 * (square + square.T)
        t_ref[lo:hi, lanes] = mean[first : first + count]
    last = iota((48, LANES), 1) == LANES - 1

    def half(core):
        own = slice(48 + 48 * core, 96 + 48 * core)
        rim = slice(0, 48) if core else slice(144, 192)
        group = 0 if core else 2
        mine = jnp.where(last, t[own, 0:LANES], t_ref[own, LANES : 2 * LANES])
        theirs = jnp.where(last, t[rim, 0:LANES], t_ref[rim, group * LANES : (group + 1) * LANES])
        far = t_ref[rim, LANES : 2 * LANES] if core else jnp.zeros((48, LANES), F32)
        return mine, t_ref[own, 2 * LANES :], theirs, far

    def put_half(ref, core):
        for k, x in enumerate(half(core)):
            ref[(k // 2) * 48 : (k // 2 + 1) * 48, (k % 2) * LANES : (k % 2 + 1) * LANES] = x

    @pl.when(core == 0)
    def _():
        put_half(keep_ref, 0)
        put_half(send_ref, 1)

    @pl.when(core == 1)
    def _():
        put_half(keep_ref, 1)
        put_half(send_ref, 0)

    for f in range(FD):
        piece(g_ref, g_hbm, g_sems, f, GROUP).wait()


def to_row(column):
    return jnp.sum(
        jnp.where(iota((GROUP, LANES), 0) == iota((GROUP, LANES), 1), column, 0.0),
        axis=0,
        keepdims=True,
    )


BLOCKS = 12


def place_kernel(where_ref, a_ref, b_ref, c_ref, d_ref, out_ref):
    at = where_ref[3]
    for k, ref in enumerate((a_ref, b_ref, c_ref, d_ref)):
        out_ref[pl.ds(pl.multiple_of(48 * (at ^ k), 8), 48), :] = ref[...]


SHRINK = 2.0**-15
FIRST = 2.0**-10
LARGEST_STEP = 1.001 / (POSE_REG * SHRINK)


def halves(x):
    t = 4097.0 * x
    top = t - (t - x)
    return top, x - top


def times(a, b):
    p = a * b
    ah, al = halves(a)
    bh, bl = halves(b)
    return p, ((ah * bh - p) + ah * bl + al * bh) + al * bl


def plus(a, b):
    t = a[0] + b[0]
    back = t - a[0]
    return t, (a[1] + b[1]) + ((a[0] - (t - back)) + (b[0] - back))


def tidy(a):
    t = a[0] + a[1]
    return t, a[1] - (t - a[0])


def mul(a, b):
    p, e = times(a[0], b[0])
    return tidy((p, e + (a[0] * b[1] + a[1] * b[0])))


def add(a, b):
    return tidy(plus(a, b))


def neg(a):
    return -a[0], -a[1]


def div(a, b):
    q = a[0] / b[0]
    rest = add(a, neg(mul((q, jnp.zeros_like(q)), b)))
    return tidy((q, rest[0] / b[0]))


def lane_total(a):
    for step in (64, 32, 16, 8, 4, 2, 1):
        a = plus(a, (pltpu.roll(a[0], step, 1), pltpu.roll(a[1], step, 1)))
    return a


def to_column(row):
    eye = iota((GROUP, LANES), 0) == iota((GROUP, LANES), 1)
    return jnp.broadcast_to(
        jnp.sum(jnp.where(eye, row, 0.0), axis=1, keepdims=True), (GROUP, LANES)
    )


def block_at(j):
    return pl.ds(pl.multiple_of(j * GROUP, 8), GROUP)


def tile_at(j):
    return pl.ds(pl.multiple_of(j * 8, 8), 8)


def product(s_ref, up_ref, col, split, j):
    acc = None
    lower, upper = slice(0, LANES), slice(LANES, 2 * LANES)
    sources = ((s_ref, lower, j, j), (s_ref, upper, j - 1, j - 1), (up_ref, slice(0, LANES), j, j + 1))
    for n, (ref, lanes, row, at) in enumerate(sources):
        s = ref[block_at(row), lanes]
        if split is None:
            sh, sl = halves(s)
        else:
            sh, sl = [x[block_at(row), lanes] for x in (split[2:] if n == 2 else split[:2])]
        high, low, hh, hl = [x[block_at(at), :] for x in col]
        p = s * high
        e = (((sh * hh - p) + sh * hl + sl * hh) + sl * hl) + s * low
        for r in range(0, GROUP, 8):
            term = p[r : r + 8], e[r : r + 8]
            acc = term if acc is None else plus(acc, term)
    for step in (4, 2, 1):
        acc = plus(acc, (pltpu.roll(acc[0], step, 0), pltpu.roll(acc[1], step, 0)))
    acc = tidy(acc)
    return acc[0] * SHRINK, acc[1] * SHRINK


def put_column(col, j, high, low):
    col[0][block_at(j), :] = high
    col[1][block_at(j), :] = low
    col[2][block_at(j), :], col[3][block_at(j), :] = halves(high)


def store_tile(ref, at, pair):
    row = iota((8, LANES), 0)
    ref[tile_at(at), :] = jnp.where(row == 0, pair[0], jnp.where(row == 1, pair[1], 0.0))


def powers(s_ref, up_ref, v_ref, cols, split, first, count, edge, base):
    for k in range(count):
        here, there = cols[k % 2], cols[1 - k % 2]

        def one(j, carry):
            pair = product(s_ref, up_ref, here, split, j)
            store_tile(v_ref, (first + k) * BLOCKS + j, pair)
            put_column(there, j, to_column(pair[0][0:1]), to_column(pair[1][0:1]))
            return carry

        lax.fori_loop(base + k * edge, BLOCKS - base - k * edge, one, 0)


def first_kernel(
    where_ref, p_ref, c_ref, n_ref, p2_ref, c2_ref, n2_ref,
    s_ref, up_ref, v_ref, v4_ref, *scratch,
):
    cols = scratch[0:4], scratch[4:8]
    split = scratch[8:12]
    core = where_ref[2]
    mine = pl.multiple_of(48 * core, 8)
    theirs = pl.multiple_of(48 - 48 * core, 8)
    diagonal = iota((GROUP, LANES), 0) == iota((GROUP, LANES), 1)
    lane = iota((GROUP, LANES), 1)
    for j in range(BLOCKS):
        rows = slice((j % 4) * 48, (j % 4 + 1) * 48)
        a = (p_ref, c_ref, n_ref)[j // 4]
        b = (p2_ref, c2_ref, n2_ref)[j // 4]
        s_ref[pl.ds(j * GROUP + mine, 48), :] = a[rows, :]
        s_ref[pl.ds(j * GROUP + theirs, 48), :] = b[rows, :]
    zero = jnp.zeros((LANES - GROUP, LANES), F32)

    def prepare(j, carry):
        own = s_ref[block_at(j), 0:LANES]
        rhs = jnp.broadcast_to(own[:, LANES - 1 : LANES], (GROUP, LANES)) * FIRST
        put_column(cols[0], j, rhs, jnp.zeros_like(rhs))
        store_tile(v_ref, j, (to_row(rhs), jnp.zeros((1, LANES), F32)))
        s_ref[block_at(j), 0:LANES] = jnp.where(lane < GROUP, own, 0.0) + jnp.where(
            diagonal, POSE_REG, 0.0
        )
        up = jnp.concatenate([s_ref[block_at(j), LANES : 2 * LANES], zero], axis=0).T
        up_ref[block_at(j), :] = up[0:GROUP]
        split[0][block_at(j), :], split[1][block_at(j), :] = halves(s_ref[block_at(j), :])
        split[2][block_at(j), :], split[3][block_at(j), :] = halves(up[0:GROUP])
        return carry

    lax.fori_loop(0, BLOCKS, prepare, 0)
    powers(s_ref, up_ref, v_ref, cols, split, 1, 4, 1, 1)
    for j in range(4):
        at = (4 * BLOCKS + 4 + j) * 8
        v4_ref[j : j + 1, :] = v_ref[at : at + 1, :]
        v4_ref[4 + j : 5 + j, :] = v_ref[at + 1 : at + 2, :]


def second_kernel(
    s_ref, up_ref, v_ref, below_ref, own_ref, above_ref, out_ref, v45_ref, *scratch,
):
    cols = scratch[0:4], scratch[4:8]
    for g, ref in enumerate((below_ref, own_ref, above_ref)):
        for j in range(4):
            pair = ref[j : j + 1, :], ref[4 + j : 5 + j, :]
            at = g * 4 + j
            store_tile(v45_ref, at, pair)
            if 1 < at < 10:
                put_column(cols[0], at, to_column(pair[0]), to_column(pair[1]))
    powers(s_ref, up_ref, v45_ref, cols, None, 1, 2, 1, 3)
    zero = jnp.zeros((1, LANES), F32)
    total = None
    for j in range(4, 8):

        def row(k, part):
            ref, at = (v_ref, k) if k < 4 else (v45_ref, k - 4)
            at = (at * BLOCKS + j) * 8 + part
            return ref[at : at + 1, :]

        def stack(pick, part):
            lines = [row(pick(m), part) for m in range(2 * ITERS)]
            return jnp.concatenate(lines + [zero] * (16 - len(lines)), axis=0)

        lower, upper = (lambda m: m // 2), (lambda m: m - m // 2)
        a, b = (stack(lower, 0), stack(lower, 1)), (stack(upper, 0), stack(upper, 1))
        p, e = times(a[0], b[0])
        term = p, e + (a[0] * b[1] + a[1] * b[0])
        total = term if total is None else plus(total, term)
    total = tidy(lane_total(total))
    diagonal = iota((16, LANES), 0) == iota((16, LANES), 1)
    put(
        out_ref,
        [jnp.sum(jnp.where(diagonal, x, 0.0), axis=0, keepdims=True) for x in total],
    )


def put(ref, pair):
    ref[...] = jnp.zeros((8, LANES), F32)
    ref[0:1, :] = pair[0]
    ref[1:2, :] = pair[1]


def gather_sum(refs):
    acc = refs[0][0:1, :], refs[0][1:2, :]
    for r in refs[1:]:
        acc = plus(acc, (r[0:1, :], r[1:2, :]))
    return tidy(acc)


def sum_kernel(a_ref, b_ref, c_ref, d_ref, out_ref):
    put(out_ref, gather_sum((a_ref, b_ref, c_ref, d_ref)))


def solve_kernel(
    where_ref, a_ref, b_ref, c_ref, d_ref, v_ref, v45_ref, base_ref, scale_ref, move_hbm, g_hbm,
    pose_ref, out_ref, sum_ref, move_ref, g_ref, sems,
):
    copies = [
        pltpu.make_async_copy(move_hbm, move_ref, sems.at[0]),
        pltpu.make_async_copy(g_hbm, g_ref, sems.at[1]),
    ]
    for copy in copies:
        copy.start()
    at_quad = where_ref[3]
    total = gather_sum((a_ref, b_ref, c_ref, d_ref))
    shape = (8, LANES)
    row = iota(shape, 0)
    lane = iota(shape, 1)
    zero = jnp.zeros(shape, F32)
    unit = jnp.where((row == 1) & (lane == LANES - 1), 1.0, 0.0)

    def where(live, a, b):
        return jnp.where(live, a[0], b[0]), jnp.where(live, a[1], b[1])

    def at(a, r, k):
        return tuple(jnp.broadcast_to(x[r : r + 1, k : k + 1], shape) for x in a)

    x = jnp.where(row == 0, total[0], unit), jnp.where(row == 0, total[1], 0.0)
    y = x
    found = (zero, zero)
    one = (zero + 1.0, zero)
    start = at(x, 0, 0)
    now = start
    lead = one[0]
    live = start[0] > 0.0
    for k in range(ITERS):
        alpha = div(now, where(live, at(y, 0, k + 1), one))
        live = live & (alpha[0] > 0.0) & (alpha[0] < LARGEST_STEP)
        alpha = where(live, alpha, (zero, zero))
        found = add(found, mul(alpha, y))
        if k + 1 == ITERS:
            break
        back = neg(alpha)
        moved = tuple(pltpu.roll(p, LANES - 1, 1) for p in y)
        x = add(x, mul(back, moved))
        fresh = at(x, 0, k + 1)
        lead = -lead * alpha[0]
        live = live & (lead * fresh[0] > 1e-11 * start[0])
        beta = div(mul(back, fresh), where(live, now, one))
        beta = where(live, beta, (zero, zero))
        y = add(x, mul(beta, y))
        now = fresh
    xc = [tuple(p[1:2, LANES - 1 - k : LANES - k] for p in found) for k in range(ITERS)]
    poses = []
    for g in range(3):
        acc = None
        for k in range(ITERS):
            ref = v_ref if k < 4 else v45_ref
            tile = ref[tile_at((k if k < 4 else k - 4) * BLOCKS + 3 + at_quad + g), :]
            wide = tuple(jnp.broadcast_to(x, (1, LANES)) for x in xc[k])
            term = mul(wide, (tile[0:1], tile[1:2]))
            acc = term if acc is None else plus(acc, term)
        poses.append((acc[0] + acc[1]) * (SHRINK / FIRST))
    column = to_column(poses[1])
    r = iota((GROUP, LANES), 0)
    l = iota((GROUP, LANES), 1)
    for c in range(6):
        line = jnp.sum(jnp.where(r == l * 6 + c, column, 0.0), axis=0, keepdims=True)
        pose_ref[c : c + 1, :] = line[:, 0:FD]
    for copy in copies:
        copy.wait()

    def frame(f, carry):
        rows = pl.ds(pl.multiple_of(f * GROUP, 8), GROUP)
        prod = (
            move_ref[rows, 0:LANES] * poses[0]
            + move_ref[rows, LANES : 2 * LANES] * poses[1]
            + move_ref[rows, 2 * LANES : 3 * LANES] * poses[2]
        )
        x = jnp.sum(prod, axis=1, keepdims=True)
        image = jnp.sum(g_ref[rows, :] * x, axis=0, keepdims=True)
        at = tile_at(f)
        sum_ref[at, :] = base_ref[at, :] - scale_ref[at, :] * image
        return carry

    lax.fori_loop(0, FD, frame, 0)
    for f in range(FD):
        out_ref[f : f + 1, :] = sum_ref[f * 8 : f * 8 + 1, :]


SMEM = pl.BlockSpec(memory_space=pltpu.SMEM)
VMEM = pl.BlockSpec(memory_space=pltpu.VMEM)
ANY = pl.BlockSpec(memory_space=pl.ANY)


def call(kernel, name, outs, smem, *args, scratch=(), hbm=0, hbm_out=0):
    return pl.pallas_call(
        kernel,
        name=name,
        out_shape=[jax.ShapeDtypeStruct(s, F32) for s in outs],
        in_specs=[SMEM] * smem + [VMEM] * (len(args) - smem - hbm) + [ANY] * hbm,
        out_specs=[VMEM] * (len(outs) - hbm_out) + [ANY] * hbm_out,
        scratch_shapes=list(scratch),
    )(*args)


def per_device(edge_frames, rotvec, trans, inv_depth, depth_damping, flow, weight, mask):
    f_dev, plocal = inv_depth.shape
    count = lax.axis_size("frames")
    pixes = lax.axis_size("pix")
    fi = lax.axis_index("frames")
    pi = lax.axis_index("pix")
    spot = jnp.stack([fi * f_dev, pi * plocal, pi % 2, fi % 4]).astype(jnp.int32)

    def shift(block, step):
        return lax.ppermute(
            block, "frames", [(i, i + step) for i in range(count) if 0 <= i + step < count]
        )

    edges = (edge_frames, flow.transpose(1, 0, 2), weight.transpose(1, 0, 2), mask)
    down, up = call(
        rim_kernel, "rim", [(8 + 4 * SIDE, plocal), (4 * SIDE, plocal)], 1, spot, *edges
    )
    from_after = shift(down, -1)
    from_before = shift(up, 1)
    tab, b, bt = call(
        pose_kernel, "pose",
        [(f_dev * SLOTS, LANES), (f_dev * GROUP, 3 * LANES), (192, f_dev * GROUP)],
        1, spot, rotvec, trans,
    )
    pairs = f_dev * SLOTS
    geo, curv, grad, block = call(
        early_kernel, "early",
        [(5 * pairs, plocal), (f_dev * 8, plocal), (f_dev * 8, plocal), (f_dev * GROUP, LANES)],
        1, spot, *edges, inv_depth, tab,
        scratch=[pltpu.VMEM((f_dev * 8, plocal), F32), pltpu.VMEM((4 * pairs, plocal), F32)],
    )
    keep, send, base, scale, g = call(
        main_kernel, "main",
        [(96, 256), (96, 256), (f_dev * 8, plocal), (f_dev * 8, plocal), (f_dev * GROUP, plocal)],
        1, spot, from_after, from_before, curv, grad, block, inv_depth, depth_damping, tab, geo, b, bt,
        hbm=3, hbm_out=1,
        scratch=[
            pltpu.VMEM((4 * FD * 8, plocal), F32),
            pltpu.VMEM((GROUP + 16, plocal), F32),
            pltpu.VMEM((GROUP + 16, plocal), F32),
            pltpu.VMEM((256, plocal), F32),
            pltpu.VMEM((GROUP, LANES), F32),
            pltpu.VMEM((GROUP, LANES), F32),
            pltpu.VMEM((f_dev * GROUP, 3 * LANES), F32),
            pltpu.VMEM((192, 3 * LANES), F32),
            pltpu.VMEM((5 * pairs, plocal), F32),
            pltpu.VMEM((f_dev * GROUP, 3 * LANES), F32),
            pltpu.VMEM((192, f_dev * GROUP), F32),
            pltpu.VMEM((f_dev * GROUP, plocal), F32),
            pltpu.SemaphoreType.DMA((f_dev,)),
            pltpu.SemaphoreType.DMA((f_dev,)),
            pltpu.SemaphoreType.DMA((f_dev,)),
            pltpu.SemaphoreType.DMA((1,)),
        ],
    )
    got = lax.ppermute(send, "pix", [(i, i ^ 1) for i in range(pixes)])
    both = keep + got
    own_half, rim = both[:48], both[48:]
    both_axes = ("frames", "pix")

    def to_neighbour(flip):
        route = []
        for i in range(count):
            for k in range(pixes):
                to = i + 1 if k % 2 == 0 else i - 1
                if 0 <= to < count:
                    route.append((i * pixes + k, to * pixes + (k ^ flip)))
        return lax.ppermute(rim, both_axes, route)

    own_far = lax.ppermute(own_half, "pix", [(i, i ^ 2) for i in range(pixes)])
    rim_near = to_neighbour(0)
    rim_far = to_neighbour(2)
    half = (own_half + own_far) + (rim_near + rim_far)

    def mates(v, step):
        return [v] + [
            lax.ppermute(v, "frames", [(i, i ^ (k * step)) for i in range(count)]) for k in (1, 2, 3)
        ]

    def twin(v):
        return lax.ppermute(v, "pix", [(i, i ^ 1) for i in range(pixes)])

    def halo(v):
        return shift(v, 4), v, shift(v, -4)

    (quad,) = call(place_kernel, "place", [(192, 256)], 1, spot, *mates(half, 1))
    pieces = halo(quad)
    wide = BLOCKS * GROUP
    columns = [pltpu.VMEM((wide, LANES), F32)] * 8
    split = [pltpu.VMEM((wide, 2 * LANES), F32)] * 2 + [pltpu.VMEM((wide, LANES), F32)] * 2
    s, up, vs, v4 = call(
        first_kernel, "first",
        [(wide, 256), (wide, LANES), (5 * BLOCKS * 8, LANES), (8, LANES)],
        1, spot, *pieces, *[twin(x) for x in pieces], scratch=columns + split,
    )
    part, v45 = call(
        second_kernel, "second", [(8, LANES), (3 * BLOCKS * 8, LANES)], 0, s, up, vs, *halo(v4),
        scratch=columns,
    )
    (part,) = call(sum_kernel, "sum", [(8, LANES)], 0, *mates(part, 4))
    pose_step, depth_step = call(
        solve_kernel, "solve", [(6, f_dev), (f_dev, plocal)], 1, spot, *mates(part, 16), vs, v45,
        base, scale, b, g,
        scratch=[
            pltpu.VMEM((f_dev * 8, plocal), F32),
            pltpu.VMEM((f_dev * GROUP, 3 * LANES), F32),
            pltpu.VMEM((f_dev * GROUP, plocal), F32),
            pltpu.SemaphoreType.DMA((2,)),
        ],
        hbm=2,
    )
    return pose_step, depth_step


def solution(mesh):
    return jax.shard_map(
        per_device,
        mesh=mesh,
        in_specs=(
            P(None, "frames"),
            P(),
            P(),
            P("frames", "pix"),
            P("frames", "pix"),
            P("frames", None, "pix"),
            P("frames", None, "pix"),
            P("frames", "pix"),
        ),
        out_specs=(P(None, "frames"), P("frames", "pix")),
        check_vma=False,
    )
```

```python
import functools
import jax
import jax.numpy as jnp
from jax import lax
from jax.experimental import pallas as pl
from jax.experimental.pallas import tpu as pltpu
from jax.sharding import PartitionSpec as P

ROWS = 48
COLS = 64
RADIUS = 8
ITERS = 6
HIGHEST = lax.Precision.HIGHEST
F32 = jnp.float32
BF16 = jnp.bfloat16
LANES = 128
FD = 16
SLOTS = 16
GROUP = FD * 6
SIDE = RADIUS * (RADIUS + 1) // 2
POSE_REG = 100.0


def iota(shape, dim):
    return lax.broadcasted_iota(jnp.int32, shape, dim)


def thirds(x):
    first = x.astype(BF16)
    rest = x - first.astype(F32)
    second = rest.astype(BF16)
    return first, second, (rest - second.astype(F32)).astype(BF16)


def pair_of(x):
    first = x.astype(BF16)
    return first, (x - first.astype(F32)).astype(BF16)


def dot(a, b):
    return jnp.dot(a, b, preferred_element_type=F32)


def spread(where_ref, ef_ref, flow_ref, weight_ref, mask_ref, rims, write):
    edges = ef_ref.shape[1]
    start = where_ref[0]
    source = ef_ref[0:1, :] - start
    delta = ef_ref[1:2, :] - start - source
    slot = jnp.where(delta < 0, delta + 8, delta + 7)
    if rims:
        j = source + 8
        down_at = jnp.where(source < 0, ((j * (j + 1)) >> 1) + delta - 8 + j, -1)
        j = 23 - source
        up_at = jnp.where(source >= FD, ((j * (j + 1)) >> 1) + slot, -1)
        row = iota((40, edges), 0)
        hot = jnp.concatenate([(row == down_at).astype(F32), (row == up_at).astype(F32)], axis=0)
    else:
        own_at = jnp.where((source >= 0) & (source < FD), source * SLOTS + slot, -1)
        hot = (iota((FD * SLOTS, edges), 0) == own_at).astype(F32)
    hot = hot.astype(BF16)
    for chunk in range(mask_ref.shape[1] // LANES):
        lanes = pl.ds(chunk * LANES, LANES)
        live = mask_ref[:, lanes].astype(F32)
        parts = []
        for comp in range(2):
            conf = weight_ref[comp, :, lanes] * live
            parts.append((conf, conf * flow_ref[comp, :, lanes]))
        values = jnp.concatenate([parts[0][0], parts[1][0], parts[0][1], parts[1][1]], axis=1)
        split = pair_of if rims else thirds
        got = sum(dot(hot, piece) for piece in reversed(split(values)))
        for q in range(4):
            write(q, lanes, got[:, q * LANES : (q + 1) * LANES])


def rim_kernel(where_ref, ef_ref, flow_ref, weight_ref, mask_ref, down_ref, up_ref):
    down_ref[0:8, :] = jnp.zeros((8, down_ref.shape[1]), F32)

    def write(q, lanes, cut):
        down_ref[8 + q * SIDE : 8 + (q + 1) * SIDE, lanes] = cut[0:SIDE]
        up_ref[q * SIDE : (q + 1) * SIDE, lanes] = cut[40 : 40 + SIDE]

    spread(where_ref, ef_ref, flow_ref, weight_ref, mask_ref, True, write)


def rotation_rows(w):
    x, y, z = w
    zero = jnp.zeros_like(x)
    cross = [[zero, -z, y], [z, zero, -x], [-y, x, zero]]
    sq = x * x + y * y + z * z
    first = 1.0 - sq / 6.0 + sq * sq / 120.0
    second = 0.5 - sq / 24.0 + sq * sq / 720.0
    return [
        [
            float(i == k)
            + first * cross[i][k]
            + second * sum(cross[i][m] * cross[m][k] for m in range(3))
            for k in range(3)
        ]
        for i in range(3)
    ]


def pose_kernel(where_ref, rotvec_ref, trans_ref, tab_ref, b_ref, bt_ref):
    start = where_ref[0]
    frames = rotvec_ref.shape[1]
    pair = iota((1, FD * SLOTS), 1)
    slot = pair & 15
    delta = jnp.where(slot < 8, slot - 8, slot - 7)
    at_source = start + (pair >> 4)
    at_target = jnp.clip(at_source + delta, 0, frames - 1)
    poses = jnp.concatenate([rotvec_ref[...], trans_ref[...], jnp.zeros((2, frames), F32)], axis=0)
    first = start - RADIUS
    poses = pltpu.roll(poses, (2 * frames - first) % frames, 1)[:, 0:LANES]

    def pick(at):
        hot = (iota((LANES, FD * SLOTS), 0) == at - first).astype(F32)
        return jnp.dot(poses, hot, precision=HIGHEST, preferred_element_type=F32)

    src = pick(at_source)
    tgt = pick(at_target)
    rs = rotation_rows([src[k : k + 1] for k in range(3)])
    rt = rotation_rows([tgt[k : k + 1] for k in range(3)])
    rel = [[sum(rt[i][k] * rs[m][k] for k in range(3)) for m in range(3)] for i in range(3)]
    tr = [
        tgt[3 + i : 4 + i] - sum(rel[i][m] * src[3 + m : 4 + m] for m in range(3)) for i in range(3)
    ]
    corner = [
        [tr[1] * rel[2][m] - tr[2] * rel[1][m] for m in range(3)],
        [tr[2] * rel[0][m] - tr[0] * rel[2][m] for m in range(3)],
        [tr[0] * rel[1][m] - tr[1] * rel[0][m] for m in range(3)],
    ]
    lines = [x for row in rel for x in row] + tr + [x for row in corner for x in row]
    lines = jnp.concatenate(lines + [jnp.zeros((LANES - len(lines), FD * SLOTS), F32)], axis=0)
    tab_ref[...] = lines.T

    lane3 = iota((SLOTS, 3 * LANES), 1)
    row3 = iota((SLOTS, 3 * LANES), 0)
    off3 = jnp.where(row3 < 8, row3 - 8, row3 - 7)

    def build(f, carry):
        frame = f + off3 + FD
        home = (frame >> 4) * LANES + (frame & 15) * 6
        tab = tab_ref[pl.ds(pl.multiple_of(f * SLOTS, SLOTS), SLOTS), :]
        for c in range(6):
            block = jnp.where(lane3 == home + c, 1.0, 0.0)
            for d in range(6):
                if c < 3:
                    at = c * 3 + d if d < 3 else 12 + c * 3 + d - 3
                elif d >= 3:
                    at = (c - 3) * 3 + d - 3
                else:
                    continue
                block = block - jnp.where(
                    lane3 == LANES + f * 6 + d, jnp.broadcast_to(tab[:, at : at + 1], lane3.shape), 0.0
                )
            b_ref[pl.ds(pl.multiple_of(f * GROUP + c * SLOTS, SLOTS), SLOTS), :] = block
        return carry

    lax.fori_loop(0, FD, build, 0)
    for g in range(4):
        cols = slice(g * 384, (g + 1) * 384)
        below = b_ref[cols, 0:LANES].T
        own = b_ref[cols, LANES : 2 * LANES].T
        above = b_ref[cols, 2 * LANES : 3 * LANES].T
        bt_ref[0:48, cols] = below[48:96]
        bt_ref[48:144, cols] = own[0:96]
        bt_ref[144:192, cols] = above[0:48]


def coords(first, chunk):
    pixel = first + chunk * LANES + iota((8, LANES), 1)
    col = ((pixel & (COLS - 1)).astype(F32) - 0.5 * (COLS - 1)) / COLS
    line = ((pixel >> 6).astype(F32) - 0.5 * (ROWS - 1)) / COLS
    return col, line


def pull(u, v, s, uv, u1, v1, pu, pv):
    spu = s * pu
    spv = s * pv
    return (
        spu,
        spv,
        -(u * spu + v * spv),
        -(uv * pu) - v1 * pv,
        u1 * pu + uv * pv,
        u * pv - v * pu,
    )


def pose_sums(u, v, s, cu, cv, eu, ev):
    uv = u * v
    u1 = 1.0 + u * u
    v1 = 1.0 + v * v
    terms = list(pull(u, v, s, uv, u1, v1, -eu, -ev))
    su_ = cu * s
    sv_ = cv * s
    ju = (-uv, u1, -v)
    jv = (-v1, uv, u)
    a00 = su_ * s
    a11 = sv_ * s
    a02 = -(a00 * u)
    a12 = -(a11 * v)
    terms += [a00, a11, a02, a12, -(a02 * u + a12 * v)]
    tu = [su_ * x for x in ju]
    tv = [sv_ * x for x in jv]
    terms += tu + tv
    terms += [-(u * x + v * y) for x, y in zip(tu, tv)]
    wu = [cu * x for x in ju]
    wv = [cv * x for x in jv]
    for a in range(3):
        for b in range(a, 3):
            terms.append(wu[a] * ju[b] + wv[a] * jv[b])
    return terms


def diagonal_rows(acc, h):
    lane = iota((8, LANES), 1)
    row = iota((8, LANES), 0)
    sums = [jnp.broadcast_to(jnp.sum(x, axis=1, keepdims=True), (8, LANES)) for x in acc]
    a = {(0, 0): 6, (1, 1): 7, (0, 2): 8, (1, 2): 9, (2, 2): 10}
    for k in range(3):
        a[(0, 3 + k)] = 11 + k
        a[(1, 3 + k)] = 14 + k
        a[(2, 3 + k)] = 17 + k
    at = 20
    for x in range(3):
        for y in range(x, 3):
            a[(3 + x, 3 + y)] = at
            at += 1
    tiles = []
    for c in range(6):
        tile = jnp.where(lane == LANES - 1, sums[c], 0.0)
        for d in range(6):
            key = (min(c, d), max(c, d))
            if key != (0, 1):
                tile = jnp.where(lane == d * SLOTS + 8 * h + row, sums[a[key]], tile)
        tiles.append(tile)
    return tiles


def early_kernel(
    where_ref, ef_ref, flow_ref, weight_ref, mask_ref, depth_ref, tab_ref,
    geo_ref, curv_ref, grad_ref, block_ref, in_ref, own_ref,
):
    def write(q, lanes, cut):
        own_ref[q * 256 : (q + 1) * 256, lanes] = cut

    spread(where_ref, ef_ref, flow_ref, weight_ref, mask_ref, False, write)
    plocal = depth_ref.shape[1]
    chunks = plocal // LANES
    for f in range(FD):
        in_ref[f * 8 : f * 8 + 8, :] = jnp.broadcast_to(depth_ref[f : f + 1, :], (8, plocal))

    def frame(f, carry):
        eight = pl.ds(pl.multiple_of(f * 8, 8), 8)
        for h in range(2):
            tab = tab_ref[pl.ds(pl.multiple_of(f * SLOTS + 8 * h, 8), 8), :]
            r = [jnp.broadcast_to(tab[:, k : k + 1], (8, LANES)) for k in range(12)]
            acc = [0.0] * 26
            for c in range(chunks):
                lanes = pl.ds(c * LANES, LANES)
                col, line = coords(where_ref[1], c)
                depth = in_ref[eight, lanes]

                def at(q):
                    return pl.ds(pl.multiple_of(q * 256 + f * SLOTS + 8 * h, 8), 8)

                cu, cv, fu, fv = [own_ref[at(q), lanes] for q in range(4)]
                inv = 1.0 / (r[6] * col + r[7] * line + r[8] + depth * r[11])
                u = (r[0] * col + r[1] * line + r[2] + depth * r[9]) * inv
                v = (r[3] * col + r[4] * line + r[5] + depth * r[10]) * inv
                su = inv * (r[9] - u * r[11])
                sv = inv * (r[10] - v * r[11])
                eu = cu * (col - u) + fu
                ev = cv * (line - v) + fv
                au = cu * su
                av = cv * sv
                curv = au * su + av * sv
                grad = -(su * eu + sv * ev)
                if h:
                    curv = curv + curv_ref[eight, lanes]
                    grad = grad + grad_ref[eight, lanes]
                curv_ref[eight, lanes] = curv
                grad_ref[eight, lanes] = grad
                for q, x in enumerate((u, v, inv, au, av)):
                    row = pl.multiple_of((f * 5 + q) * SLOTS + 8 * h, 8)
                    geo_ref[pl.ds(row, 8), lanes] = x
                acc = [x + y for x, y in zip(acc, pose_sums(u, v, depth * inv, cu, cv, eu, ev))]
            for c, tile in enumerate(diagonal_rows(acc, h)):
                block_ref[pl.ds(pl.multiple_of(f * GROUP + c * SLOTS + 8 * h, 8), 8), :] = tile
        return carry

    lax.fori_loop(0, FD, frame, 0)


def main_kernel(
    where_ref, rdown_ref, rup_ref, curv_ref, grad_ref, block_ref, depth_ref, damp_ref, tab_ref,
    geo_hbm, b_hbm, bt_hbm,
    keep_ref, send_ref, base_ref, scale_ref, g_hbm,
    half_ref, hi0_ref, hi1_ref, in_ref, q0_ref, q1_ref, w_ref, t_ref, geo_ref, b_ref, bt_ref, g_ref,
    geo_sems, b_sems, g_sems, bt_sem,
):
    def piece(src, dst, sems, f, rows):
        at = pl.ds(pl.multiple_of(f * rows, 8), rows)
        return pltpu.make_async_copy(src.at[at, :], dst.at[at, :], sems.at[f])

    for f in range(FD):
        piece(geo_hbm, geo_ref, geo_sems, f, 5 * SLOTS).start()
        piece(b_hbm, b_ref, b_sems, f, GROUP).start()
    bt_copy = pltpu.make_async_copy(bt_hbm, bt_ref, bt_sem.at[0])
    bt_copy.start()
    core = where_ref[2]
    plocal = depth_ref.shape[1]
    chunks = plocal // LANES
    row8 = iota((8, plocal), 0)
    for f in range(FD):
        j = 7 - f if f < 8 else f - 8
        base = j * (j + 1) // 2
        for q in range(4):
            if f < 8:
                first = q * SIDE + base
                extra = jnp.where(row8 <= j, rup_ref[first : first + 8, :], 0.0)
            else:
                first = 8 + q * SIDE + base - 7 + j
                extra = jnp.where(row8 >= 7 - j, rdown_ref[first : first + 8, :], 0.0)
            half_ref[(q * FD + f) * 8 : (q * FD + f + 1) * 8, :] = extra
        in_ref[f * 8 : f * 8 + 8, :] = jnp.broadcast_to(depth_ref[f : f + 1, :], (8, plocal))
        in_ref[128 + f * 8 : 136 + f * 8, :] = jnp.broadcast_to(damp_ref[f : f + 1, :], (8, plocal))
    lane = iota((8, LANES), 1)

    def tiles(f, merged, hi_ref, q_ref):
        eight = pl.ds(pl.multiple_of(f * 8, 8), 8)
        tab = tab_ref[pl.ds(pl.multiple_of(f * SLOTS + 8 * merged, 8), 8), :]
        t0, t1, t2 = [jnp.broadcast_to(tab[:, k : k + 1], (8, LANES)) for k in (9, 10, 11)]
        acc = [0.0] * 26
        for c in range(chunks):
            lanes = pl.ds(c * LANES, LANES)
            col, line = coords(where_ref[1], c)
            depth = in_ref[eight, lanes]

            def geo(q, h):
                return geo_ref[pl.ds(pl.multiple_of((f * 5 + q) * SLOTS + 8 * h, 8), 8), lanes]

            cu, cv, fu, fv = [
                half_ref[pl.ds(pl.multiple_of((q * FD + f) * 8, 8), 8), lanes] for q in range(4)
            ]
            u, v, inv = [geo(q, merged) for q in range(3)]
            su = inv * (t0 - u * t2)
            sv = inv * (t1 - v * t2)
            eu = cu * (col - u) + fu
            ev = cv * (line - v) + fv
            au = cu * su
            av = cv * sv
            acc = [x + y for x, y in zip(acc, pose_sums(u, v, depth * inv, cu, cv, eu, ev))]
            curv = curv_ref[eight, lanes] + (au * su + av * sv)
            grad = grad_ref[eight, lanes] - (su * eu + sv * ev)
            total = in_ref[pl.ds(pl.multiple_of(128 + f * 8, 8), 8), lanes] + jnp.sum(
                curv, axis=0, keepdims=True
            )
            base = jnp.sum(grad, axis=0, keepdims=True) / total
            root = jnp.sqrt(total)
            scale = 1.0 / root
            base_ref[eight, lanes] = base
            scale_ref[eight, lanes] = scale
            lifted = base * root
            hi_ref[GROUP : GROUP + 8, lanes] = lifted
            hi_ref[GROUP + 8 : GROUP + 16, lanes] = lifted - lifted.astype(BF16).astype(F32)
            for h in range(2):
                if h != merged:
                    u, v, inv = [geo(q, h) for q in range(3)]
                    gu, gv = geo(3, h), geo(4, h)
                else:
                    u, v, inv = [geo(q, h) for q in range(3)]
                    gu, gv = geo(3, h) + au, geo(4, h) + av
                rows = pull(
                    u, v, depth * inv, u * v, 1.0 + u * u, 1.0 + v * v, gu * scale, gv * scale
                )
                for k, x in enumerate(rows):
                    g_ref[pl.ds(pl.multiple_of(f * GROUP + k * SLOTS + 8 * h, 8), 8), lanes] = x
                    hi_ref[k * SLOTS + 8 * h : k * SLOTS + 8 * h + 8, lanes] = x
        q_ref[...] = block_ref[pl.ds(pl.multiple_of(f * GROUP, 8), GROUP), :]
        for c, tile in enumerate(diagonal_rows(acc, merged)):
            at = slice(c * SLOTS + 8 * merged, c * SLOTS + 8 * merged + 8)
            q_ref[at, :] = q_ref[at, :] + tile

    def matmuls(f, hi_ref, q_ref):
        rows = pl.ds(pl.multiple_of(f * GROUP, 8), GROUP)
        g = hi_ref[...]
        top, low = pair_of(g)
        both = lax.dot_general(
            jnp.concatenate([top[0:GROUP], low[0:GROUP]], axis=0), top, (((1,), (1,)), ((), ())),
            preferred_element_type=F32,
        )
        m = both[0:GROUP, 0:GROUP] + both[GROUP:, 0:GROUP] + both[GROUP:, 0:GROUP].T
        vec = q_ref[:, LANES - 1 : LANES] - (
            both[0:GROUP, GROUP : GROUP + 1]
            + both[GROUP:, GROUP : GROUP + 1]
            + both[0:GROUP, GROUP + 8 : GROUP + 9]
        )
        q = q_ref[:, 0:GROUP] - m
        q_top, q_low = pair_of(q)
        b_top, b_low = pair_of(b_ref[rows, :])
        both = dot(jnp.concatenate([q_top, q_low], axis=0), b_top)
        w = both[0:GROUP] + both[GROUP:]
        w_ref[rows, 0:LANES] = jnp.where(
            iota((GROUP, LANES), 1) == LANES - 1, jnp.broadcast_to(vec, (GROUP, LANES)), w[:, 0:LANES]
        )
        w_ref[rows, LANES : 2 * LANES] = w[:, LANES : 2 * LANES] + dot(q_top, b_low[:, LANES : 2 * LANES])
        w_ref[rows, 2 * LANES :] = w[:, 2 * LANES :]

    def frames(i, carry, merged):
        work = ((2 * i, hi0_ref, q0_ref), (2 * i + 1, hi1_ref, q1_ref))
        for f, _, _ in work:
            piece(geo_hbm, geo_ref, geo_sems, f, 5 * SLOTS).wait()
            piece(b_hbm, b_ref, b_sems, f, GROUP).wait()
        for f, hi_ref, q_ref in work:
            tiles(f, merged, hi_ref, q_ref)
        for f, hi_ref, q_ref in work:
            matmuls(f, hi_ref, q_ref)
        for f, _, _ in work:
            piece(g_ref, g_hbm, g_sems, f, GROUP).start()
        return carry

    lax.fori_loop(0, 4, functools.partial(frames, merged=0), 0)
    lax.fori_loop(4, 8, functools.partial(frames, merged=1), 0)
    bt_copy.wait()
    bt_top, bt_low = pair_of(bt_ref[...])
    w_top, w_low = pair_of(w_ref[...])
    both = dot(jnp.concatenate([bt_top, bt_low], axis=0), w_top)
    t = both[0:192] + both[192:] + dot(bt_top, w_low)
    t_ref[...] = t
    for lo, hi, group, first in ((0, 48, 0, 48), (48, 144, 1, 0), (144, 192, 2, 0)):
        count = hi - lo
        lanes = slice(group * LANES, (group + 1) * LANES)
        square = jnp.concatenate(
            [jnp.zeros((first, LANES), F32)] * (first > 0)
            + [t[lo:hi, lanes], jnp.zeros((LANES - first - count, LANES), F32)],
            axis=0,
        )
        mean = 0.5 * (square + square.T)
        t_ref[lo:hi, lanes] = mean[first : first + count]
    last = iota((48, LANES), 1) == LANES - 1

    def half(core):
        own = slice(48 + 48 * core, 96 + 48 * core)
        rim = slice(0, 48) if core else slice(144, 192)
        group = 0 if core else 2
        mine = jnp.where(last, t[own, 0:LANES], t_ref[own, LANES : 2 * LANES])
        theirs = jnp.where(last, t[rim, 0:LANES], t_ref[rim, group * LANES : (group + 1) * LANES])
        far = t_ref[rim, LANES : 2 * LANES] if core else jnp.zeros((48, LANES), F32)
        return mine, t_ref[own, 2 * LANES :], theirs, far

    def put_half(ref, core):
        for k, x in enumerate(half(core)):
            ref[(k // 2) * 48 : (k // 2 + 1) * 48, (k % 2) * LANES : (k % 2 + 1) * LANES] = x

    @pl.when(core == 0)
    def _():
        put_half(keep_ref, 0)
        put_half(send_ref, 1)

    @pl.when(core == 1)
    def _():
        put_half(keep_ref, 1)
        put_half(send_ref, 0)

    for f in range(FD):
        piece(g_ref, g_hbm, g_sems, f, GROUP).wait()


def to_row(column):
    return jnp.sum(
        jnp.where(iota((GROUP, LANES), 0) == iota((GROUP, LANES), 1), column, 0.0),
        axis=0,
        keepdims=True,
    )


BLOCKS = 12


def place_kernel(where_ref, a_ref, b_ref, c_ref, d_ref, out_ref):
    at = where_ref[3]
    for k, ref in enumerate((a_ref, b_ref, c_ref, d_ref)):
        out_ref[pl.ds(pl.multiple_of(48 * (at ^ k), 8), 48), :] = ref[...]


SHRINK = 2.0**-15
FIRST = 2.0**-10
LARGEST_STEP = 1.001 / (POSE_REG * SHRINK)


def halves(x):
    t = 4097.0 * x
    top = t - (t - x)
    return top, x - top


def times(a, b):
    p = a * b
    ah, al = halves(a)
    bh, bl = halves(b)
    return p, ((ah * bh - p) + ah * bl + al * bh) + al * bl


def plus(a, b):
    t = a[0] + b[0]
    back = t - a[0]
    return t, (a[1] + b[1]) + ((a[0] - (t - back)) + (b[0] - back))


def tidy(a):
    t = a[0] + a[1]
    return t, a[1] - (t - a[0])


def mul(a, b):
    p, e = times(a[0], b[0])
    return tidy((p, e + (a[0] * b[1] + a[1] * b[0])))


def add(a, b):
    return tidy(plus(a, b))


def neg(a):
    return -a[0], -a[1]


def div(a, b):
    q = a[0] / b[0]
    rest = add(a, neg(mul((q, jnp.zeros_like(q)), b)))
    return tidy((q, rest[0] / b[0]))


def lane_total(a):
    for step in (64, 32, 16, 8, 4, 2, 1):
        a = plus(a, (pltpu.roll(a[0], step, 1), pltpu.roll(a[1], step, 1)))
    return a


def to_column(row):
    eye = iota((GROUP, LANES), 0) == iota((GROUP, LANES), 1)
    return jnp.broadcast_to(
        jnp.sum(jnp.where(eye, row, 0.0), axis=1, keepdims=True), (GROUP, LANES)
    )


def block_at(j):
    return pl.ds(pl.multiple_of(j * GROUP, 8), GROUP)


def tile_at(j):
    return pl.ds(pl.multiple_of(j * 8, 8), 8)


def product(s_ref, up_ref, col, split, j):
    acc = None
    lower, upper = slice(0, LANES), slice(LANES, 2 * LANES)
    sources = ((s_ref, lower, j, j), (s_ref, upper, j - 1, j - 1), (up_ref, slice(0, LANES), j, j + 1))
    for n, (ref, lanes, row, at) in enumerate(sources):
        s = ref[block_at(row), lanes]
        if split is None:
            sh, sl = halves(s)
        else:
            sh, sl = [x[block_at(row), lanes] for x in (split[2:] if n == 2 else split[:2])]
        high, low, hh, hl = [x[block_at(at), :] for x in col]
        p = s * high
        e = (((sh * hh - p) + sh * hl + sl * hh) + sl * hl) + s * low
        for r in range(0, GROUP, 8):
            term = p[r : r + 8], e[r : r + 8]
            acc = term if acc is None else plus(acc, term)
    for step in (4, 2, 1):
        acc = plus(acc, (pltpu.roll(acc[0], step, 0), pltpu.roll(acc[1], step, 0)))
    acc = tidy(acc)
    return acc[0] * SHRINK, acc[1] * SHRINK


def put_column(col, j, high, low):
    col[0][block_at(j), :] = high
    col[1][block_at(j), :] = low
    col[2][block_at(j), :], col[3][block_at(j), :] = halves(high)


def store_tile(ref, at, pair):
    row = iota((8, LANES), 0)
    ref[tile_at(at), :] = jnp.where(row == 0, pair[0], jnp.where(row == 1, pair[1], 0.0))


def powers(s_ref, up_ref, v_ref, cols, split, first, count, edge, base):
    for k in range(count):
        here, there = cols[k % 2], cols[1 - k % 2]

        def one(j, carry):
            pair = product(s_ref, up_ref, here, split, j)
            store_tile(v_ref, (first + k) * BLOCKS + j, pair)
            put_column(there, j, to_column(pair[0][0:1]), to_column(pair[1][0:1]))
            return carry

        lax.fori_loop(base + k * edge, BLOCKS - base - k * edge, one, 0)


def first_kernel(
    where_ref, p_ref, c_ref, n_ref, p2_ref, c2_ref, n2_ref,
    s_ref, up_ref, v_ref, v4_ref, *scratch,
):
    cols = scratch[0:4], scratch[4:8]
    split = scratch[8:12]
    core = where_ref[2]
    mine = pl.multiple_of(48 * core, 8)
    theirs = pl.multiple_of(48 - 48 * core, 8)
    diagonal = iota((GROUP, LANES), 0) == iota((GROUP, LANES), 1)
    lane = iota((GROUP, LANES), 1)
    for j in range(BLOCKS):
        rows = slice((j % 4) * 48, (j % 4 + 1) * 48)
        a = (p_ref, c_ref, n_ref)[j // 4]
        b = (p2_ref, c2_ref, n2_ref)[j // 4]
        s_ref[pl.ds(j * GROUP + mine, 48), :] = a[rows, :]
        s_ref[pl.ds(j * GROUP + theirs, 48), :] = b[rows, :]
    zero = jnp.zeros((LANES - GROUP, LANES), F32)

    def prepare(j, carry):
        own = s_ref[block_at(j), 0:LANES]
        rhs = jnp.broadcast_to(own[:, LANES - 1 : LANES], (GROUP, LANES)) * FIRST
        put_column(cols[0], j, rhs, jnp.zeros_like(rhs))
        store_tile(v_ref, j, (to_row(rhs), jnp.zeros((1, LANES), F32)))
        s_ref[block_at(j), 0:LANES] = jnp.where(lane < GROUP, own, 0.0) + jnp.where(
            diagonal, POSE_REG, 0.0
        )
        up = jnp.concatenate([s_ref[block_at(j), LANES : 2 * LANES], zero], axis=0).T
        up_ref[block_at(j), :] = up[0:GROUP]
        split[0][block_at(j), :], split[1][block_at(j), :] = halves(s_ref[block_at(j), :])
        split[2][block_at(j), :], split[3][block_at(j), :] = halves(up[0:GROUP])
        return carry

    lax.fori_loop(0, BLOCKS, prepare, 0)
    powers(s_ref, up_ref, v_ref, cols, split, 1, 4, 1, 1)
    for j in range(4):
        at = (4 * BLOCKS + 4 + j) * 8
        v4_ref[j : j + 1, :] = v_ref[at : at + 1, :]
        v4_ref[4 + j : 5 + j, :] = v_ref[at + 1 : at + 2, :]


def second_kernel(
    s_ref, up_ref, v_ref, below_ref, own_ref, above_ref, out_ref, v45_ref, *scratch,
):
    cols = scratch[0:4], scratch[4:8]
    for g, ref in enumerate((below_ref, own_ref, above_ref)):
        for j in range(4):
            pair = ref[j : j + 1, :], ref[4 + j : 5 + j, :]
            at = g * 4 + j
            store_tile(v45_ref, at, pair)
            if 1 < at < 10:
                put_column(cols[0], at, to_column(pair[0]), to_column(pair[1]))
    powers(s_ref, up_ref, v45_ref, cols, None, 1, 2, 1, 3)
    zero = jnp.zeros((1, LANES), F32)
    total = None
    for j in range(4, 8):

        def row(k, part):
            ref, at = (v_ref, k) if k < 4 else (v45_ref, k - 4)
            at = (at * BLOCKS + j) * 8 + part
            return ref[at : at + 1, :]

        def stack(pick, part):
            lines = [row(pick(m), part) for m in range(2 * ITERS)]
            return jnp.concatenate(lines + [zero] * (16 - len(lines)), axis=0)

        lower, upper = (lambda m: m // 2), (lambda m: m - m // 2)
        a, b = (stack(lower, 0), stack(lower, 1)), (stack(upper, 0), stack(upper, 1))
        p, e = times(a[0], b[0])
        term = p, e + (a[0] * b[1] + a[1] * b[0])
        total = term if total is None else plus(total, term)
    total = tidy(lane_total(total))
    diagonal = iota((16, LANES), 0) == iota((16, LANES), 1)
    put(
        out_ref,
        [jnp.sum(jnp.where(diagonal, x, 0.0), axis=0, keepdims=True) for x in total],
    )


def put(ref, pair):
    ref[...] = jnp.zeros((8, LANES), F32)
    ref[0:1, :] = pair[0]
    ref[1:2, :] = pair[1]


def gather_sum(refs):
    acc = refs[0][0:1, :], refs[0][1:2, :]
    for r in refs[1:]:
        acc = plus(acc, (r[0:1, :], r[1:2, :]))
    return tidy(acc)


def sum_kernel(a_ref, b_ref, c_ref, d_ref, out_ref):
    put(out_ref, gather_sum((a_ref, b_ref, c_ref, d_ref)))


def solve_kernel(
    where_ref, a_ref, b_ref, c_ref, d_ref, v_ref, v45_ref, base_ref, scale_ref, move_hbm, g_hbm,
    pose_ref, out_ref, sum_ref, move_ref, g_ref, sems,
):
    copies = [
        pltpu.make_async_copy(move_hbm, move_ref, sems.at[0]),
        pltpu.make_async_copy(g_hbm, g_ref, sems.at[1]),
    ]
    for copy in copies:
        copy.start()
    at_quad = where_ref[3]
    total = gather_sum((a_ref, b_ref, c_ref, d_ref))
    shape = (8, LANES)
    row = iota(shape, 0)
    lane = iota(shape, 1)
    zero = jnp.zeros(shape, F32)
    unit = jnp.where((row == 1) & (lane == LANES - 1), 1.0, 0.0)

    def where(live, a, b):
        return jnp.where(live, a[0], b[0]), jnp.where(live, a[1], b[1])

    def at(a, r, k):
        return tuple(jnp.broadcast_to(x[r : r + 1, k : k + 1], shape) for x in a)

    x = jnp.where(row == 0, total[0], unit), jnp.where(row == 0, total[1], 0.0)
    y = x
    found = (zero, zero)
    one = (zero + 1.0, zero)
    start = at(x, 0, 0)
    now = start
    lead = one[0]
    live = start[0] > 0.0
    for k in range(ITERS):
        alpha = div(now, where(live, at(y, 0, k + 1), one))
        live = live & (alpha[0] > 0.0) & (alpha[0] < LARGEST_STEP)
        alpha = where(live, alpha, (zero, zero))
        found = add(found, mul(alpha, y))
        if k + 1 == ITERS:
            break
        back = neg(alpha)
        moved = tuple(pltpu.roll(p, LANES - 1, 1) for p in y)
        x = add(x, mul(back, moved))
        fresh = at(x, 0, k + 1)
        lead = -lead * alpha[0]
        live = live & (lead * fresh[0] > 1e-11 * start[0])
        beta = div(mul(back, fresh), where(live, now, one))
        beta = where(live, beta, (zero, zero))
        y = add(x, mul(beta, y))
        now = fresh
    xc = [tuple(p[1:2, LANES - 1 - k : LANES - k] for p in found) for k in range(ITERS)]
    poses = []
    for g in range(3):
        acc = None
        for k in range(ITERS):
            ref = v_ref if k < 4 else v45_ref
            tile = ref[tile_at((k if k < 4 else k - 4) * BLOCKS + 3 + at_quad + g), :]
            wide = tuple(jnp.broadcast_to(x, (1, LANES)) for x in xc[k])
            term = mul(wide, (tile[0:1], tile[1:2]))
            acc = term if acc is None else plus(acc, term)
        poses.append((acc[0] + acc[1]) * (SHRINK / FIRST))
    column = to_column(poses[1])
    r = iota((GROUP, LANES), 0)
    l = iota((GROUP, LANES), 1)
    for c in range(6):
        line = jnp.sum(jnp.where(r == l * 6 + c, column, 0.0), axis=0, keepdims=True)
        pose_ref[c : c + 1, :] = line[:, 0:FD]
    for copy in copies:
        copy.wait()

    def frame(f, carry):
        rows = pl.ds(pl.multiple_of(f * GROUP, 8), GROUP)
        prod = (
            move_ref[rows, 0:LANES] * poses[0]
            + move_ref[rows, LANES : 2 * LANES] * poses[1]
            + move_ref[rows, 2 * LANES : 3 * LANES] * poses[2]
        )
        x = jnp.sum(prod, axis=1, keepdims=True)
        image = jnp.sum(g_ref[rows, :] * x, axis=0, keepdims=True)
        at = tile_at(f)
        sum_ref[at, :] = base_ref[at, :] - scale_ref[at, :] * image
        return carry

    lax.fori_loop(0, FD, frame, 0)
    for f in range(FD):
        out_ref[f : f + 1, :] = sum_ref[f * 8 : f * 8 + 1, :]


SMEM = pl.BlockSpec(memory_space=pltpu.SMEM)
VMEM = pl.BlockSpec(memory_space=pltpu.VMEM)
ANY = pl.BlockSpec(memory_space=pl.ANY)


def call(kernel, name, outs, smem, *args, scratch=(), hbm=0, hbm_out=0):
    return pl.pallas_call(
        kernel,
        name=name,
        out_shape=[jax.ShapeDtypeStruct(s, F32) for s in outs],
        in_specs=[SMEM] * smem + [VMEM] * (len(args) - smem - hbm) + [ANY] * hbm,
        out_specs=[VMEM] * (len(outs) - hbm_out) + [ANY] * hbm_out,
        scratch_shapes=list(scratch),
    )(*args)


def per_device(edge_frames, rotvec, trans, inv_depth, depth_damping, flow, weight, mask):
    f_dev, plocal = inv_depth.shape
    count = lax.axis_size("frames")
    pixes = lax.axis_size("pix")
    fi = lax.axis_index("frames")
    pi = lax.axis_index("pix")
    spot = jnp.stack([fi * f_dev, pi * plocal, pi % 2, fi % 4]).astype(jnp.int32)

    def shift(block, step):
        return lax.ppermute(
            block, "frames", [(i, i + step) for i in range(count) if 0 <= i + step < count]
        )

    edges = (edge_frames, flow.transpose(1, 0, 2), weight.transpose(1, 0, 2), mask)
    down, up = call(
        rim_kernel, "rim", [(8 + 4 * SIDE, plocal), (4 * SIDE, plocal)], 1, spot, *edges
    )
    from_after = shift(down, -1)
    from_before = shift(up, 1)
    tab, b, bt = call(
        pose_kernel, "pose",
        [(f_dev * SLOTS, LANES), (f_dev * GROUP, 3 * LANES), (192, f_dev * GROUP)],
        1, spot, rotvec, trans,
    )
    pairs = f_dev * SLOTS
    geo, curv, grad, block = call(
        early_kernel, "early",
        [(5 * pairs, plocal), (f_dev * 8, plocal), (f_dev * 8, plocal), (f_dev * GROUP, LANES)],
        1, spot, *edges, inv_depth, tab,
        scratch=[pltpu.VMEM((f_dev * 8, plocal), F32), pltpu.VMEM((4 * pairs, plocal), F32)],
    )
    keep, send, base, scale, g = call(
        main_kernel, "main",
        [(96, 256), (96, 256), (f_dev * 8, plocal), (f_dev * 8, plocal), (f_dev * GROUP, plocal)],
        1, spot, from_after, from_before, curv, grad, block, inv_depth, depth_damping, tab, geo, b, bt,
        hbm=3, hbm_out=1,
        scratch=[
            pltpu.VMEM((4 * FD * 8, plocal), F32),
            pltpu.VMEM((GROUP + 16, plocal), F32),
            pltpu.VMEM((GROUP + 16, plocal), F32),
            pltpu.VMEM((256, plocal), F32),
            pltpu.VMEM((GROUP, LANES), F32),
            pltpu.VMEM((GROUP, LANES), F32),
            pltpu.VMEM((f_dev * GROUP, 3 * LANES), F32),
            pltpu.VMEM((192, 3 * LANES), F32),
            pltpu.VMEM((5 * pairs, plocal), F32),
            pltpu.VMEM((f_dev * GROUP, 3 * LANES), F32),
            pltpu.VMEM((192, f_dev * GROUP), F32),
            pltpu.VMEM((f_dev * GROUP, plocal), F32),
            pltpu.SemaphoreType.DMA((f_dev,)),
            pltpu.SemaphoreType.DMA((f_dev,)),
            pltpu.SemaphoreType.DMA((f_dev,)),
            pltpu.SemaphoreType.DMA((1,)),
        ],
    )
    got = lax.ppermute(send, "pix", [(i, i ^ 1) for i in range(pixes)])
    both = keep + got
    own_half, rim = both[:48], both[48:]
    both_axes = ("frames", "pix")

    def to_neighbour(flip):
        route = []
        for i in range(count):
            for k in range(pixes):
                to = i + 1 if k % 2 == 0 else i - 1
                if 0 <= to < count:
                    route.append((i * pixes + k, to * pixes + (k ^ flip)))
        return lax.ppermute(rim, both_axes, route)

    own_far = lax.ppermute(own_half, "pix", [(i, i ^ 2) for i in range(pixes)])
    rim_near = to_neighbour(0)
    rim_far = to_neighbour(2)
    half = (own_half + own_far) + (rim_near + rim_far)

    def mates(v, step):
        return [v] + [
            lax.ppermute(v, "frames", [(i, i ^ (k * step)) for i in range(count)]) for k in (1, 2, 3)
        ]

    def twin(v):
        return lax.ppermute(v, "pix", [(i, i ^ 1) for i in range(pixes)])

    def halo(v):
        return shift(v, 4), v, shift(v, -4)

    (quad,) = call(place_kernel, "place", [(192, 256)], 1, spot, *mates(half, 1))
    pieces = halo(quad)
    wide = BLOCKS * GROUP
    columns = [pltpu.VMEM((wide, LANES), F32)] * 8
    split = [pltpu.VMEM((wide, 2 * LANES), F32)] * 2 + [pltpu.VMEM((wide, LANES), F32)] * 2
    s, up, vs, v4 = call(
        first_kernel, "first",
        [(wide, 256), (wide, LANES), (5 * BLOCKS * 8, LANES), (8, LANES)],
        1, spot, *pieces, *[twin(x) for x in pieces], scratch=columns + split,
    )
    part, v45 = call(
        second_kernel, "second", [(8, LANES), (3 * BLOCKS * 8, LANES)], 0, s, up, vs, *halo(v4),
        scratch=columns,
    )
    (part,) = call(sum_kernel, "sum", [(8, LANES)], 0, *mates(part, 4))
    pose_step, depth_step = call(
        solve_kernel, "solve", [(6, f_dev), (f_dev, plocal)], 1, spot, *mates(part, 16), vs, v45,
        base, scale, b, g,
        scratch=[
            pltpu.VMEM((f_dev * 8, plocal), F32),
            pltpu.VMEM((f_dev * GROUP, 3 * LANES), F32),
            pltpu.VMEM((f_dev * GROUP, plocal), F32),
            pltpu.SemaphoreType.DMA((2,)),
        ],
        hbm=2,
    )
    return pose_step, depth_step


def solution(mesh):
    return jax.shard_map(
        per_device,
        mesh=mesh,
        in_specs=(
            P(None, "frames"),
            P(),
            P(),
            P("frames", "pix"),
            P("frames", "pix"),
            P("frames", None, "pix"),
            P("frames", None, "pix"),
            P("frames", "pix"),
        ),
        out_specs=(P(None, "frames"), P("frames", "pix")),
        check_vma=False,
    )
```
